128 devices in a mesh: ep: 32 (over y, x, core), dp: 4 (over z).
Axes of the slice: x: 4, y: 4, z: 4, core: 2. Of those that a mesh axis runs over, the one named last changes fastest.
Arguments:
- resid: bfloat16 [2048, 4096], P(('ep', 'dp')), may hold values from -6 to 6
- queries: bfloat16 [2048, 8192], P(('ep', 'dp')), may hold values from -4.5 to 4.5
- new_keys: bfloat16 [2048, 512], P(('ep', 'dp')), may hold values from -4.5 to 4.5
- new_values: bfloat16 [2048, 512], P(('ep', 'dp')), may hold values from -6 to 6
- cache_keys: bfloat16 [2048, 128, 512], P(('ep', 'dp')), may hold values from -4.5 to 4.5
- cache_values: bfloat16 [2048, 128, 512], P(('ep', 'dp')), may hold values from -6 to 6
- cache_len: int32 [2048], P(('ep', 'dp')), may hold values from 1 to 128
- out_proj: bfloat16 [8192, 4096], P('ep'), may hold values from -0.0625 to 0.0625
- norm_gain: float32 [4096], replicated, may hold values from 0.1 to 1.9
- router: bfloat16 [4096, 64], replicated, may hold values from -4 to 4
- expert_ids: int32 [2048, 8], P(('ep', 'dp')), may hold values from 0 to 63, all different within a row; in each aligned block of 16 rows (0 to 15, 16 to 31, ...) at most 4 rows name the same one
- gate_slab: bfloat16 [128, 4096, 384], P(('ep', 'dp')), may hold values from -0.09375 to 0.09375
- up_slab: bfloat16 [128, 4096, 384], P(('ep', 'dp')), may hold values from -0.09375 to 0.09375
- down_slab: bfloat16 [128, 384, 4096], P(('ep', 'dp')), may hold values from -0.21875 to 0.21875
Outputs:
- mixed: float32 [2048, 4096], P(('ep', 'dp'))
The draws below stay inside these ranges and needn't reach their ends.
Inputs may be any that keep to these rules, and one draw needn't show every extreme that they name: `expert_ids`: each row names 8 different experts; among the rows of one device no expert is named by more than 4 rows.
All inputs are finite; a program needn't handle non-finite values.
Results may differ from the reference program's by a relative error of at most 0.009.
Values may be sent and summed in bfloat16 or wider, within the bound.
A program may use at most 128 MiB of HBM per device.

```python
import math
import jax
import jax.numpy as jnp
import numpy as np
from jax import lax

D = 4096
H = 64
KVH = 4
HD = 128
TOP = 8
FF = 768
TOK_DEV = 16
CACHE = 128
EXPERTS = 64
HF = 384
CAP = 4
TOKENS = 2048
N_EP = 32
DEVICES = 128


edge_value = 4.5


def draw_queries(key, part):
    sampled = jnp.clip(jax.random.normal(jax.random.fold_in(key, 1), (TOKENS, H * HD), jnp.float32), -edge_value, edge_value)
    return sampled.astype(jnp.bfloat16)


def draw_cache_keys(key, part):
    sampled = jnp.clip(jax.random.normal(jax.random.fold_in(key, 2), (TOKENS, CACHE, KVH * HD), jnp.float32), -edge_value, edge_value)
    return sampled.astype(jnp.bfloat16)


def draw_router(key, part):
    sampled = jnp.clip(jax.random.normal(jax.random.fold_in(key, 3), (D, EXPERTS), jnp.float32), -4.0, 4.0) / math.sqrt(D)
    return sampled.astype(jnp.bfloat16)


def with_ends(entries, own_key, low, high):
    place = [jax.random.randint(jax.random.fold_in(own_key, axis), (), 0, length) for axis, length in enumerate(entries.shape)]
    main_axis = entries.shape.index(max(entries.shape))
    neighbour = place[:main_axis] + [(place[main_axis] + 1) % entries.shape[main_axis]] + place[main_axis + 1:]
    return entries.at[tuple(place)].set(low).at[tuple(neighbour)].set(high)


def shard_levels(rng, shape, split, least, high):
    loudness, own = 1.0, jax.random.fold_in(rng, 6)
    for axis_at, parts in split:
        steps = jnp.exp(jax.random.uniform(jax.random.fold_in(own, axis_at), (parts,), jnp.float32, least / len(split), high / len(split)))
        loudness = loudness * jnp.repeat(steps, shape[axis_at] // parts).reshape([-1 if axis == axis_at else 1 for axis in range(len(shape))])
    return loudness


def assign_block(rng, own, number, rows, number_of, top, reach, lean):
    order = jax.random.permutation(rng, number_of)
    heavy_load, ordinary = portions_of(number_of, rows * top, reach, lean, True), portions_of(number_of, rows * top, reach, lean, False)
    places = jnp.arange(number_of)

    def named(sizes, offset_by):
        used = int((sizes > 0).sum())
        fixed = max(1, used // 4)
        passed = fixed + (places - fixed + offset_by * (used - fixed)) % max(1, number_of - fixed)
        return jnp.zeros((number_of,), jnp.int32).at[order[jnp.where(places < fixed, places, passed)]].set(jnp.asarray(sizes, jnp.int32))

    sizes = jnp.where(number % 4 == 0, named(heavy_load, number // 4), named(ordinary, number - number // 4 - 1))
    mixed = jax.random.permutation(jax.random.fold_in(own, 3), number_of)
    donor, sink = mixed[0:number_of // 2 * 2:2], mixed[1:number_of // 2 * 2:2]
    margin = jnp.minimum(sizes[donor] - 1, reach - sizes[sink]) // 2
    margin = jnp.where((donor == order[0]) | (sink == order[0]) | (sizes[sink] == 0), 0, jnp.maximum(margin, 0))
    passed = jax.random.randint(jax.random.fold_in(own, 4), (number_of // 2,), 0, 1 << 20) % (margin + 1)
    sizes = sizes.at[donor].add(-passed).at[sink].add(passed)
    labels = jnp.searchsorted(jnp.cumsum(sizes), jnp.arange(rows * top), side="right").astype(jnp.int32)
    listing = labels.reshape(top, rows).T
    listing = listing[jax.random.permutation(jax.random.fold_in(own, 1), rows)]
    offset_by = jax.random.randint(jax.random.fold_in(own, 2), (rows, 1), 0, top)
    return jnp.take_along_axis(listing, (jnp.arange(top)[None, :] + offset_by) % top, axis=1)


def portions_of(count, total, limit, skew, full):
    portions = [(1 << 20) // math.isqrt(rank ** skew) + 1 for rank in range(1, count + 1)]
    largest = limit if full else min(limit, max(-(-total // count), total * portions[0] // sum(portions)))
    least = 1 if total - largest >= count - 1 else 0
    given, spare = [largest] + [least] * (count - 1), total - largest - least * (count - 1)
    while spare > 0:
        movable = [i for i in range(1, count) if given[i] < largest] or [i for i in range(1, count) if given[i] < limit]
        mass, left = sum([portions[i] for i in movable]), spare
        for i in movable:
            addition = min(limit - given[i], max(1, left * portions[i] // mass), spare)
            given[i] = given[i] + addition
            spare = spare - addition
    return np.array(given)


def scatter_about(key, dims, width, reach, cuts=(), held_as=jnp.bfloat16):
    values = width * jax.random.normal(key, dims, jnp.float32)
    if cuts:
        values = values * shard_levels(key, dims, cuts, -0.22, 0.18)
    return jnp.clip(values, -reach, reach).astype(held_as)


def setup_inputs(seed: int = 0) -> dict:
    seeds = jax.random.split(jax.random.key(seed), 15)
    resid = scatter_about(seeds[0], (TOKENS, D), 1.0, 6.0, ((0, 128),))
    queries = draw_queries(jax.random.fold_in(seeds[14], 71), 0)
    new_keys = scatter_about(seeds[2], (TOKENS, KVH * HD), 1.0, 4.5, ((0, 128),))
    new_values = scatter_about(seeds[3], (TOKENS, KVH * HD), 1.0, 6.0, ((0, 128),))
    cache_keys = draw_cache_keys(jax.random.fold_in(seeds[14], 71), 0)
    cache_values = scatter_about(seeds[5], (TOKENS, CACHE, KVH * HD), 1.0, 6.0, ((0, 128),))
    cache_len = with_ends(jax.random.randint(seeds[6], (TOKENS,), 1, CACHE + 1), jax.random.fold_in(seeds[6], 1), 1, CACHE).astype(jnp.int32)
    out_proj = scatter_about(seeds[7], (H * HD, D), (H * HD) ** -0.5, 0.0625, ((0, 32),))
    norm_gain = jnp.clip(1.0 + 0.18 * jax.random.normal(seeds[8], (D,), jnp.float32), 0.1, 1.9)
    router = draw_router(jax.random.fold_in(seeds[14], 71), 0)
    expert_ids_keys = jax.random.split(jax.random.fold_in(seeds[10], 1), TOKENS // TOK_DEV)
    expert_ids_turns = jax.random.permutation(jax.random.fold_in(seeds[10], 3), TOKENS // TOK_DEV)
    expert_ids = jax.vmap(lambda own, number: assign_block(jax.random.fold_in(seeds[10], 2), own, number, TOK_DEV, EXPERTS, TOP, CAP, 2))(expert_ids_keys, expert_ids_turns).reshape((TOKENS, TOP))
    gate_slab = scatter_about(seeds[11], (DEVICES, D, HF), D ** -0.5, 0.09375, ((0, 128),))
    up_slab = scatter_about(seeds[12], (DEVICES, D, HF), D ** -0.5, 0.09375, ((0, 128),))
    down_slab = scatter_about(seeds[13], (DEVICES, HF, D), FF ** -0.5, 0.21875, ((0, 128),))
    return {"resid": resid, "queries": queries, "new_keys": new_keys, "new_values": new_values, "cache_keys": cache_keys, "cache_values": cache_values, "cache_len": cache_len, "out_proj": out_proj, "norm_gain": norm_gain, "router": router, "expert_ids": expert_ids, "gate_slab": gate_slab, "up_slab": up_slab, "down_slab": down_slab}


def attend_block(query_rows, key_new, value_new, key_cache, value_cache, lengths):
    local_rows = query_rows.shape[0]
    cache_span = key_cache.shape[1]
    group_size = H // KVH
    query_heads = query_rows.astype(jnp.float32).reshape(local_rows, KVH, group_size, HD)
    past_keys = key_cache.astype(jnp.float32).reshape(local_rows, cache_span, KVH, HD)
    past_values = value_cache.astype(jnp.float32).reshape(local_rows, cache_span, KVH, HD)
    score_scale = 1.0 / math.sqrt(HD)
    past_scores = jnp.einsum('tgqd,tcgd->tgqc', query_heads, past_keys) * score_scale
    own_scores = jnp.einsum('tgqd,tgd->tgq', query_heads, key_new.astype(jnp.float32).reshape(local_rows, KVH, HD)) * score_scale
    is_valid = lax.broadcasted_iota(jnp.int32, (local_rows, cache_span), 1) < lengths[:, None]
    past_scores = jnp.where(is_valid[:, None, None, :], past_scores, -1e+30)
    peak_score = jnp.maximum(lax.optimization_barrier(jnp.max(past_scores, axis=3)), own_scores)
    past_exp = jnp.exp(past_scores - peak_score[..., None])
    own_exp = jnp.exp(own_scores - peak_score)
    denom_sum = lax.optimization_barrier(jnp.sum(past_exp, axis=3)) + own_exp
    past_weights = lax.optimization_barrier((past_exp / denom_sum[..., None]).astype(jnp.bfloat16))
    own_weights = lax.optimization_barrier((own_exp / denom_sum).astype(jnp.bfloat16))
    blended = jnp.einsum('tgqc,tcgd->tgqd', past_weights.astype(jnp.float32), past_values)
    blended = blended + own_weights.astype(jnp.float32)[..., None] * value_new.astype(jnp.float32).reshape(local_rows, KVH, 1, HD)
    return blended.reshape(local_rows, H * HD).astype(jnp.bfloat16)

def attend_packed(packed):
    return attend_block(*packed)

def blocked(array):
    return array.reshape((DEVICES, TOK_DEV) + array.shape[1:])

def reference(resid, queries, new_keys, new_values, cache_keys, cache_values, cache_len, out_proj, norm_gain, router, expert_ids, gate_slab, up_slab, down_slab):
    packed = (blocked(queries), blocked(new_keys), blocked(new_values), blocked(cache_keys), blocked(cache_values), blocked(cache_len))
    attended = lax.map(attend_packed, packed).reshape(TOKENS, H * HD)
    column_width = H * HD // N_EP
    attn_out = jnp.zeros((TOKENS, D), jnp.float32)
    for shard_index in range(N_EP):
        row_start = shard_index * column_width
        product = jnp.dot(attended[:, row_start:row_start + column_width], out_proj[row_start:row_start + column_width], preferred_element_type=jnp.float32)
        rounded = lax.optimization_barrier(product.astype(jnp.bfloat16))
        attn_out = attn_out + rounded.astype(jnp.float32)
    hidden = resid.astype(jnp.float32) + attn_out
    meansq = lax.optimization_barrier(jnp.mean(hidden * hidden, axis=1, keepdims=True))
    normed = (hidden * lax.rsqrt(jnp.maximum(meansq, 0.25)) * norm_gain).astype(jnp.bfloat16)
    logits = jnp.dot(normed, router, preferred_element_type=jnp.float32)
    chosen = jnp.take_along_axis(logits, expert_ids.astype(jnp.int32), axis=1)
    peak_logit = lax.optimization_barrier(jnp.max(chosen, axis=1, keepdims=True))
    exp_logit = jnp.exp(chosen - peak_logit)
    gate_probs = lax.optimization_barrier((exp_logit / lax.optimization_barrier(jnp.sum(exp_logit, axis=1, keepdims=True))).astype(jnp.bfloat16))
    flat_ids = expert_ids.reshape(-1).astype(jnp.int32)
    token_of = (jnp.arange(TOKENS * TOP, dtype=jnp.int32) // TOP).astype(jnp.int32)
    onehot = (flat_ids[:, None] == jnp.arange(EXPERTS, dtype=jnp.int32)[None, :]).astype(jnp.int32)
    earlier = jnp.cumsum(onehot, axis=0).astype(jnp.int32) - onehot
    ranking = lax.optimization_barrier(jnp.sum(earlier * onehot, axis=1)).astype(jnp.int32)
    row_depth = DEVICES * CAP
    row_table = jnp.zeros((EXPERTS, row_depth), jnp.int32).at[flat_ids, ranking].set(token_of)

    def run_expert(expert):
        rows_in = jnp.take(normed, row_table[expert], axis=0)
        gate_full = jnp.concatenate((gate_slab[2 * expert], gate_slab[2 * expert + 1]), axis=1)
        up_full = jnp.concatenate((up_slab[2 * expert], up_slab[2 * expert + 1]), axis=1)
        down_full = jnp.concatenate((down_slab[2 * expert], down_slab[2 * expert + 1]), axis=0)
        gate_val = jnp.dot(rows_in, gate_full, preferred_element_type=jnp.float32)
        up_val = jnp.dot(rows_in, up_full, preferred_element_type=jnp.float32)
        activated = (jax.nn.silu(gate_val) * up_val).astype(jnp.bfloat16)
        return jnp.dot(activated, down_full, preferred_element_type=jnp.float32).astype(jnp.bfloat16)
    produced = lax.map(run_expert, jnp.arange(EXPERTS, dtype=jnp.int32))
    picked = produced[flat_ids, ranking].reshape(TOKENS, TOP, D)
    expert_mix = jnp.einsum('tk,tkd->td', gate_probs.astype(jnp.float32), picked.astype(jnp.float32))
    return hidden + expert_mix
```

```python
import functools
import math

import jax
import jax.numpy as jnp
from jax import lax
from jax.experimental import pallas as pl
from jax.experimental.pallas import tpu as pltpu
from jax.sharding import PartitionSpec as P

D = 4096
H = 64
KVH = 4
HD = 128
TOP = 8
MESH = pl.DeviceIdType.MESH

PART = 1408
ORDER = (("x", "y", "z"), ("y", "z", "x"), ("z", "x", "y"))
HF = 384


def attend(queries, new_keys, new_values, cache_keys, cache_values, cache_len):
    local_rows = queries.shape[0]
    cache_span = cache_keys.shape[1]
    group_size = H // KVH
    query_heads = queries.reshape(local_rows, KVH, group_size, HD)
    past_keys = cache_keys.reshape(local_rows, cache_span, KVH, HD)
    past_values = cache_values.reshape(local_rows, cache_span, KVH, HD)
    score_scale = 1.0 / math.sqrt(HD)
    past_scores = (
        jnp.einsum("tgqd,tcgd->tgqc", query_heads, past_keys, preferred_element_type=jnp.float32)
        * score_scale
    )
    own_scores = (
        jnp.einsum(
            "tgqd,tgd->tgq",
            query_heads,
            new_keys.reshape(local_rows, KVH, HD),
            preferred_element_type=jnp.float32,
        )
        * score_scale
    )
    is_valid = lax.broadcasted_iota(jnp.int32, (local_rows, cache_span), 1) < cache_len[:, None]
    past_scores = jnp.where(is_valid[:, None, None, :], past_scores, -1e30)
    peak_score = jnp.maximum(jnp.max(past_scores, axis=3), own_scores)
    past_exp = jnp.exp(past_scores - peak_score[..., None])
    own_exp = jnp.exp(own_scores - peak_score)
    denom_sum = jnp.sum(past_exp, axis=3) + own_exp
    past_weights = (past_exp / denom_sum[..., None]).astype(jnp.bfloat16)
    own_weights = (own_exp / denom_sum).astype(jnp.bfloat16)
    blended = jnp.einsum(
        "tgqc,tcgd->tgqd", past_weights, past_values, preferred_element_type=jnp.float32
    )
    blended = blended + own_weights.astype(jnp.float32)[..., None] * new_values.reshape(
        local_rows, KVH, 1, HD
    ).astype(jnp.float32)
    return blended.reshape(local_rows, H * HD).astype(jnp.bfloat16)


class Place:
    def __init__(self):
        ep = lax.axis_index("ep")
        self.c = lax.rem(ep, 2)
        self.coord = {
            "x": lax.rem(lax.div(ep, 2), 4),
            "y": lax.div(ep, 8),
            "z": lax.axis_index("dp"),
        }

    def rel(self, dim, offset):
        if isinstance(offset, int) and offset == 0:
            return self.coord[dim]
        return lax.rem(self.coord[dim] + offset, 4)

    def device(self, dim=None, offset=0, other_core=False):
        at = dict(self.coord)
        if dim is not None:
            at[dim] = self.rel(dim, offset)
        core = 1 - self.c if other_core else self.c
        return ((at["y"] * 4 + at["x"]) * 2 + core, at["z"])


class Names:
    def __init__(self):
        self.table = {}

    def __call__(self, *key):
        return self.table.setdefault(key, len(self.table))


SENDS = 260


def moe_kernel(
    x_in, gate, up, down, out,
    rows, gu, dn, acc, act, part, pair_out, pair_in, ra1, ra2, rb1, rb2, rc1, rc2,
    send_sem, recv_sem, load_sem,
):
    here = Place()
    c = here.c
    other = 1 - c
    rel, device = here.rel, here.device
    ahead = 1 + 2 * c
    behind = 3 - 2 * c
    names = Names()
    pending = {}

    def send(src, dst, key, dev):
        i = names(*key)
        copy = pltpu.make_async_remote_copy(
            src_ref=src, dst_ref=dst, send_sem=send_sem.at[i], recv_sem=recv_sem.at[i],
            device_id=dev, device_id_type=MESH,
        )
        copy.start()
        pending[key] = copy

    def landed(dst, key):
        i = names(*key)
        pltpu.make_async_remote_copy(
            src_ref=dst, dst_ref=dst, send_sem=send_sem.at[i], recv_sem=recv_sem.at[i],
            device_id=device(other_core=True), device_id_type=MESH,
        ).wait_recv()

    def where(p, o1, o2, o3):
        at = {d: (slice(None) if o is None else rel(d, o)) for d, o in zip(ORDER[p], (o1, o2, o3))}
        return at["y"], at["x"], at["z"]

    def block(p, o1, o2, o3, core=None):
        return rows.at[(p, c if core is None else core) + where(p, o1, o2, o3)]

    barrier = pltpu.get_barrier_semaphore()
    for dim in ("x", "y", "z"):
        for o in (1, 3):
            pl.semaphore_signal(barrier, inc=1, device_id=device(dim, o), device_id_type=MESH)
    pl.semaphore_signal(barrier, inc=1, device_id=device(other_core=True), device_id_type=MESH)

    loads = [
        pltpu.make_async_copy(gate, gu.at[pl.ds(0, D), pl.ds(0, HF)], load_sem.at[0]),
        pltpu.make_async_copy(up, gu.at[pl.ds(0, D), pl.ds(HF, HF)], load_sem.at[1]),
        pltpu.make_async_copy(down, dn.at[:, pl.ds(0, D)], load_sem.at[2]),
    ]
    for copy in loads:
        copy.start()
    mine = [x_in.at[:, pl.ds(p * PART, PART)] for p in range(3)]
    for p in range(3):
        rows[(p, c) + where(p, 0, 0, 0)] = x_in[:, p * PART : (p + 1) * PART]
    pl.semaphore_wait(barrier, 7)

    parts = range(3)
    dims = ORDER
    for p in parts:
        own = block(p, 0, 0, 0)
        send(mine[p], own, (p, "1f"), device(dims[p][0], ahead))
        send(mine[p], own, (p, "1b"), device(dims[p][0], behind))
    for p in parts:
        own = block(p, 0, 0, 0)
        send(mine[p], own, (p, "2+", 0), device(dims[p][1], 1))
        send(mine[p], own, (p, "2-", 0), device(dims[p][1], 3))

    gu[D:, :] = jnp.zeros((3 * PART - D, 2 * HF), jnp.bfloat16)
    dn[:, D:] = jnp.zeros((HF, 3 * PART - D), jnp.bfloat16)

    @pl.loop(0, 32)
    def _(i):
        acc[i // 16, lax.rem(i, 16) // 4, lax.rem(i, 4)] = jnp.zeros((4, 16, 2 * HF), jnp.float32)

    def send_sub(p, j):
        ref = block(p, j, 0, 0)
        send(ref, ref, (p, "2+", j), device(dims[p][1], 1))
        send(ref, ref, (p, "2-", j), device(dims[p][1], 3))

    def send_line(p, j):
        ref = block(p, None, j, 0)
        send(ref, ref, (p, "3+", j), device(dims[p][2], 1))
        send(ref, ref, (p, "3-", j), device(dims[p][2], 3))

    def pass_on(p, o2, o3):
        ref = block(p, None, o2, o3)
        send(ref, ref, (p, "pair", o2, o3), device(other_core=True))

    for p in parts:
        ref = block(p, behind, 0, 0)
        landed(ref, (p, "1f"))
        send(ref, ref, (p, "1g"), device(dims[p][0], ahead))
        landed(block(p, ahead, 0, 0), (p, "1b"))
        send_sub(p, 1)
        send_sub(p, 3)
    for p in parts:
        landed(block(p, 2, 0, 0), (p, "1g"))
        send_sub(p, 2)
        send_line(p, 0)
        pass_on(p, 0, 0)
    for j in (0, 1, 3, 2):
        for p in parts:
            ref = block(p, j, 3, 0)
            landed(ref, (p, "2+", j))
            if j in (0, 1):
                send(ref, ref, (p, "2g", j), device(dims[p][1], 1))
            ref = block(p, j, 1, 0)
            landed(ref, (p, "2-", j))
            if j in (3, 2):
                send(ref, ref, (p, "2g", j), device(dims[p][1], 3))
    for p in parts:
        send_line(p, 1)
        send_line(p, 3)
        pass_on(p, 1, 0)
        pass_on(p, 3, 0)
    for copy in loads:
        copy.wait()
    for p in parts:
        for j in (0, 1, 3, 2):
            landed(block(p, j, 2, 0), (p, "2g", j))
        send_line(p, 2)
        pass_on(p, 2, 0)

    def project(p, o2, o3):
        landed(block(p, None, o2, o3, other), (p, "pair", o2, o3))
        at = where(p, None, o2, o3)

        @pl.loop(0, 3)
        def _(n):
            cols = pl.ds(pl.multiple_of(n * 256, 256), 256)
            x = rows[(p, slice(None)) + at].reshape(128, PART)
            y = jnp.dot(x, gu[p * PART : (p + 1) * PART, cols], preferred_element_type=jnp.float32)
            idx = (slice(None),) + at + (slice(None), cols)
            acc[idx] += y.reshape(2, 4, 16, 256)

    seen = None
    for j in (0, 1, 3, 2):
        for p in parts:
            project(p, j, 0)
        for p in parts:
            ref = block(p, None, j, 3)
            landed(ref, (p, "3+", j))
            if j in (0, 1):
                send(ref, ref, (p, "3g", j), device(dims[p][2], 1))
            ref = block(p, None, j, 1)
            landed(ref, (p, "3-", j))
            if j in (3, 2):
                send(ref, ref, (p, "3g", j), device(dims[p][2], 3))
            pass_on(p, j, 3)
            pass_on(p, j, 1)
        if seen is not None:
            for p in parts:
                project(p, seen, 3)
                project(p, seen, 1)
        seen = j
    for p in parts:
        project(p, seen, 3)
        project(p, seen, 1)
    for j in (0, 3, 1, 2):
        for p in parts:
            landed(block(p, None, j, 2), (p, "3g", j))
            pass_on(p, j, 2)
    for j in (0, 3, 1, 2):
        for p in parts:
            project(p, j, 2)

    expert = lax.div(lax.axis_index("ep") * 4 + lax.axis_index("dp"), 2)

    @pl.loop(0, 32)
    def _(i):
        at = (i // 16, lax.rem(i, 16) // 4, lax.rem(i, 4))
        sums = acc[at].reshape(64, 2 * HF)
        tail = rows[(2,) + at + (slice(None), slice(None), slice(PART - 128, PART))]
        tail = tail.reshape(64, 128).astype(jnp.float32)
        lanes = lax.broadcasted_iota(jnp.int32, (64, 128), 1)
        prob = jnp.sum(jnp.where(lanes == expert, tail, 0.0), axis=1, keepdims=True)
        g, u = sums[:, :HF], sums[:, HF:]
        h = (g / (1.0 + jnp.exp(-g)) * u).astype(jnp.bfloat16).astype(jnp.float32) * prob
        act[at] = h.astype(jnp.bfloat16).reshape(4, 16, HF)

    def spot(p, o2, o3):
        a2 = slice(None) if o2 is None else rel(dims[p][1], o2)
        a3 = slice(None) if o3 is None else rel(dims[p][0], o3)
        return (a3, a2) if p == 1 else (a2, a3)

    def line(p, o1, o2):
        return part.at[(p, o1) + spot(p, o2, None)]

    def sub(p, o3):
        return part.at[(p, 0) + spot(p, 0, o3)]

    def hidden_of(p, o1, core):
        at = {d: (rel(d, o1) if d == dims[p][2] else slice(None)) for d in "xyz"}
        return act[core, at["y"], at["x"], at["z"]].reshape(256, HF)

    def product(p, o1, core, dst):
        @pl.loop(0, 5)
        def _(n):
            cols = pl.ds(pl.multiple_of(n * 256, 256), 256)
            wcols = pl.ds(pl.multiple_of(p * PART + n * 256, 128), 256)
            y = jnp.dot(hidden_of(p, o1, core), dn[:, wcols], preferred_element_type=jnp.float32)
            dst[:, :, :, cols] = y.astype(jnp.bfloat16).reshape(4, 4, 16, 256)

        if p < 2:
            y = jnp.dot(hidden_of(p, o1, core), dn[:, p * PART + 1280 : (p + 1) * PART], preferred_element_type=jnp.float32)
            dst[:, :, :, 1280:] = y.astype(jnp.bfloat16).reshape(4, 4, 16, 128)
        else:
            dst[:, :, :, 1280:] = jnp.zeros((4, 4, 16, 128), jnp.bfloat16)

    def add(dst, *srcs):
        @pl.loop(0, 4)
        def _(i):
            total = dst[i].astype(jnp.float32)
            for s in srcs:
                total += s[i].astype(jnp.float32)
            dst[i] = total.astype(jnp.bfloat16)

    def add_sub(dst, *srcs):
        total = dst[...].astype(jnp.float32)
        for s in srcs:
            total += s[...].astype(jnp.float32)
        dst[...] = total.astype(jnp.bfloat16)

    waited = set()

    def sums_for(o1):
        for p in parts:
            for key in list(pending):
                if key[:2] == (p, "sum") and key not in waited:
                    pending[key].wait_send()
                    waited.add(key)
            product(p, o1, other, pair_out.at[p])
            send(pair_out.at[p], pair_in.at[p, o1], (p, "sum", o1), device(other_core=True))
        for p in parts:
            product(p, o1, c, part.at[p, o1])
        for p in parts:
            landed(pair_in.at[p, o1], (p, "sum", o1))
            @pl.loop(0, 4)
            def _(i):
                add(part.at[p, o1, i], pair_in.at[p, o1, i])

    def up_of(p, level):
        return device(dims[p][level], 1)

    def down_of(p, level):
        return device(dims[p][level], 3)

    UPWARD, DOWNWARD = (2, 1), (3, 0)

    sums_for(2)
    for k in range(2):
        for p in parts:
            send(line(p, 2, UPWARD[k]), ra1.at[p, 0, k], (p, "a1+", k), up_of(p, 2))
            send(line(p, 2, DOWNWARD[k]), ra1.at[p, 1, k], (p, "a1-", k), down_of(p, 2))
    sums_for(1)
    for j in DOWNWARD:
        for p in parts:
            send(line(p, 1, j), ra2.at[p, 0, j], (p, "a2+", j), up_of(p, 2))
    sums_for(3)
    for j in UPWARD:
        for p in parts:
            send(line(p, 3, j), ra2.at[p, 1, j], (p, "a2-", j), down_of(p, 2))
    for k in range(2):
        for p in parts:
            j = UPWARD[k]
            landed(ra1.at[p, 0, k], (p, "a1+", k))
            add(line(p, 1, j), ra1.at[p, 0, k])
            send(line(p, 1, j), ra2.at[p, 0, j], (p, "a2+", j), up_of(p, 2))
            j = DOWNWARD[k]
            landed(ra1.at[p, 1, k], (p, "a1-", k))
            add(line(p, 3, j), ra1.at[p, 1, k])
            send(line(p, 3, j), ra2.at[p, 1, j], (p, "a2-", j), down_of(p, 2))
    sums_for(0)

    def finish_line(p, j):
        landed(ra2.at[p, 0, j], (p, "a2+", j))
        landed(ra2.at[p, 1, j], (p, "a2-", j))
        add(line(p, 0, j), ra2.at[p, 0, j], ra2.at[p, 1, j])

    def block_of(p, o2, o3):
        return part.at[(p, 0) + spot(p, o2, o3)]

    for p in parts:
        finish_line(p, 2)
        for k in range(2):
            send(block_of(p, 2, UPWARD[k]), rb1.at[p, 0, k], (p, "b1+", k), up_of(p, 1))
            send(block_of(p, 2, DOWNWARD[k]), rb1.at[p, 1, k], (p, "b1-", k), down_of(p, 1))
    for p in parts:
        finish_line(p, 3)
        for j in UPWARD:
            send(block_of(p, 3, j), rb2.at[p, 1, j], (p, "b2-", j), down_of(p, 1))
    for p in parts:
        finish_line(p, 1)
        for j in DOWNWARD:
            send(block_of(p, 1, j), rb2.at[p, 0, j], (p, "b2+", j), up_of(p, 1))
    for k in range(2):
        for p in parts:
            j = UPWARD[k]
            landed(rb1.at[p, 0, k], (p, "b1+", k))
            add_sub(block_of(p, 1, j), rb1.at[p, 0, k])
            send(block_of(p, 1, j), rb2.at[p, 0, j], (p, "b2+", j), up_of(p, 1))
            j = DOWNWARD[k]
            landed(rb1.at[p, 1, k], (p, "b1-", k))
            add_sub(block_of(p, 3, j), rb1.at[p, 1, k])
            send(block_of(p, 3, j), rb2.at[p, 1, j], (p, "b2-", j), down_of(p, 1))
    for p in parts:
        finish_line(p, 0)

    def finish_block(p, j):
        landed(rb2.at[p, 0, j], (p, "b2+", j))
        landed(rb2.at[p, 1, j], (p, "b2-", j))
        add_sub(sub(p, j), rb2.at[p, 0, j], rb2.at[p, 1, j])

    for p in parts:
        finish_block(p, 2)
        send(sub(p, 2), rc1.at[p], (p, "c1"), device(dims[p][0], ahead))
    for p in parts:
        finish_block(p, 3)
        finish_block(p, 1)
        send(sub(p, behind), rc2.at[p, 0], (p, "c2"), device(dims[p][0], behind))
    for p in parts:
        landed(rc1.at[p], (p, "c1"))
        add_sub(sub(p, ahead), rc1.at[p])
        send(sub(p, ahead), rc2.at[p, 1], (p, "c3"), device(dims[p][0], ahead))
    for p in parts:
        finish_block(p, 0)
    for p in parts:
        landed(rc2.at[p, 0], (p, "c2"))
        landed(rc2.at[p, 1], (p, "c3"))
        total = (
            sub(p, 0)[...].astype(jnp.float32)
            + rc2[p, 0].astype(jnp.float32)
            + rc2[p, 1].astype(jnp.float32)
        )
        width = min(PART, D - p * PART)
        out[:, p * PART : p * PART + width] = total[:, :width]
    for key, copy in pending.items():
        if key not in waited:
            copy.wait_send()
    assert len(names.table) <= SENDS, len(names.table)


def moe(x_in, gate, up, down):
    bf = jnp.bfloat16
    vmem = pl.BlockSpec(memory_space=pltpu.VMEM)
    hbm = pl.BlockSpec(memory_space=pl.ANY)
    return pl.pallas_call(
        moe_kernel,
        out_shape=jax.ShapeDtypeStruct((16, D), jnp.float32),
        in_specs=[vmem, hbm, hbm, hbm],
        out_specs=vmem,
        scratch_shapes=[
            pltpu.VMEM((3, 2, 4, 4, 4, 16, PART), bf),
            pltpu.VMEM((3 * PART, 2 * HF), bf),
            pltpu.VMEM((HF, 3 * PART), bf),
            pltpu.VMEM((2, 4, 4, 4, 16, 2 * HF), jnp.float32),
            pltpu.VMEM((2, 4, 4, 4, 16, HF), bf),
            pltpu.VMEM((3, 4, 4, 4, 16, PART), bf),
            pltpu.VMEM((3, 4, 4, 16, PART), bf),
            pltpu.VMEM((3, 4, 4, 4, 16, PART), bf),
            pltpu.VMEM((3, 2, 2, 4, 16, PART), bf),
            pltpu.VMEM((3, 2, 4, 4, 16, PART), bf),
            pltpu.VMEM((3, 2, 2, 16, PART), bf),
            pltpu.VMEM((3, 2, 4, 16, PART), bf),
            pltpu.VMEM((3, 16, PART), bf),
            pltpu.VMEM((3, 2, 16, PART), bf),
            pltpu.SemaphoreType.DMA((SENDS,)),
            pltpu.SemaphoreType.DMA((SENDS,)),
            pltpu.SemaphoreType.DMA((3,)),
        ],
        compiler_params=pltpu.CompilerParams(
            collective_id=0, has_side_effects=True, vmem_limit_bytes=67043328
        ),
        name="moe",
    )(x_in, gate, up, down)


def local(
    resid,
    queries,
    new_keys,
    new_values,
    cache_keys,
    cache_values,
    cache_len,
    out_proj,
    norm_gain,
    router,
    expert_ids,
    gate_slab,
    up_slab,
    down_slab,
):
    attended = attend(queries, new_keys, new_values, cache_keys, cache_values, cache_len)
    regrouped = lax.all_to_all(attended, "ep", split_axis=1, concat_axis=0, tiled=True)
    attn_out = lax.psum_scatter(
        jnp.dot(regrouped, out_proj, preferred_element_type=jnp.float32).astype(jnp.bfloat16),
        "ep",
        scatter_dimension=0,
        tiled=True,
    ).astype(jnp.float32)
    hidden = resid.astype(jnp.float32) + attn_out
    meansq = jnp.mean(hidden * hidden, axis=1, keepdims=True)
    normed = (hidden * lax.rsqrt(jnp.maximum(meansq, 0.25)) * norm_gain).astype(jnp.bfloat16)
    logits = jnp.dot(normed, router, preferred_element_type=jnp.float32)
    experts = router.shape[1]
    labels = jnp.arange(experts, dtype=jnp.int32)
    onehot = expert_ids[:, :, None] == labels[None, None, :]
    chosen = jnp.sum(jnp.where(onehot, logits[:, None, :], 0.0), axis=2)
    peak_logit = jnp.max(chosen, axis=1, keepdims=True)
    exp_logit = jnp.exp(chosen - peak_logit)
    gate_probs = (exp_logit / jnp.sum(exp_logit, axis=1, keepdims=True)).astype(jnp.bfloat16)
    weights = jnp.sum(jnp.where(onehot, gate_probs.astype(jnp.float32)[:, :, None], 0.0), axis=1)
    weights = jnp.pad(weights.astype(jnp.bfloat16), ((0, 0), (0, 3 * PART - D - experts)))
    x_in = jnp.concatenate([normed, weights], axis=1)
    return hidden + moe(x_in, gate_slab[0], up_slab[0], down_slab[0])


def solution(mesh):
    in_specs = (
        P(("ep", "dp"), None),
        P(("ep", "dp"), None),
        P(("ep", "dp"), None),
        P(("ep", "dp"), None),
        P(("ep", "dp"), None, None),
        P(("ep", "dp"), None, None),
        P(("ep", "dp")),
        P("ep", None),
        P(),
        P(),
        P(("ep", "dp"), None),
        P(("ep", "dp"), None, None),
        P(("ep", "dp"), None, None),
        P(("ep", "dp"), None, None),
    )
    out_specs = P(("ep", "dp"), None)
    return jax.shard_map(local, mesh=mesh, in_specs=in_specs, out_specs=out_specs, check_vma=False)
```

```python
import functools
import math

import jax
import jax.numpy as jnp
from jax import lax
from jax.experimental import pallas as pl
from jax.experimental.pallas import tpu as pltpu
from jax.sharding import PartitionSpec as P

D = 4096
H = 64
KVH = 4
HD = 128
TOP = 8
MESH = pl.DeviceIdType.MESH

PART = 1408
ORDER = (("x", "y", "z"), ("y", "z", "x"), ("z", "x", "y"))
HF = 384


def attend(queries, new_keys, new_values, cache_keys, cache_values, cache_len):
    local_rows = queries.shape[0]
    cache_span = cache_keys.shape[1]
    group_size = H // KVH
    query_heads = queries.reshape(local_rows, KVH, group_size, HD)
    past_keys = cache_keys.reshape(local_rows, cache_span, KVH, HD)
    past_values = cache_values.reshape(local_rows, cache_span, KVH, HD)
    score_scale = 1.0 / math.sqrt(HD)
    past_scores = (
        jnp.einsum("tgqd,tcgd->tgqc", query_heads, past_keys, preferred_element_type=jnp.float32)
        * score_scale
    )
    own_scores = (
        jnp.einsum(
            "tgqd,tgd->tgq",
            query_heads,
            new_keys.reshape(local_rows, KVH, HD),
            preferred_element_type=jnp.float32,
        )
        * score_scale
    )
    is_valid = lax.broadcasted_iota(jnp.int32, (local_rows, cache_span), 1) < cache_len[:, None]
    past_scores = jnp.where(is_valid[:, None, None, :], past_scores, -1e30)
    peak_score = jnp.maximum(jnp.max(past_scores, axis=3), own_scores)
    past_exp = jnp.exp(past_scores - peak_score[..., None])
    own_exp = jnp.exp(own_scores - peak_score)
    denom_sum = jnp.sum(past_exp, axis=3) + own_exp
    past_weights = (past_exp / denom_sum[..., None]).astype(jnp.bfloat16)
    own_weights = (own_exp / denom_sum).astype(jnp.bfloat16)
    blended = jnp.einsum(
        "tgqc,tcgd->tgqd", past_weights, past_values, preferred_element_type=jnp.float32
    )
    blended = blended + own_weights.astype(jnp.float32)[..., None] * new_values.reshape(
        local_rows, KVH, 1, HD
    ).astype(jnp.float32)
    return blended.reshape(local_rows, H * HD).astype(jnp.bfloat16)


class Place:
    def __init__(self):
        ep = lax.axis_index("ep")
        self.c = lax.rem(ep, 2)
        self.coord = {
            "x": lax.rem(lax.div(ep, 2), 4),
            "y": lax.div(ep, 8),
            "z": lax.axis_index("dp"),
        }

    def rel(self, dim, offset):
        if isinstance(offset, int) and offset == 0:
            return self.coord[dim]
        return lax.rem(self.coord[dim] + offset, 4)

    def device(self, dim=None, offset=0, other_core=False):
        at = dict(self.coord)
        if dim is not None:
            at[dim] = self.rel(dim, offset)
        core = 1 - self.c if other_core else self.c
        return ((at["y"] * 4 + at["x"]) * 2 + core, at["z"])


class Names:
    def __init__(self):
        self.table = {}

    def __call__(self, *key):
        return self.table.setdefault(key, len(self.table))


SENDS = 260


def moe_kernel(
    x_in, gate, up, down, out,
    rows, gu, dn, acc, act, part, pair_out, pair_in, ra1, ra2, rb1, rb2, rc,
    send_sem, recv_sem, load_sem,
):
    here = Place()
    c = here.c
    other = 1 - c
    rel, device = here.rel, here.device
    names = Names()
    pending = {}

    def send(src, dst, key, dev):
        i = names(*key)
        copy = pltpu.make_async_remote_copy(
            src_ref=src, dst_ref=dst, send_sem=send_sem.at[i], recv_sem=recv_sem.at[i],
            device_id=dev, device_id_type=MESH,
        )
        copy.start()
        pending[key] = copy

    def landed(dst, key):
        i = names(*key)
        pltpu.make_async_remote_copy(
            src_ref=dst, dst_ref=dst, send_sem=send_sem.at[i], recv_sem=recv_sem.at[i],
            device_id=device(other_core=True), device_id_type=MESH,
        ).wait_recv()

    def where(p, o1, o2, o3):
        at = {d: (slice(None) if o is None else rel(d, o)) for d, o in zip(ORDER[p], (o1, o2, o3))}
        return at["y"], at["x"], at["z"]

    def block(p, o1, o2, o3, core=None):
        return rows.at[(p, c if core is None else core) + where(p, o1, o2, o3)]

    barrier = pltpu.get_barrier_semaphore()
    for dim in ("x", "y", "z"):
        for o in (1, 2, 3):
            pl.semaphore_signal(barrier, inc=1, device_id=device(dim, o), device_id_type=MESH)
    pl.semaphore_signal(barrier, inc=1, device_id=device(other_core=True), device_id_type=MESH)

    loads = [
        pltpu.make_async_copy(gate, gu.at[pl.ds(0, D), pl.ds(0, HF)], load_sem.at[0]),
        pltpu.make_async_copy(up, gu.at[pl.ds(0, D), pl.ds(HF, HF)], load_sem.at[1]),
        pltpu.make_async_copy(down, dn.at[:, pl.ds(0, D)], load_sem.at[2]),
    ]
    for copy in loads:
        copy.start()
    mine = [x_in.at[:, pl.ds(p * PART, PART)] for p in range(3)]
    for p in range(3):
        rows[(p, c) + where(p, 0, 0, 0)] = x_in[:, p * PART : (p + 1) * PART]
    pl.semaphore_wait(barrier, 10)

    parts = range(3)
    dims = ORDER
    for p in parts:
        own = block(p, 0, 0, 0)
        for o in (1, 3, 2):
            send(mine[p], own, (p, "1", o), device(dims[p][0], o))
    for p in parts:
        own = block(p, 0, 0, 0)
        send(mine[p], own, (p, "2+", 0), device(dims[p][1], 1))
        send(mine[p], own, (p, "2-", 0), device(dims[p][1], 3))

    gu[D:, :] = jnp.zeros((3 * PART - D, 2 * HF), jnp.bfloat16)
    dn[:, D:] = jnp.zeros((HF, 3 * PART - D), jnp.bfloat16)

    @pl.loop(0, 32)
    def _(i):
        acc[i // 16, lax.rem(i, 16) // 4, lax.rem(i, 4)] = jnp.zeros((4, 16, 2 * HF), jnp.float32)

    def send_sub(p, j):
        ref = block(p, j, 0, 0)
        send(ref, ref, (p, "2+", j), device(dims[p][1], 1))
        send(ref, ref, (p, "2-", j), device(dims[p][1], 3))

    def send_line(p, j):
        ref = block(p, None, j, 0)
        send(ref, ref, (p, "3+", j), device(dims[p][2], 1))
        send(ref, ref, (p, "3-", j), device(dims[p][2], 3))

    def pass_on(p, o2, o3):
        ref = block(p, None, o2, o3)
        send(ref, ref, (p, "pair", o2, o3), device(other_core=True))

    for p in parts:
        for o in (1, 3):
            landed(block(p, 4 - o, 0, 0), (p, "1", o))
        send_sub(p, 1)
        send_sub(p, 3)
    for p in parts:
        landed(block(p, 2, 0, 0), (p, "1", 2))
        send_sub(p, 2)
        send_line(p, 0)
        pass_on(p, 0, 0)
    for j in (0, 1, 3, 2):
        for p in parts:
            ref = block(p, j, 3, 0)
            landed(ref, (p, "2+", j))
            if j in (0, 1):
                send(ref, ref, (p, "2g", j), device(dims[p][1], 1))
            ref = block(p, j, 1, 0)
            landed(ref, (p, "2-", j))
            if j in (3, 2):
                send(ref, ref, (p, "2g", j), device(dims[p][1], 3))
    for p in parts:
        send_line(p, 1)
        send_line(p, 3)
        pass_on(p, 1, 0)
        pass_on(p, 3, 0)
    for copy in loads:
        copy.wait()
    for p in parts:
        for j in (0, 1, 3, 2):
            landed(block(p, j, 2, 0), (p, "2g", j))
        send_line(p, 2)
        pass_on(p, 2, 0)

    def project(*lines):
        for p in parts:
            for o2, o3 in lines:
                landed(block(p, None, o2, o3, other), (p, "pair", o2, o3))
            at = [where(p, None, o2, o3) for o2, o3 in lines]

            @pl.loop(0, 3)
            def _(n):
                cols = pl.ds(pl.multiple_of(n * 256, 256), 256)
                x = [rows[(p, slice(None)) + a].reshape(128, PART) for a in at]
                x = jnp.concatenate(x, axis=0)
                w = gu[p * PART : (p + 1) * PART, cols]
                y = jnp.dot(x, w, preferred_element_type=jnp.float32)
                for i, a in enumerate(at):
                    idx = (slice(None),) + a + (slice(None), cols)
                    acc[idx] += y[i * 128 : (i + 1) * 128].reshape(2, 4, 16, 256)

    def neighbours(j):
        for p in parts:
            ref = block(p, None, j, 3)
            landed(ref, (p, "3+", j))
            if j in (0, 3):
                send(ref, ref, (p, "3g", j), device(dims[p][2], 1))
            ref = block(p, None, j, 1)
            landed(ref, (p, "3-", j))
            if j in (1, 2):
                send(ref, ref, (p, "3g", j), device(dims[p][2], 3))
            pass_on(p, j, 3)
            pass_on(p, j, 1)

    def opposite(*lines):
        for p in parts:
            for j in lines:
                landed(block(p, None, j, 2), (p, "3g", j))
                pass_on(p, j, 2)

    project((0, 0), (1, 0))
    neighbours(0)
    project((3, 0), (2, 0))
    neighbours(1)
    project((0, 3), (0, 1))
    neighbours(3)
    project((1, 3), (1, 1))
    neighbours(2)
    project((3, 3), (3, 1))
    opposite(0, 1)
    project((2, 3), (2, 1))
    opposite(3, 2)
    project((0, 2), (1, 2))
    project((3, 2), (2, 2))

    expert = lax.div(lax.axis_index("ep") * 4 + lax.axis_index("dp"), 2)

    @pl.loop(0, 32)
    def _(i):
        at = (i // 16, lax.rem(i, 16) // 4, lax.rem(i, 4))
        sums = acc[at].reshape(64, 2 * HF)
        tail = rows[(2,) + at + (slice(None), slice(None), slice(PART - 128, PART))]
        tail = tail.reshape(64, 128).astype(jnp.float32)
        lanes = lax.broadcasted_iota(jnp.int32, (64, 128), 1)
        prob = jnp.sum(jnp.where(lanes == expert, tail, 0.0), axis=1, keepdims=True)
        g, u = sums[:, :HF], sums[:, HF:]
        h = (g / (1.0 + jnp.exp(-g)) * u).astype(jnp.bfloat16).astype(jnp.float32) * prob
        act[at] = h.astype(jnp.bfloat16).reshape(4, 16, HF)

    def spot(p, o2, o3):
        a2 = slice(None) if o2 is None else rel(dims[p][1], o2)
        a3 = slice(None) if o3 is None else rel(dims[p][0], o3)
        return (a3, a2) if p == 1 else (a2, a3)

    def line(p, o1, o2):
        return part.at[(p, o1) + spot(p, o2, None)]

    def sub(p, o3):
        return part.at[(p, 0) + spot(p, 0, o3)]

    def hidden_of(p, o1, core):
        at = {d: (rel(d, o1) if d == dims[p][2] else slice(None)) for d in "xyz"}
        return act[core, at["y"], at["x"], at["z"]].reshape(256, HF)

    def product(p, o1):
        def piece(cols, wcols, width):
            h = jnp.concatenate([hidden_of(p, o1, other), hidden_of(p, o1, c)], axis=0)
            y = jnp.dot(h, dn[:, wcols], preferred_element_type=jnp.float32).astype(jnp.bfloat16)
            pair_out[p, :, :, :, cols] = y[:256].reshape(4, 4, 16, width)
            part[p, o1, :, :, :, cols] = y[256:].reshape(4, 4, 16, width)

        @pl.loop(0, 5)
        def _(n):
            start = pl.multiple_of(n * 256, 256)
            piece(pl.ds(start, 256), pl.ds(pl.multiple_of(p * PART + start, 128), 256), 256)

        if p < 2:
            piece(pl.ds(1280, 128), pl.ds(p * PART + 1280, 128), 128)
        else:
            pair_out[p, :, :, :, 1280:] = jnp.zeros((4, 4, 16, 128), jnp.bfloat16)
            part[p, o1, :, :, :, 1280:] = jnp.zeros((4, 4, 16, 128), jnp.bfloat16)

    def add(dst, *srcs):
        @pl.loop(0, 4)
        def _(i):
            total = dst[i].astype(jnp.float32)
            for s in srcs:
                total += s[i].astype(jnp.float32)
            dst[i] = total.astype(jnp.bfloat16)

    def add_sub(dst, *srcs):
        total = dst[...].astype(jnp.float32)
        for s in srcs:
            total += s[...].astype(jnp.float32)
        dst[...] = total.astype(jnp.bfloat16)

    waited = set()

    def sums_for(o1, then):
        def finish(p):
            landed(pair_in.at[p, o1], (p, "sum", o1))

            @pl.loop(0, 4)
            def _(i):
                add(part.at[p, o1, i], pair_in.at[p, o1, i])

            then(p)

        for p in parts:
            for key in list(pending):
                if key[:2] == (p, "sum") and key not in waited:
                    pending[key].wait_send()
                    waited.add(key)
            product(p, o1)
            send(pair_out.at[p], pair_in.at[p, o1], (p, "sum", o1), device(other_core=True))
            if p:
                finish(p - 1)
        finish(2)

    def up_of(p, level):
        return device(dims[p][level], 1)

    def down_of(p, level):
        return device(dims[p][level], 3)

    UPWARD, DOWNWARD = (2, 1), (3, 0)

    def first(p):
        for k in range(2):
            send(line(p, 2, UPWARD[k]), ra1.at[p, 0, k], (p, "a1+", k), up_of(p, 2))
            send(line(p, 2, DOWNWARD[k]), ra1.at[p, 1, k], (p, "a1-", k), down_of(p, 2))

    def nothing(p):
        pass

    def second(direction, j):
        for p in parts:
            o1, sign, joined = (1, "+", UPWARD) if direction == 0 else (3, "-", DOWNWARD)
            if j in joined:
                k = joined.index(j)
                landed(ra1.at[p, direction, k], (p, "a1" + sign, k))
                add(line(p, o1, j), ra1.at[p, direction, k])
            send(line(p, o1, j), ra2.at[p, direction, j], (p, "a2" + sign, j), device(dims[p][2], o1))

    sums_for(2, first)
    sums_for(1, nothing)
    sums_for(3, nothing)
    for up_line, down_line in ((2, 2), (1, 3), (3, 1), (0, 0)):
        second(0, up_line)
        second(1, down_line)
    sums_for(0, nothing)

    def finish_line(p, j):
        landed(ra2.at[p, 0, j], (p, "a2+", j))
        landed(ra2.at[p, 1, j], (p, "a2-", j))
        add(line(p, 0, j), ra2.at[p, 0, j], ra2.at[p, 1, j])

    def block_of(p, o2, o3):
        return part.at[(p, 0) + spot(p, o2, o3)]

    for p in parts:
        finish_line(p, 2)
        for k in range(2):
            send(block_of(p, 2, UPWARD[k]), rb1.at[p, 0, k], (p, "b1+", k), up_of(p, 1))
            send(block_of(p, 2, DOWNWARD[k]), rb1.at[p, 1, k], (p, "b1-", k), down_of(p, 1))
    for p in parts:
        finish_line(p, 3)
        for j in UPWARD:
            send(block_of(p, 3, j), rb2.at[p, 1, j], (p, "b2-", j), down_of(p, 1))
    for p in parts:
        finish_line(p, 1)
        for j in DOWNWARD:
            send(block_of(p, 1, j), rb2.at[p, 0, j], (p, "b2+", j), up_of(p, 1))
    for k in range(2):
        for p in parts:
            j = UPWARD[k]
            landed(rb1.at[p, 0, k], (p, "b1+", k))
            add_sub(block_of(p, 1, j), rb1.at[p, 0, k])
            send(block_of(p, 1, j), rb2.at[p, 0, j], (p, "b2+", j), up_of(p, 1))
            j = DOWNWARD[k]
            landed(rb1.at[p, 1, k], (p, "b1-", k))
            add_sub(block_of(p, 3, j), rb1.at[p, 1, k])
            send(block_of(p, 3, j), rb2.at[p, 1, j], (p, "b2-", j), down_of(p, 1))
    for p in parts:
        finish_line(p, 0)

    def finish_block(p, j):
        landed(rb2.at[p, 0, j], (p, "b2+", j))
        landed(rb2.at[p, 1, j], (p, "b2-", j))
        add_sub(sub(p, j), rb2.at[p, 0, j], rb2.at[p, 1, j])

    for o in (2, 3, 1):
        for p in parts:
            finish_block(p, o)
            send(sub(p, o), rc.at[p, o - 1], (p, "c", o), device(dims[p][0], o))
    for p in parts:
        finish_block(p, 0)
    for p in parts:
        total = sub(p, 0)[...].astype(jnp.float32)
        for o in (3, 1, 2):
            landed(rc.at[p, o - 1], (p, "c", o))
            total += rc[p, o - 1].astype(jnp.float32)
        width = min(PART, D - p * PART)
        out[:, p * PART : p * PART + width] = total[:, :width]
    for key, copy in pending.items():
        if key not in waited:
            copy.wait_send()
    assert len(names.table) <= SENDS, len(names.table)


def moe(x_in, gate, up, down):
    bf = jnp.bfloat16
    vmem = pl.BlockSpec(memory_space=pltpu.VMEM)
    hbm = pl.BlockSpec(memory_space=pl.ANY)
    return pl.pallas_call(
        moe_kernel,
        out_shape=jax.ShapeDtypeStruct((16, D), jnp.float32),
        in_specs=[vmem, hbm, hbm, hbm],
        out_specs=vmem,
        scratch_shapes=[
            pltpu.VMEM((3, 2, 4, 4, 4, 16, PART), bf),
            pltpu.VMEM((3 * PART, 2 * HF), bf),
            pltpu.VMEM((HF, 3 * PART), bf),
            pltpu.VMEM((2, 4, 4, 4, 16, 2 * HF), jnp.float32),
            pltpu.VMEM((2, 4, 4, 4, 16, HF), bf),
            pltpu.VMEM((3, 4, 4, 4, 16, PART), bf),
            pltpu.VMEM((3, 4, 4, 16, PART), bf),
            pltpu.VMEM((3, 4, 4, 4, 16, PART), bf),
            pltpu.VMEM((3, 2, 2, 4, 16, PART), bf),
            pltpu.VMEM((3, 2, 4, 4, 16, PART), bf),
            pltpu.VMEM((3, 2, 2, 16, PART), bf),
            pltpu.VMEM((3, 2, 4, 16, PART), bf),
            pltpu.VMEM((3, 3, 16, PART), bf),
            pltpu.SemaphoreType.DMA((SENDS,)),
            pltpu.SemaphoreType.DMA((SENDS,)),
            pltpu.SemaphoreType.DMA((3,)),
        ],
        compiler_params=pltpu.CompilerParams(
            collective_id=0, has_side_effects=True, vmem_limit_bytes=67043328
        ),
        name="moe",
    )(x_in, gate, up, down)


HALF = D // 2


def project_kernel(
    att, resid, gain, router, ids, w, hidden_out, x_out,
    seen, part, pair_out, pair_in, ra1, ra2, rc,
    send_sem, recv_sem, all_send, all_recv,
):
    here = Place()
    c = here.c
    other = 1 - c
    rel, device = here.rel, here.device
    ep, dp = lax.axis_index("ep"), lax.axis_index("dp")
    names = Names()
    pending = {}

    def send(src, dst, key, dev):
        i = names(*key)
        copy = pltpu.make_async_remote_copy(
            src_ref=src, dst_ref=dst, send_sem=send_sem.at[i], recv_sem=recv_sem.at[i],
            device_id=dev, device_id_type=MESH,
        )
        copy.start()
        pending[key] = copy

    def landed(dst, key):
        i = names(*key)
        pltpu.make_async_remote_copy(
            src_ref=dst, dst_ref=dst, send_sem=send_sem.at[i], recv_sem=recv_sem.at[i],
            device_id=device(other_core=True), device_id_type=MESH,
        ).wait_recv()

    def slot(e):
        return lax.rem(e, 2) * 16 + lax.div(e, 2)

    barrier = pltpu.get_barrier_semaphore()
    for k in range(1, 32):
        pl.semaphore_signal(barrier, inc=1, device_id=(lax.rem(ep + k, 32), dp), device_id_type=MESH)
    seen[slot(ep)] = att[:, pl.ds(pl.multiple_of(ep * 256, 256), 256)]
    pl.semaphore_wait(barrier, 31)

    for k in range(1, 32):
        to = lax.rem(ep + k, 32)
        pltpu.make_async_remote_copy(
            src_ref=att.at[:, pl.ds(pl.multiple_of(to * 256, 256), 256)],
            dst_ref=seen.at[slot(ep)],
            send_sem=all_send.at[0],
            recv_sem=all_recv.at[0],
            device_id=(to, dp),
            device_id_type=MESH,
        ).start()
    everything = pltpu.make_async_remote_copy(
        src_ref=seen.at[pl.ds(0, 31)], dst_ref=seen.at[pl.ds(0, 31)],
        send_sem=all_send.at[0], recv_sem=all_recv.at[0],
        device_id=device(other_core=True), device_id_type=MESH,
    )
    everything.wait_recv()

    first_dim = ("x", "y")
    second_dim = ("y", "x")

    def spot(q, o1, o2):
        at = {first_dim[q]: rel(first_dim[q], o1), second_dim[q]: rel(second_dim[q], o2)}
        return part.at[q, at["y"], at["x"]]

    def product(q):
        @pl.loop(0, HALF // 256)
        def _(n):
            start = pl.multiple_of(n * 256, 256)
            theirs = seen[pl.ds(other * 16, 16)].reshape(256, 256)
            ours = seen[pl.ds(c * 16, 16)].reshape(256, 256)
            rows = jnp.concatenate([theirs, ours], axis=0)
            cols = pl.ds(pl.multiple_of(q * HALF + start, 256), 256)
            y = jnp.dot(rows, w[:, cols], preferred_element_type=jnp.float32).astype(jnp.bfloat16)
            pair_out[q, :, :, :, pl.ds(start, 256)] = y[:256].reshape(4, 4, 16, 256)
            part[q, :, :, :, pl.ds(start, 256)] = y[256:].reshape(4, 4, 16, 256)

    def add(dst, *srcs):
        total = dst[...].astype(jnp.float32)
        for src in srcs:
            total += src[...].astype(jnp.float32)
        dst[...] = total.astype(jnp.bfloat16)

    UPWARD, DOWNWARD = (2, 1), (3, 0)
    for q in range(2):
        product(q)
        send(pair_out.at[q], pair_in.at[q], (q, "sum"), device(other_core=True))
    for q in range(2):
        landed(pair_in.at[q], (q, "sum"))

        def join(o1, o2):
            at = {first_dim[q]: rel(first_dim[q], o1), second_dim[q]: rel(second_dim[q], o2)}
            add(spot(q, o1, o2), pair_in.at[q, at["y"], at["x"]])

        for k in range(2):
            join(2, UPWARD[k])
            send(spot(q, 2, UPWARD[k]), ra1.at[q, 0, k], (q, "a1+", k), device(first_dim[q], 1))
            join(2, DOWNWARD[k])
            send(spot(q, 2, DOWNWARD[k]), ra1.at[q, 1, k], (q, "a1-", k), device(first_dim[q], 3))
        for o1 in (1, 3, 0):
            for o2 in range(4):
                join(o1, o2)

    def second(direction, j):
        for q in range(2):
            o1, sign, joined = (1, "+", UPWARD) if direction == 0 else (3, "-", DOWNWARD)
            if j in joined:
                k = joined.index(j)
                landed(ra1.at[q, direction, k], (q, "a1" + sign, k))
                add(spot(q, o1, j), ra1.at[q, direction, k])
            send(spot(q, o1, j), ra2.at[q, direction, j], (q, "a2" + sign, j), device(first_dim[q], o1))

    for up_block, down_block in ((3, 2), (2, 3), (1, 1), (0, 0)):
        second(0, up_block)
        second(1, down_block)

    def finish(q, j):
        landed(ra2.at[q, 0, j], (q, "a2+", j))
        landed(ra2.at[q, 1, j], (q, "a2-", j))
        add(spot(q, 0, j), ra2.at[q, 0, j], ra2.at[q, 1, j])

    for o in (2, 3, 1):
        for q in range(2):
            finish(q, o)
            send(spot(q, 0, o), rc.at[q, o - 1], (q, "c", o), device(second_dim[q], o))
    for q in range(2):
        finish(q, 0)
    square = jnp.zeros((16, 1), jnp.float32)
    for q in range(2):
        total = spot(q, 0, 0)[...].astype(jnp.float32)
        for o in (3, 1, 2):
            landed(rc.at[q, o - 1], (q, "c", o))
            total += rc[q, o - 1].astype(jnp.float32)
        cols = slice(q * HALF, (q + 1) * HALF)
        hidden = resid[:, cols].astype(jnp.float32) + total
        hidden_out[:, cols] = hidden
        square += jnp.sum(hidden * hidden, axis=1, keepdims=True)
    scale = lax.rsqrt(jnp.maximum(square * (1.0 / D), 0.25))
    logits = jnp.zeros((16, router.shape[1]), jnp.float32)
    for q in range(2):
        cols = slice(q * HALF, (q + 1) * HALF)
        normed = (hidden_out[:, cols] * scale * gain[:, cols]).astype(jnp.bfloat16)
        x_out[:, cols] = normed
        logits += jnp.dot(normed, router[cols, :], preferred_element_type=jnp.float32)
    labels = lax.broadcasted_iota(jnp.int32, logits.shape, 1)
    named = ids[:, 0:1] == labels
    for k in range(1, TOP):
        named = named | (ids[:, k : k + 1] == labels)
    peak = jnp.max(jnp.where(named, logits, -jnp.inf), axis=1, keepdims=True)
    grown = jnp.where(named, jnp.exp(jnp.where(named, logits - peak, 0.0)), 0.0)
    probs = grown / jnp.sum(grown, axis=1, keepdims=True)
    rest = jnp.zeros((16, 3 * PART - D - router.shape[1]), jnp.float32)
    x_out[:, D:] = jnp.concatenate([probs, rest], axis=1).astype(jnp.bfloat16)

    everything.wait_send()
    for copy in pending.values():
        copy.wait_send()


def attention_out(attended, resid, norm_gain, router, expert_ids, out_proj):
    bf = jnp.bfloat16
    vmem = pl.BlockSpec(memory_space=pltpu.VMEM)
    return pl.pallas_call(
        project_kernel,
        out_shape=(
            jax.ShapeDtypeStruct((16, D), jnp.float32),
            jax.ShapeDtypeStruct((16, 3 * PART), bf),
        ),
        in_specs=[vmem] * 6,
        out_specs=(vmem, vmem),
        scratch_shapes=[
            pltpu.VMEM((32, 16, 256), bf),
            pltpu.VMEM((2, 4, 4, 16, HALF), bf),
            pltpu.VMEM((2, 4, 4, 16, HALF), bf),
            pltpu.VMEM((2, 4, 4, 16, HALF), bf),
            pltpu.VMEM((2, 2, 2, 16, HALF), bf),
            pltpu.VMEM((2, 2, 4, 16, HALF), bf),
            pltpu.VMEM((2, 3, 16, HALF), bf),
            pltpu.SemaphoreType.DMA((40,)),
            pltpu.SemaphoreType.DMA((40,)),
            pltpu.SemaphoreType.DMA((1,)),
            pltpu.SemaphoreType.DMA((1,)),
        ],
        compiler_params=pltpu.CompilerParams(
            collective_id=1, has_side_effects=True, vmem_limit_bytes=40 * 2**20
        ),
        name="attention_out",
    )(attended, resid, norm_gain.reshape(1, D), router, expert_ids, out_proj)


def local(
    resid,
    queries,
    new_keys,
    new_values,
    cache_keys,
    cache_values,
    cache_len,
    out_proj,
    norm_gain,
    router,
    expert_ids,
    gate_slab,
    up_slab,
    down_slab,
):
    attended = attend(queries, new_keys, new_values, cache_keys, cache_values, cache_len)
    hidden, x_in = attention_out(attended, resid, norm_gain, router, expert_ids, out_proj)
    return hidden + moe(x_in, gate_slab[0], up_slab[0], down_slab[0])


def solution(mesh):
    in_specs = (
        P(("ep", "dp"), None),
        P(("ep", "dp"), None),
        P(("ep", "dp"), None),
        P(("ep", "dp"), None),
        P(("ep", "dp"), None, None),
        P(("ep", "dp"), None, None),
        P(("ep", "dp")),
        P("ep", None),
        P(),
        P(),
        P(("ep", "dp"), None),
        P(("ep", "dp"), None, None),
        P(("ep", "dp"), None, None),
        P(("ep", "dp"), None, None),
    )
    out_specs = P(("ep", "dp"), None)
    return jax.shard_map(local, mesh=mesh, in_specs=in_specs, out_specs=out_specs, check_vma=False)
```

```python
import functools
import math

import jax
import jax.numpy as jnp
from jax import lax
from jax.experimental import pallas as pl
from jax.experimental.pallas import tpu as pltpu
from jax.sharding import PartitionSpec as P

D = 4096
H = 64
KVH = 4
HD = 128
TOP = 8
MESH = pl.DeviceIdType.MESH

PART = 1408
ORDER = (("x", "y", "z"), ("y", "z", "x"), ("z", "x", "y"))
HF = 384


def attend(queries, new_keys, new_values, cache_keys, cache_values, cache_len):
    local_rows = queries.shape[0]
    cache_span = cache_keys.shape[1]
    group_size = H // KVH
    query_heads = queries.reshape(local_rows, KVH, group_size, HD)
    past_keys = cache_keys.reshape(local_rows, cache_span, KVH, HD)
    past_values = cache_values.reshape(local_rows, cache_span, KVH, HD)
    score_scale = 1.0 / math.sqrt(HD)
    past_scores = (
        jnp.einsum("tgqd,tcgd->tgqc", query_heads, past_keys, preferred_element_type=jnp.float32)
        * score_scale
    )
    own_scores = (
        jnp.einsum(
            "tgqd,tgd->tgq",
            query_heads,
            new_keys.reshape(local_rows, KVH, HD),
            preferred_element_type=jnp.float32,
        )
        * score_scale
    )
    is_valid = lax.broadcasted_iota(jnp.int32, (local_rows, cache_span), 1) < cache_len[:, None]
    past_scores = jnp.where(is_valid[:, None, None, :], past_scores, -1e30)
    peak_score = jnp.maximum(jnp.max(past_scores, axis=3), own_scores)
    past_exp = jnp.exp(past_scores - peak_score[..., None])
    own_exp = jnp.exp(own_scores - peak_score)
    denom_sum = jnp.sum(past_exp, axis=3) + own_exp
    past_weights = (past_exp / denom_sum[..., None]).astype(jnp.bfloat16)
    own_weights = (own_exp / denom_sum).astype(jnp.bfloat16)
    blended = jnp.einsum(
        "tgqc,tcgd->tgqd", past_weights, past_values, preferred_element_type=jnp.float32
    )
    blended = blended + own_weights.astype(jnp.float32)[..., None] * new_values.reshape(
        local_rows, KVH, 1, HD
    ).astype(jnp.float32)
    return blended.reshape(local_rows, H * HD).astype(jnp.bfloat16)


class Place:
    def __init__(self):
        ep = lax.axis_index("ep")
        self.c = lax.rem(ep, 2)
        self.coord = {
            "x": lax.rem(lax.div(ep, 2), 4),
            "y": lax.div(ep, 8),
            "z": lax.axis_index("dp"),
        }

    def rel(self, dim, offset):
        if isinstance(offset, int) and offset == 0:
            return self.coord[dim]
        return lax.rem(self.coord[dim] + offset, 4)

    def device(self, dim=None, offset=0, other_core=False):
        at = dict(self.coord)
        if dim is not None:
            at[dim] = self.rel(dim, offset)
        core = 1 - self.c if other_core else self.c
        return ((at["y"] * 4 + at["x"]) * 2 + core, at["z"])


class Names:
    def __init__(self):
        self.table = {}

    def __call__(self, *key):
        return self.table.setdefault(key, len(self.table))


GROUPS = ("1", "2", "2g", "3", "3g", "pair", "a1", "a2", "b1", "b2", "c", ("sum", 0), ("sum", 1), ("sum", 2))
KEYS = 126


def moe_kernel(
    x_in, hidden, gate, up, down, out,
    residual, rows, gu, dn, acc, act, part, pair_out, pair_in, ra1, ra2, rb1, rb2, rc,
    send_sem, recv_sem, load_sem,
):
    here = Place()
    c = here.c
    other = 1 - c
    rel, device = here.rel, here.device
    names = Names()
    parts = range(3)
    dims = ORDER

    def send(src, dst, key, dev, group):
        copy = pltpu.make_async_remote_copy(
            src_ref=src, dst_ref=dst, send_sem=send_sem.at[GROUPS.index(group)], recv_sem=recv_sem.at[names(*key)],
            device_id=dev, device_id_type=MESH,
        )
        copy.start()
        return copy

    def landed(ref, key):
        pltpu.make_async_remote_copy(
            src_ref=ref, dst_ref=ref, send_sem=send_sem.at[0], recv_sem=recv_sem.at[names(*key)],
            device_id=device(other_core=True), device_id_type=MESH,
        ).wait_recv()

    def sent(ref, group):
        pltpu.make_async_remote_copy(
            src_ref=ref, dst_ref=ref, send_sem=send_sem.at[GROUPS.index(group)], recv_sem=recv_sem.at[0],
            device_id=device(other_core=True), device_id_type=MESH,
        ).wait_send()

    def amount(p, n):
        if n == 1:
            return rows.at[p, 0, 0, 0, 0]
        if n < 4:
            return rows.at[p, 0, 0, 0, pl.ds(0, n)]
        if n < 16:
            return rows.at[p, 0, 0, pl.ds(0, n // 4)]
        return rows.at[p, 0, pl.ds(0, n // 16)]

    def where(p, o1, o2, o3):
        at = {d: (slice(None) if o is None else rel(d, o)) for d, o in zip(ORDER[p], (o1, o2, o3))}
        return at["y"], at["x"], at["z"]

    def block(p, o1, o2, o3, core=None):
        return rows.at[(p, c if core is None else core) + where(p, o1, o2, o3)]

    def send_sub(p, j):
        ref = block(p, j, 0, 0)
        send(ref, ref, (p, "2", j), device(dims[p][1], 1), "2")
        send(ref, ref, (p, "2", j), device(dims[p][1], 3), "2")

    def send_line(p, j):
        ref = block(p, None, j, 0)
        send(ref, ref, (p, "3", j), device(dims[p][2], 1), "3")
        send(ref, ref, (p, "3", j), device(dims[p][2], 3), "3")

    def send_block(p, i, j):
        ref = block(p, i, j, 0)
        send(ref, ref, (p, "3", j), device(dims[p][2], 1), "3")
        send(ref, ref, (p, "3", j), device(dims[p][2], 3), "3")

    def unit(o2, o3):
        if o3 in (1, 3):
            return "near", o2
        return o3, o2 in (0, 1)

    def pass_on(p, o2, o3):
        ref = block(p, None, o2, o3)
        send(ref, ref, (p, "pair") + unit(o2, o3), device(other_core=True), "pair")

    barrier = pltpu.get_barrier_semaphore()
    for dim in ("x", "y", "z"):
        for o in (1, 2, 3):
            pl.semaphore_signal(barrier, inc=1, device_id=device(dim, o), device_id_type=MESH)
    pl.semaphore_signal(barrier, inc=1, device_id=device(other_core=True), device_id_type=MESH)

    fetch = pltpu.make_async_copy(hidden, residual, load_sem.at[3])
    fetch.start()
    starts = [
        pltpu.make_async_copy(x_in.at[:, pl.ds(p * PART, PART)], rows.at[(p, c) + where(p, 0, 0, 0)], load_sem.at[4 + p])
        for p in range(3)
    ]
    for copy in starts:
        copy.start()
    loads = [
        pltpu.make_async_copy(gate, gu.at[pl.ds(0, D), pl.ds(0, HF)], load_sem.at[0]),
        pltpu.make_async_copy(up, gu.at[pl.ds(0, D), pl.ds(HF, HF)], load_sem.at[1]),
        pltpu.make_async_copy(down, dn.at[:, pl.ds(0, D)], load_sem.at[2]),
    ]
    for copy in loads:
        copy.start()
    pl.semaphore_wait(barrier, 10)

    for copy in starts:
        copy.wait()
    fetch.wait()
    for p in parts:
        own = block(p, 0, 0, 0)
        for o in (1, 3):
            send(own, own, (p, "1n"), device(dims[p][0], o), "1")
        send(own, own, (p, "1f"), device(dims[p][0], 2), "1")
    for p in parts:
        send_sub(p, 0)

    gu[D:, :] = jnp.zeros((3 * PART - D, 2 * HF), jnp.bfloat16)
    dn[:, D:] = jnp.zeros((HF, 3 * PART - D), jnp.bfloat16)

    @pl.loop(0, 32)
    def _(i):
        acc[i // 16, lax.rem(i, 16) // 4, lax.rem(i, 4)] = jnp.zeros((4, 16, 2 * HF), jnp.float32)

    for p in parts:
        send_block(p, 0, 0)
    for p in parts:
        landed(amount(p, 2), (p, "1n"))
        send_sub(p, 1)
        send_sub(p, 3)
    for p in parts:
        landed(amount(p, 1), (p, "1f"))
        send_sub(p, 2)
    for p in parts:
        for i in (1, 3, 2):
            send_block(p, i, 0)
        pass_on(p, 0, 0)
    for j in (0, 1, 3, 2):
        for p in parts:
            landed(amount(p, 2), (p, "2", j))
            o = 3 if j in (0, 1) else 1
            ref = block(p, j, o, 0)
            send(ref, ref, (p, "2g"), device(dims[p][1], 4 - o), "2g")
            send_block(p, j, 1)
            send_block(p, j, 3)
    for p in parts:
        pass_on(p, 1, 0)
        pass_on(p, 3, 0)
    for copy in loads:
        copy.wait()
    for p in parts:
        landed(amount(p, 4), (p, "2g"))
        send_line(p, 2)
        pass_on(p, 2, 0)

    def project(*lines):
        for p in parts:
            landed(amount(p, 8), (p, "pair") + unit(*lines[0]))
            at = [where(p, None, o2, o3) for o2, o3 in lines]

            @pl.loop(0, 3, unroll=3)
            def _(n):
                cols = pl.ds(pl.multiple_of(n * 256, 256), 256)
                x = [rows[(p, slice(None)) + a].reshape(128, PART) for a in at]
                x = jnp.concatenate(x, axis=0)
                w = gu[p * PART : (p + 1) * PART, cols]
                y = jnp.dot(x, w, preferred_element_type=jnp.float32)
                for i, a in enumerate(at):
                    idx = (slice(None),) + a + (slice(None), cols)
                    acc[idx] += y[i * 128 : (i + 1) * 128].reshape(2, 4, 16, 256)

    def neighbours(j):
        for p in parts:
            landed(amount(p, 8), (p, "3", j))
            o = 3 if j in (0, 3) else 1
            ref = block(p, None, j, o)
            send(ref, ref, (p, "3g", j in (0, 1)), device(dims[p][2], 4 - o), "3g")
            pass_on(p, j, 3)
            pass_on(p, j, 1)

    def opposite(*lines):
        for p in parts:
            landed(amount(p, 8), (p, "3g", lines[0] in (0, 1)))
            for j in lines:
                pass_on(p, j, 2)

    project((0, 0), (1, 0))
    neighbours(0)
    project((3, 0), (2, 0))
    neighbours(1)
    project((0, 3), (0, 1))
    neighbours(3)
    project((1, 3), (1, 1))
    neighbours(2)
    project((3, 3), (3, 1))
    opposite(0, 1)
    project((2, 3), (2, 1))
    opposite(3, 2)
    project((0, 2), (1, 2))
    project((3, 2), (2, 2))

    expert = lax.div(lax.axis_index("ep") * 4 + lax.axis_index("dp"), 2)

    def activate(at):
        sums = acc[at].reshape(64, 2 * HF)
        tail = rows[(2,) + at + (slice(None), slice(PART - 128, PART))]
        tail = tail.reshape(64, 128).astype(jnp.float32)
        lanes = lax.broadcasted_iota(jnp.int32, (64, 128), 1)
        prob = jnp.sum(jnp.where(lanes == expert, tail, 0.0), axis=1, keepdims=True)
        g, u = sums[:, :HF], sums[:, HF:]
        h = (g / (1.0 + jnp.exp(-g)) * u).astype(jnp.bfloat16).astype(jnp.float32) * prob
        act[at] = h.astype(jnp.bfloat16).reshape(4, 16, HF)

    every = slice(None)

    def activate_opposite(p):
        far = rel(dims[p][2], 2)

        @pl.loop(0, 8)
        def _(i):
            core, k = i // 4, lax.rem(i, 4)
            activate(((core, k, every, far), (core, k, far, every), (core, far, k, every))[p])

    def activate_rest():
        @pl.loop(0, 18)
        def _(i):
            k = lax.rem(i, 9)
            oy, ox = k // 3, lax.rem(k, 3)
            oy, ox = oy + oy // 2, ox + ox // 2
            activate((i // 9, rel("y", oy), rel("x", ox), every))

    def spot(p, o2, o3):
        a2 = slice(None) if o2 is None else rel(dims[p][1], o2)
        a3 = slice(None) if o3 is None else rel(dims[p][0], o3)
        return (a3, a2) if p == 1 else (a2, a3)

    def line(p, o1, o2):
        return part.at[(p, o1) + spot(p, o2, None)]

    def sub(p, o3):
        return part.at[(p, 0) + spot(p, 0, o3)]

    def hidden_of(p, o1, core):
        at = {d: (rel(d, o1) if d == dims[p][2] else slice(None)) for d in "xyz"}
        return act[core, at["y"], at["x"], at["z"]].reshape(256, HF)

    def product(p, o1):
        def piece(cols, wcols, width):
            h = jnp.concatenate([hidden_of(p, o1, other), hidden_of(p, o1, c)], axis=0)
            y = jnp.dot(h, dn[:, wcols], preferred_element_type=jnp.float32).astype(jnp.bfloat16)
            pair_out[p, :, :, :, cols] = y[:256].reshape(4, 4, 16, width)
            part[p, o1, :, :, :, cols] = y[256:].reshape(4, 4, 16, width)

        @pl.loop(0, 5, unroll=5)
        def _(n):
            start = pl.multiple_of(n * 256, 256)
            piece(pl.ds(start, 256), pl.ds(pl.multiple_of(p * PART + start, 128), 256), 256)

        if p < 2:
            piece(pl.ds(1280, 128), pl.ds(p * PART + 1280, 128), 128)
        else:
            pair_out[p, :, :, :, 1280:] = jnp.zeros((4, 4, 16, 128), jnp.bfloat16)
            part[p, o1, :, :, :, 1280:] = jnp.zeros((4, 4, 16, 128), jnp.bfloat16)

    def add(dst, *srcs):
        @pl.loop(0, 4)
        def _(i):
            total = dst[i].astype(jnp.float32)
            for s in srcs:
                total += s[i].astype(jnp.float32)
            dst[i] = total.astype(jnp.bfloat16)

    def add_sub(dst, *srcs):
        total = dst[...].astype(jnp.float32)
        for s in srcs:
            total += s[...].astype(jnp.float32)
        dst[...] = total.astype(jnp.bfloat16)

    last = {}

    def sums_for(o1, then, before=None):
        def finish(p):
            landed(pair_in.at[p, o1], (p, "sum", o1))

            @pl.loop(0, 4)
            def _(i):
                add(part.at[p, o1, i], pair_in.at[p, o1, i])

            then(p)

        for p in parts:
            if p in last:
                last[p].wait_send()
            if before is not None:
                before(p)
            product(p, o1)
            last[p] = send(pair_out.at[p], pair_in.at[p, o1], (p, "sum", o1), device(other_core=True), ("sum", p))
            if p:
                finish(p - 1)
        finish(2)

    def up_of(p, level):
        return device(dims[p][level], 1)

    def down_of(p, level):
        return device(dims[p][level], 3)

    UPWARD, DOWNWARD = (2, 1), (3, 0)

    def first(p):
        for k in range(2):
            send(line(p, 2, UPWARD[k]), ra1.at[p, 0, k], (p, "a1", 0, k), up_of(p, 2), "a1")
            send(line(p, 2, DOWNWARD[k]), ra1.at[p, 1, k], (p, "a1", 1, k), down_of(p, 2), "a1")

    def nothing(p):
        pass

    def second(direction, j):
        o1, joined = (1, UPWARD) if direction == 0 else (3, DOWNWARD)
        for p in parts:
            if j in joined:
                k = joined.index(j)
                landed(ra1.at[p, direction, k], (p, "a1", direction, k))
                add(line(p, o1, j), ra1.at[p, direction, k])
            send(line(p, o1, j), ra2.at[p, direction, j], (p, "a2", j), device(dims[p][2], o1), "a2")

    sums_for(2, first, activate_opposite)
    activate_rest()
    sums_for(1, nothing)
    sums_for(3, nothing)
    second(0, 2)
    second(1, 2)
    second(0, 1)
    second(1, 3)
    second(0, 3)
    second(1, 1)
    sums_for(0, nothing)

    def finish_line(p, j):
        landed(ra2.at[p, 0, pl.ds(0, 2)], (p, "a2", j))
        add(line(p, 0, j), ra2.at[p, 0, j], ra2.at[p, 1, j])

    def block_of(p, o2, o3):
        return part.at[(p, 0) + spot(p, o2, o3)]

    for p in parts:
        finish_line(p, 2)
        for k in range(2):
            send(block_of(p, 2, UPWARD[k]), rb1.at[p, 0, k], (p, "b1", 0, k), up_of(p, 1), "b1")
            send(block_of(p, 2, DOWNWARD[k]), rb1.at[p, 1, k], (p, "b1", 1, k), down_of(p, 1), "b1")
    second(0, 0)
    second(1, 0)
    for p in parts:
        finish_line(p, 3)
        for j in UPWARD:
            send(block_of(p, 3, j), rb2.at[p, 1, j], (p, "b2", j), down_of(p, 1), "b2")
    for p in parts:
        finish_line(p, 1)
        for j in DOWNWARD:
            send(block_of(p, 1, j), rb2.at[p, 0, j], (p, "b2", j), up_of(p, 1), "b2")
    for k in range(2):
        for p in parts:
            j = UPWARD[k]
            landed(rb1.at[p, 0, k], (p, "b1", 0, k))
            add_sub(block_of(p, 1, j), rb1.at[p, 0, k])
            send(block_of(p, 1, j), rb2.at[p, 0, j], (p, "b2", j), up_of(p, 1), "b2")
            j = DOWNWARD[k]
            landed(rb1.at[p, 1, k], (p, "b1", 1, k))
            add_sub(block_of(p, 3, j), rb1.at[p, 1, k])
            send(block_of(p, 3, j), rb2.at[p, 1, j], (p, "b2", j), down_of(p, 1), "b2")
    for p in parts:
        finish_line(p, 0)

    def finish_block(p, j):
        landed(rb2.at[p, 0, pl.ds(0, 2)], (p, "b2", j))
        add_sub(sub(p, j), rb2.at[p, 0, j], rb2.at[p, 1, j])

    for o in (2, 3, 1):
        for p in parts:
            finish_block(p, o)
            send(sub(p, o), rc.at[p, o - 1], (p, "c"), device(dims[p][0], o), "c")
    for p in parts:
        finish_block(p, 0)
    for p in parts:
        landed(rc.at[p], (p, "c"))
        total = sub(p, 0)[...].astype(jnp.float32)
        for o in (3, 1, 2):
            total += rc[p, o - 1].astype(jnp.float32)
        width = min(PART, D - p * PART)
        cols = slice(p * PART, p * PART + width)
        out[:, cols] = residual[:, cols] + total[:, :width]
    for group, n in (("1", 3), ("2", 8), ("2g", 4), ("3", 32), ("3g", 16), ("pair", 64)):
        sent(amount(slice(None), n), group)
    for group, n in (("a1", 16), ("a2", 32), ("b1", 4), ("b2", 8), ("c", 3)):
        sent(amount(slice(None), n), group)
    for p in parts:
        last[p].wait_send()
    assert len(names.table) == KEYS, len(names.table)


def moe(x_in, hidden, gate, up, down):
    bf = jnp.bfloat16
    vmem = pl.BlockSpec(memory_space=pltpu.VMEM)
    hbm = pl.BlockSpec(memory_space=pl.ANY)
    return pl.pallas_call(
        moe_kernel,
        out_shape=jax.ShapeDtypeStruct((16, D), jnp.float32),
        in_specs=[hbm] * 5,
        out_specs=vmem,
        scratch_shapes=[
            pltpu.VMEM((16, D), jnp.float32),
            pltpu.VMEM((3, 2, 4, 4, 4, 16, PART), bf),
            pltpu.VMEM((3 * PART, 2 * HF), bf),
            pltpu.VMEM((HF, 3 * PART), bf),
            pltpu.VMEM((2, 4, 4, 4, 16, 2 * HF), jnp.float32),
            pltpu.VMEM((2, 4, 4, 4, 16, HF), bf),
            pltpu.VMEM((3, 4, 4, 4, 16, PART), bf),
            pltpu.VMEM((3, 4, 4, 16, PART), bf),
            pltpu.VMEM((3, 4, 4, 4, 16, PART), bf),
            pltpu.VMEM((3, 2, 2, 4, 16, PART), bf),
            pltpu.VMEM((3, 2, 4, 4, 16, PART), bf),
            pltpu.VMEM((3, 2, 2, 16, PART), bf),
            pltpu.VMEM((3, 2, 4, 16, PART), bf),
            pltpu.VMEM((3, 3, 16, PART), bf),
            pltpu.SemaphoreType.DMA((len(GROUPS),)),
            pltpu.SemaphoreType.DMA((KEYS,)),
            pltpu.SemaphoreType.DMA((7,)),
        ],
        compiler_params=pltpu.CompilerParams(
            collective_id=0, has_side_effects=True, vmem_limit_bytes=67043328
        ),
        name="moe",
    )(x_in, hidden, gate, up, down)


HALF = D // 2


def project_kernel(
    att, resid_hbm, gain_hbm, router_hbm, ids_hbm, w_hbm, hidden_out, x_out,
    resid, gain, router, ids, w, seen, part, pair_out, pair_in, ra1, ra2, rc,
    send_sem, recv_sem, all_send, all_recv, load_sem,
):
    here = Place()
    c = here.c
    other = 1 - c
    rel, device = here.rel, here.device
    ep, dp = lax.axis_index("ep"), lax.axis_index("dp")
    names = Names()
    groups = ("sum", "a1", "a2", "c")
    loads = [
        pltpu.make_async_copy(src, dst, load_sem.at[i])
        for i, (src, dst) in enumerate(
            ((w_hbm, w), (resid_hbm, resid), (gain_hbm, gain), (router_hbm, router), (ids_hbm, ids))
        )
    ]
    for copy in loads:
        copy.start()

    def send(src, dst, key, dev):
        pltpu.make_async_remote_copy(
            src_ref=src, dst_ref=dst, send_sem=send_sem.at[groups.index(key[1])], recv_sem=recv_sem.at[names(*key)],
            device_id=dev, device_id_type=MESH,
        ).start()

    def landed(ref, key):
        pltpu.make_async_remote_copy(
            src_ref=ref, dst_ref=ref, send_sem=send_sem.at[0], recv_sem=recv_sem.at[names(*key)],
            device_id=device(other_core=True), device_id_type=MESH,
        ).wait_recv()

    def sent(ref, group):
        pltpu.make_async_remote_copy(
            src_ref=ref, dst_ref=ref, send_sem=send_sem.at[groups.index(group)], recv_sem=recv_sem.at[0],
            device_id=device(other_core=True), device_id_type=MESH,
        ).wait_send()

    def slot(e):
        return lax.rem(e, 2) * 16 + lax.div(e, 2)

    barrier = pltpu.get_barrier_semaphore()
    for k in range(1, 32):
        pl.semaphore_signal(barrier, inc=1, device_id=(lax.rem(ep + k, 32), dp), device_id_type=MESH)
    seen[slot(ep)] = att[:, pl.ds(pl.multiple_of(ep * 256, 256), 256)]
    pl.semaphore_wait(barrier, 31)

    for k in range(1, 32):
        to = lax.rem(ep + k, 32)
        pltpu.make_async_remote_copy(
            src_ref=att.at[:, pl.ds(pl.multiple_of(to * 256, 256), 256)],
            dst_ref=seen.at[slot(ep)],
            send_sem=all_send.at[0],
            recv_sem=all_recv.at[0],
            device_id=(to, dp),
            device_id_type=MESH,
        ).start()
    everything = pltpu.make_async_remote_copy(
        src_ref=seen.at[pl.ds(0, 31)], dst_ref=seen.at[pl.ds(0, 31)],
        send_sem=all_send.at[0], recv_sem=all_recv.at[0],
        device_id=device(other_core=True), device_id_type=MESH,
    )
    loads[0].wait()
    everything.wait_recv()

    first_dim = ("x", "y")
    second_dim = ("y", "x")

    def spot(q, o1, o2):
        at = {first_dim[q]: rel(first_dim[q], o1), second_dim[q]: rel(second_dim[q], o2)}
        return part.at[q, at["y"], at["x"]]

    def product(q):
        @pl.loop(0, HALF // 256, unroll=4)
        def _(n):
            start = pl.multiple_of(n * 256, 256)
            theirs = seen[pl.ds(other * 16, 16)].reshape(256, 256)
            ours = seen[pl.ds(c * 16, 16)].reshape(256, 256)
            rows = jnp.concatenate([theirs, ours], axis=0)
            cols = pl.ds(pl.multiple_of(q * HALF + start, 256), 256)
            y = jnp.dot(rows, w[:, cols], preferred_element_type=jnp.float32).astype(jnp.bfloat16)
            pair_out[q, :, :, :, pl.ds(start, 256)] = y[:256].reshape(4, 4, 16, 256)
            part[q, :, :, :, pl.ds(start, 256)] = y[256:].reshape(4, 4, 16, 256)

    def add(dst, *srcs):
        total = dst[...].astype(jnp.float32)
        for src in srcs:
            total += src[...].astype(jnp.float32)
        dst[...] = total.astype(jnp.bfloat16)

    UPWARD, DOWNWARD = (2, 1), (3, 0)
    for q in range(2):
        product(q)
        send(pair_out.at[q], pair_in.at[q], (q, "sum"), device(other_core=True))
    for q in range(2):
        landed(pair_in.at[q], (q, "sum"))

        def join(o1, o2):
            at = {first_dim[q]: rel(first_dim[q], o1), second_dim[q]: rel(second_dim[q], o2)}
            add(spot(q, o1, o2), pair_in.at[q, at["y"], at["x"]])

        for k in range(2):
            join(2, UPWARD[k])
            send(spot(q, 2, UPWARD[k]), ra1.at[q, 0, k], (q, "a1", 0, k), device(first_dim[q], 1))
            join(2, DOWNWARD[k])
            send(spot(q, 2, DOWNWARD[k]), ra1.at[q, 1, k], (q, "a1", 1, k), device(first_dim[q], 3))
        for o1 in (1, 3, 0):
            for o2 in range(4):
                join(o1, o2)

    def second(direction, j):
        for q in range(2):
            o1, joined = (1, UPWARD) if direction == 0 else (3, DOWNWARD)
            if j in joined:
                k = joined.index(j)
                landed(ra1.at[q, direction, k], (q, "a1", direction, k))
                add(spot(q, o1, j), ra1.at[q, direction, k])
            send(spot(q, o1, j), ra2.at[q, direction, j], (q, "a2", j), device(first_dim[q], o1))

    for up_block, down_block in ((3, 2), (2, 3), (1, 1), (0, 0)):
        second(0, up_block)
        second(1, down_block)

    def finish(q, j):
        landed(ra2.at[q, 0, pl.ds(0, 2)], (q, "a2", j))
        add(spot(q, 0, j), ra2.at[q, 0, j], ra2.at[q, 1, j])

    for o in (2, 3, 1):
        for q in range(2):
            finish(q, o)
            send(spot(q, 0, o), rc.at[q, o - 1], (q, "c"), device(second_dim[q], o))
    for q in range(2):
        finish(q, 0)
    for copy in loads[1:]:
        copy.wait()
    square = jnp.zeros((16, 1), jnp.float32)
    for q in range(2):
        landed(rc.at[q], (q, "c"))
        total = spot(q, 0, 0)[...].astype(jnp.float32)
        for o in (3, 1, 2):
            total += rc[q, o - 1].astype(jnp.float32)
        cols = slice(q * HALF, (q + 1) * HALF)
        hidden = resid[:, cols].astype(jnp.float32) + total
        hidden_out[:, cols] = hidden
        square += jnp.sum(hidden * hidden, axis=1, keepdims=True)
    scale = lax.rsqrt(jnp.maximum(square * (1.0 / D), 0.25))
    logits = jnp.zeros((router.shape[0], 16), jnp.float32)
    for q in range(2):
        cols = slice(q * HALF, (q + 1) * HALF)
        normed = (hidden_out[:, cols] * scale * gain[:, cols]).astype(jnp.bfloat16)
        x_out[:, cols] = normed
        logits += lax.dot_general(
            router[:, cols], normed, (((1,), (1,)), ((), ())), preferred_element_type=jnp.float32
        )
    labels = lax.broadcasted_iota(jnp.int32, logits.shape, 0)
    named = ids[0:1, :] == labels
    for k in range(1, TOP):
        named = named | (ids[k : k + 1, :] == labels)
    peak = jnp.max(jnp.where(named, logits, -jnp.inf), axis=0, keepdims=True)
    grown = jnp.where(named, jnp.exp(jnp.where(named, logits - peak, 0.0)), 0.0)
    probs = (grown / jnp.sum(grown, axis=0, keepdims=True)).astype(jnp.bfloat16)
    experts = router.shape[0]
    spread = (experts, 3 * PART - D)
    ones = lax.broadcasted_iota(jnp.int32, spread, 0) == lax.broadcasted_iota(jnp.int32, spread, 1)
    x_out[:, D:] = lax.dot_general(
        probs, ones.astype(jnp.float32).astype(jnp.bfloat16), (((0,), (0,)), ((), ())),
        preferred_element_type=jnp.float32,
    ).astype(jnp.bfloat16)

    everything.wait_send()
    sent(pair_out, "sum")
    sent(part.at[0, pl.ds(0, 2)], "a1")
    sent(part.at[0], "a2")
    sent(part.at[:, 0, pl.ds(0, 3)], "c")
    assert len(names.table) == 20


def attention_out(attended, resid, norm_gain, router, expert_ids, out_proj):
    bf = jnp.bfloat16
    vmem = pl.BlockSpec(memory_space=pltpu.VMEM)
    return pl.pallas_call(
        project_kernel,
        out_shape=(
            jax.ShapeDtypeStruct((16, D), jnp.float32),
            jax.ShapeDtypeStruct((16, 3 * PART), bf),
        ),
        in_specs=[vmem] + [pl.BlockSpec(memory_space=pl.ANY)] * 5,
        out_specs=(vmem, vmem),
        scratch_shapes=[
            pltpu.VMEM((16, D), bf),
            pltpu.VMEM((1, D), jnp.float32),
            pltpu.VMEM(router.shape[::-1], bf),
            pltpu.VMEM((TOP, 16), jnp.int32),
            pltpu.VMEM((256, D), bf),
            pltpu.VMEM((32, 16, 256), bf),
            pltpu.VMEM((2, 4, 4, 16, HALF), bf),
            pltpu.VMEM((2, 4, 4, 16, HALF), bf),
            pltpu.VMEM((2, 4, 4, 16, HALF), bf),
            pltpu.VMEM((2, 2, 2, 16, HALF), bf),
            pltpu.VMEM((2, 2, 4, 16, HALF), bf),
            pltpu.VMEM((2, 3, 16, HALF), bf),
            pltpu.SemaphoreType.DMA((4,)),
            pltpu.SemaphoreType.DMA((20,)),
            pltpu.SemaphoreType.DMA((1,)),
            pltpu.SemaphoreType.DMA((1,)),
            pltpu.SemaphoreType.DMA((5,)),
        ],
        compiler_params=pltpu.CompilerParams(
            collective_id=1, has_side_effects=True, vmem_limit_bytes=67043328
        ),
        name="attention_out",
    )(attended, resid, norm_gain.reshape(1, D), router.T, expert_ids.T, out_proj)


def local(
    resid,
    queries,
    new_keys,
    new_values,
    cache_keys,
    cache_values,
    cache_len,
    out_proj,
    norm_gain,
    router,
    expert_ids,
    gate_slab,
    up_slab,
    down_slab,
):
    attended = attend(queries, new_keys, new_values, cache_keys, cache_values, cache_len)
    hidden, x_in = attention_out(attended, resid, norm_gain, router, expert_ids, out_proj)
    return moe(x_in, hidden, gate_slab[0], up_slab[0], down_slab[0])


def solution(mesh):
    in_specs = (
        P(("ep", "dp"), None),
        P(("ep", "dp"), None),
        P(("ep", "dp"), None),
        P(("ep", "dp"), None),
        P(("ep", "dp"), None, None),
        P(("ep", "dp"), None, None),
        P(("ep", "dp")),
        P("ep", None),
        P(),
        P(),
        P(("ep", "dp"), None),
        P(("ep", "dp"), None, None),
        P(("ep", "dp"), None, None),
        P(("ep", "dp"), None, None),
    )
    out_specs = P(("ep", "dp"), None)
    return jax.shard_map(local, mesh=mesh, in_specs=in_specs, out_specs=out_specs, check_vma=False)
```

```python
import functools
import math

import jax
import jax.numpy as jnp
from jax import lax
from jax.experimental import pallas as pl
from jax.experimental.pallas import tpu as pltpu
from jax.sharding import PartitionSpec as P

D = 4096
H = 64
KVH = 4
HD = 128
TOP = 8
MESH = pl.DeviceIdType.MESH

PART = 1408
ORDER = (("x", "y", "z"), ("y", "z", "x"), ("z", "x", "y"))
HF = 384


def attend(queries, new_keys, new_values, cache_keys, cache_values, cache_len):
    local_rows = queries.shape[0]
    cache_span = cache_keys.shape[1]
    group_size = H // KVH
    query_heads = queries.reshape(local_rows, KVH, group_size, HD)
    past_keys = cache_keys.reshape(local_rows, cache_span, KVH, HD)
    past_values = cache_values.reshape(local_rows, cache_span, KVH, HD)
    score_scale = 1.0 / math.sqrt(HD)
    past_scores = (
        jnp.einsum("tgqd,tcgd->tgqc", query_heads, past_keys, preferred_element_type=jnp.float32)
        * score_scale
    )
    own_scores = (
        jnp.einsum(
            "tgqd,tgd->tgq",
            query_heads,
            new_keys.reshape(local_rows, KVH, HD),
            preferred_element_type=jnp.float32,
        )
        * score_scale
    )
    is_valid = lax.broadcasted_iota(jnp.int32, (local_rows, cache_span), 1) < cache_len[:, None]
    past_scores = jnp.where(is_valid[:, None, None, :], past_scores, -1e30)
    peak_score = jnp.maximum(jnp.max(past_scores, axis=3), own_scores)
    past_exp = jnp.exp(past_scores - peak_score[..., None])
    own_exp = jnp.exp(own_scores - peak_score)
    denom_sum = jnp.sum(past_exp, axis=3) + own_exp
    past_weights = (past_exp / denom_sum[..., None]).astype(jnp.bfloat16)
    own_weights = (own_exp / denom_sum).astype(jnp.bfloat16)
    blended = jnp.einsum(
        "tgqc,tcgd->tgqd", past_weights, past_values, preferred_element_type=jnp.float32
    )
    blended = blended + own_weights.astype(jnp.float32)[..., None] * new_values.reshape(
        local_rows, KVH, 1, HD
    ).astype(jnp.float32)
    return blended.reshape(local_rows, H * HD).astype(jnp.bfloat16)


class Place:
    def __init__(self):
        ep = lax.axis_index("ep")
        self.c = lax.rem(ep, 2)
        self.coord = {
            "x": lax.rem(lax.div(ep, 2), 4),
            "y": lax.div(ep, 8),
            "z": lax.axis_index("dp"),
        }

    def rel(self, dim, offset):
        if isinstance(offset, int) and offset == 0:
            return self.coord[dim]
        return lax.rem(self.coord[dim] + offset, 4)

    def device(self, dim=None, offset=0, other_core=False):
        at = dict(self.coord)
        if dim is not None:
            at[dim] = self.rel(dim, offset)
        core = 1 - self.c if other_core else self.c
        return ((at["y"] * 4 + at["x"]) * 2 + core, at["z"])


class Names:
    def __init__(self):
        self.table = {}

    def __call__(self, *key):
        return self.table.setdefault(key, len(self.table))


GROUPS = ("1", "2", "2g", "3", "3g", "pair", "a1", "a2", "b1", "b2", "c", ("sum", 0), ("sum", 1), ("sum", 2))
KEYS = 129


def moe_kernel(
    x_in, hidden, gate, up, down, out,
    residual, rows, gu, dn, acc, act, part, pair_out, pair_in, ra1, ra2, rb1, rb2, rc,
    send_sem, recv_sem, load_sem,
):
    here = Place()
    c = here.c
    other = 1 - c
    rel, device = here.rel, here.device
    names = Names()
    parts = range(3)
    dims = ORDER

    def send(src, dst, key, dev, group):
        copy = pltpu.make_async_remote_copy(
            src_ref=src, dst_ref=dst, send_sem=send_sem.at[GROUPS.index(group)], recv_sem=recv_sem.at[names(*key)],
            device_id=dev, device_id_type=MESH,
        )
        copy.start()
        return copy

    def landed(ref, key):
        pltpu.make_async_remote_copy(
            src_ref=ref, dst_ref=ref, send_sem=send_sem.at[0], recv_sem=recv_sem.at[names(*key)],
            device_id=device(other_core=True), device_id_type=MESH,
        ).wait_recv()

    def sent(ref, group):
        pltpu.make_async_remote_copy(
            src_ref=ref, dst_ref=ref, send_sem=send_sem.at[GROUPS.index(group)], recv_sem=recv_sem.at[0],
            device_id=device(other_core=True), device_id_type=MESH,
        ).wait_send()

    def amount(p, n):
        if n == 1:
            return rows.at[p, 0, 0, 0, 0]
        if n < 4:
            return rows.at[p, 0, 0, 0, pl.ds(0, n)]
        if n < 16:
            return rows.at[p, 0, 0, pl.ds(0, n // 4)]
        return rows.at[p, 0, pl.ds(0, n // 16)]

    def where(p, o1, o2, o3):
        at = {d: (slice(None) if o is None else rel(d, o)) for d, o in zip(ORDER[p], (o1, o2, o3))}
        return at["y"], at["x"], at["z"]

    def block(p, o1, o2, o3, core=None):
        return rows.at[(p, c if core is None else core) + where(p, o1, o2, o3)]

    def send_sub(p, j):
        ref = block(p, j, 0, 0)
        send(ref, ref, (p, "2", j), device(dims[p][1], 1), "2")
        send(ref, ref, (p, "2", j), device(dims[p][1], 3), "2")

    def send_line(p, j):
        ref = block(p, None, j, 0)
        send(ref, ref, (p, "3", j), device(dims[p][2], 1), "3")
        send(ref, ref, (p, "3", j), device(dims[p][2], 3), "3")

    def send_block(p, i, j):
        ref = block(p, i, j, 0)
        send(ref, ref, (p, "3", j), device(dims[p][2], 1), "3")
        send(ref, ref, (p, "3", j), device(dims[p][2], 3), "3")

    def unit(o2, o3):
        if o3 in (1, 3):
            return "near", o2
        if o3 == 0:
            return "own", (0, 1, 2, 1)[o2]
        return "far", o2 in (0, 1)

    def pass_on(p, o2, o3):
        ref = block(p, None, o2, o3)
        send(ref, ref, (p, "pair") + unit(o2, o3), device(other_core=True), "pair")

    def project(*lines):
        for p in parts:
            landed(amount(p, 4 * len(lines)), (p, "pair") + unit(*lines[0]))
            at = [where(p, None, o2, o3) for o2, o3 in lines]

            @pl.loop(0, 3, unroll=3)
            def _(n):
                cols = pl.ds(pl.multiple_of(n * 256, 256), 256)
                x = [rows[(p, slice(None)) + a].reshape(128, PART) for a in at]
                x = jnp.concatenate(x, axis=0)
                w = gu[p * PART : (p + 1) * PART, cols]
                y = jnp.dot(x, w, preferred_element_type=jnp.float32)
                for i, a in enumerate(at):
                    idx = (slice(None),) + a + (slice(None), cols)
                    acc[idx] += y[i * 128 : (i + 1) * 128].reshape(2, 4, 16, 256)

    barrier = pltpu.get_barrier_semaphore()
    for dim in ("x", "y", "z"):
        for o in (1, 2, 3):
            pl.semaphore_signal(barrier, inc=1, device_id=device(dim, o), device_id_type=MESH)
    pl.semaphore_signal(barrier, inc=1, device_id=device(other_core=True), device_id_type=MESH)

    fetch = pltpu.make_async_copy(hidden, residual, load_sem.at[3])
    fetch.start()
    starts = [
        pltpu.make_async_copy(x_in.at[:, pl.ds(p * PART, PART)], rows.at[(p, c) + where(p, 0, 0, 0)], load_sem.at[4 + p])
        for p in range(3)
    ]
    for copy in starts:
        copy.start()
    loads = [
        pltpu.make_async_copy(gate, gu.at[pl.ds(0, D), pl.ds(0, HF)], load_sem.at[0]),
        pltpu.make_async_copy(up, gu.at[pl.ds(0, D), pl.ds(HF, HF)], load_sem.at[1]),
        pltpu.make_async_copy(down, dn.at[:, pl.ds(0, D)], load_sem.at[2]),
    ]
    for copy in loads:
        copy.start()
    pl.semaphore_wait(barrier, 10)

    for copy in starts:
        copy.wait()
    fetch.wait()
    for p in parts:
        own = block(p, 0, 0, 0)
        for o in (1, 3):
            send(own, own, (p, "1n"), device(dims[p][0], o), "1")
        send(own, own, (p, "1f"), device(dims[p][0], 2), "1")
    for p in parts:
        send_sub(p, 0)

    gu[D:, :] = jnp.zeros((3 * PART - D, 2 * HF), jnp.bfloat16)
    dn[:, D:] = jnp.zeros((HF, 3 * PART - D), jnp.bfloat16)

    @pl.loop(0, 32)
    def _(i):
        acc[i // 16, lax.rem(i, 16) // 4, lax.rem(i, 4)] = jnp.zeros((4, 16, 2 * HF), jnp.float32)

    for p in parts:
        send_block(p, 0, 0)
    for p in parts:
        landed(amount(p, 2), (p, "1n"))
        send_sub(p, 1)
        send_sub(p, 3)
    for p in parts:
        landed(amount(p, 1), (p, "1f"))
        send_sub(p, 2)
    for p in parts:
        for i in (1, 3, 2):
            send_block(p, i, 0)
        pass_on(p, 0, 0)
    for copy in loads:
        copy.wait()
    project((0, 0))
    for j in (0, 1, 3, 2):
        for p in parts:
            landed(amount(p, 2), (p, "2", j))
            o = 3 if j in (0, 1) else 1
            ref = block(p, j, o, 0)
            send(ref, ref, (p, "2g"), device(dims[p][1], 4 - o), "2g")
            send_block(p, j, 1)
            send_block(p, j, 3)
    for p in parts:
        pass_on(p, 1, 0)
        pass_on(p, 3, 0)
    project((1, 0), (3, 0))
    for p in parts:
        landed(amount(p, 4), (p, "2g"))
        send_line(p, 2)
        pass_on(p, 2, 0)

    def neighbours(j):
        for p in parts:
            landed(amount(p, 8), (p, "3", j))
            o = 3 if j in (0, 3) else 1
            ref = block(p, None, j, o)
            send(ref, ref, (p, "3g", j in (0, 1)), device(dims[p][2], 4 - o), "3g")
            pass_on(p, j, 3)
            pass_on(p, j, 1)

    def opposite(*lines):
        for p in parts:
            landed(amount(p, 8), (p, "3g", lines[0] in (0, 1)))
            for j in lines:
                pass_on(p, j, 2)

    neighbours(0)
    project((2, 0))
    neighbours(1)
    project((0, 3), (0, 1))
    neighbours(3)
    project((1, 3), (1, 1))
    neighbours(2)
    project((3, 3), (3, 1))
    opposite(0, 1)
    project((2, 3), (2, 1))
    opposite(3, 2)
    project((0, 2), (1, 2))
    project((3, 2), (2, 2))

    expert = lax.div(lax.axis_index("ep") * 4 + lax.axis_index("dp"), 2)

    def activate(at):
        sums = acc[at].reshape(64, 2 * HF)
        tail = rows[(2,) + at + (slice(None), slice(PART - 128, PART))]
        tail = tail.reshape(64, 128).astype(jnp.float32)
        lanes = lax.broadcasted_iota(jnp.int32, (64, 128), 1)
        prob = jnp.sum(jnp.where(lanes == expert, tail, 0.0), axis=1, keepdims=True)
        g, u = sums[:, :HF], sums[:, HF:]
        h = (g * (0.5 + 0.5 * jnp.tanh(0.5 * g)) * u).astype(jnp.bfloat16).astype(jnp.float32) * prob
        act[at] = h.astype(jnp.bfloat16).reshape(4, 16, HF)

    every = slice(None)

    def activate_opposite(p):
        far = rel(dims[p][2], 2)

        @pl.loop(0, 8)
        def _(i):
            core, k = i // 4, lax.rem(i, 4)
            activate(((core, k, every, far), (core, k, far, every), (core, far, k, every))[p])

    def activate_rest():
        @pl.loop(0, 18)
        def _(i):
            k = lax.rem(i, 9)
            oy, ox = k // 3, lax.rem(k, 3)
            oy, ox = oy + oy // 2, ox + ox // 2
            activate((i // 9, rel("y", oy), rel("x", ox), every))

    def spot(p, o2, o3):
        a2 = slice(None) if o2 is None else rel(dims[p][1], o2)
        a3 = slice(None) if o3 is None else rel(dims[p][0], o3)
        return (a3, a2) if p == 1 else (a2, a3)

    def line(p, o1, o2):
        return part.at[(p, o1) + spot(p, o2, None)]

    def sub(p, o3):
        return part.at[(p, 0) + spot(p, 0, o3)]

    def hidden_of(p, o1, core):
        at = {d: (rel(d, o1) if d == dims[p][2] else slice(None)) for d in "xyz"}
        return act[core, at["y"], at["x"], at["z"]].reshape(256, HF)

    def product(p, o1):
        def piece(cols, wcols, width):
            h = jnp.concatenate([hidden_of(p, o1, other), hidden_of(p, o1, c)], axis=0)
            y = jnp.dot(h, dn[:, wcols], preferred_element_type=jnp.float32).astype(jnp.bfloat16)
            pair_out[p, :, :, :, cols] = y[:256].reshape(4, 4, 16, width)
            part[p, o1, :, :, :, cols] = y[256:].reshape(4, 4, 16, width)

        @pl.loop(0, 5, unroll=5)
        def _(n):
            start = pl.multiple_of(n * 256, 256)
            piece(pl.ds(start, 256), pl.ds(pl.multiple_of(p * PART + start, 128), 256), 256)

        if p < 2:
            piece(pl.ds(1280, 128), pl.ds(p * PART + 1280, 128), 128)
        else:
            pair_out[p, :, :, :, 1280:] = jnp.zeros((4, 4, 16, 128), jnp.bfloat16)
            part[p, o1, :, :, :, 1280:] = jnp.zeros((4, 4, 16, 128), jnp.bfloat16)

    def add(dst, *srcs):
        @pl.loop(0, 4)
        def _(i):
            total = dst[i].astype(jnp.float32)
            for s in srcs:
                total += s[i].astype(jnp.float32)
            dst[i] = total.astype(jnp.bfloat16)

    def add_sub(dst, *srcs):
        total = dst[...].astype(jnp.float32)
        for s in srcs:
            total += s[...].astype(jnp.float32)
        dst[...] = total.astype(jnp.bfloat16)

    last = {}

    def sums_for(o1, then, before=None):
        def finish(p):
            landed(pair_in.at[p, o1], (p, "sum", o1))

            @pl.loop(0, 4)
            def _(i):
                add(part.at[p, o1, i], pair_in.at[p, o1, i])

            then(p)

        for p in parts:
            if p in last:
                last[p].wait_send()
            if before is not None:
                before(p)
            product(p, o1)
            last[p] = send(pair_out.at[p], pair_in.at[p, o1], (p, "sum", o1), device(other_core=True), ("sum", p))
            if p:
                finish(p - 1)
        finish(2)

    def up_of(p, level):
        return device(dims[p][level], 1)

    def down_of(p, level):
        return device(dims[p][level], 3)

    UPWARD, DOWNWARD = (2, 1), (3, 0)

    def first(p):
        for k in range(2):
            send(line(p, 2, UPWARD[k]), ra1.at[p, 0, k], (p, "a1", 0, k), up_of(p, 2), "a1")
            send(line(p, 2, DOWNWARD[k]), ra1.at[p, 1, k], (p, "a1", 1, k), down_of(p, 2), "a1")

    def nothing(p):
        pass

    def second(direction, j):
        o1, joined = (1, UPWARD) if direction == 0 else (3, DOWNWARD)
        for p in parts:
            if j in joined:
                k = joined.index(j)
                landed(ra1.at[p, direction, k], (p, "a1", direction, k))
                add(line(p, o1, j), ra1.at[p, direction, k])
            send(line(p, o1, j), ra2.at[p, direction, j], (p, "a2", j), device(dims[p][2], o1), "a2")

    sums_for(2, first, activate_opposite)
    activate_rest()
    sums_for(1, nothing)
    sums_for(3, nothing)
    second(0, 2)
    second(1, 2)
    second(0, 1)
    second(1, 3)
    second(0, 3)
    second(1, 1)
    sums_for(0, nothing)

    def finish_line(p, j):
        landed(ra2.at[p, 0, pl.ds(0, 2)], (p, "a2", j))
        add(line(p, 0, j), ra2.at[p, 0, j], ra2.at[p, 1, j])

    def block_of(p, o2, o3):
        return part.at[(p, 0) + spot(p, o2, o3)]

    for p in parts:
        finish_line(p, 2)
        for k in range(2):
            send(block_of(p, 2, UPWARD[k]), rb1.at[p, 0, k], (p, "b1", 0, k), up_of(p, 1), "b1")
            send(block_of(p, 2, DOWNWARD[k]), rb1.at[p, 1, k], (p, "b1", 1, k), down_of(p, 1), "b1")
    second(0, 0)
    second(1, 0)
    for p in parts:
        finish_line(p, 3)
        for j in UPWARD:
            send(block_of(p, 3, j), rb2.at[p, 1, j], (p, "b2", j), down_of(p, 1), "b2")
    for p in parts:
        finish_line(p, 1)
        for j in DOWNWARD:
            send(block_of(p, 1, j), rb2.at[p, 0, j], (p, "b2", j), up_of(p, 1), "b2")
    for k in range(2):
        for p in parts:
            j = UPWARD[k]
            landed(rb1.at[p, 0, k], (p, "b1", 0, k))
            add_sub(block_of(p, 1, j), rb1.at[p, 0, k])
            send(block_of(p, 1, j), rb2.at[p, 0, j], (p, "b2", j), up_of(p, 1), "b2")
            j = DOWNWARD[k]
            landed(rb1.at[p, 1, k], (p, "b1", 1, k))
            add_sub(block_of(p, 3, j), rb1.at[p, 1, k])
            send(block_of(p, 3, j), rb2.at[p, 1, j], (p, "b2", j), down_of(p, 1), "b2")
    for p in parts:
        finish_line(p, 0)

    def finish_block(p, j):
        landed(rb2.at[p, 0, pl.ds(0, 2)], (p, "b2", j))
        add_sub(sub(p, j), rb2.at[p, 0, j], rb2.at[p, 1, j])

    for o in (2, 3, 1):
        for p in parts:
            finish_block(p, o)
            send(sub(p, o), rc.at[p, o - 1], (p, "c"), device(dims[p][0], o), "c")
    for p in parts:
        finish_block(p, 0)
    for p in parts:
        landed(rc.at[p], (p, "c"))
        total = sub(p, 0)[...].astype(jnp.float32)
        for o in (3, 1, 2):
            total += rc[p, o - 1].astype(jnp.float32)
        width = min(PART, D - p * PART)
        cols = slice(p * PART, p * PART + width)
        out[:, cols] = residual[:, cols] + total[:, :width]
    for group, n in (("1", 3), ("2", 8), ("2g", 4), ("3", 32), ("3g", 16), ("pair", 64)):
        sent(amount(slice(None), n), group)
    for group, n in (("a1", 16), ("a2", 32), ("b1", 4), ("b2", 8), ("c", 3)):
        sent(amount(slice(None), n), group)
    for p in parts:
        last[p].wait_send()
    assert len(names.table) == KEYS, len(names.table)


def moe(x_in, hidden, gate, up, down):
    bf = jnp.bfloat16
    vmem = pl.BlockSpec(memory_space=pltpu.VMEM)
    hbm = pl.BlockSpec(memory_space=pl.ANY)
    return pl.pallas_call(
        moe_kernel,
        out_shape=jax.ShapeDtypeStruct((16, D), jnp.float32),
        in_specs=[hbm] * 5,
        out_specs=vmem,
        scratch_shapes=[
            pltpu.VMEM((16, D), jnp.float32),
            pltpu.VMEM((3, 2, 4, 4, 4, 16, PART), bf),
            pltpu.VMEM((3 * PART, 2 * HF), bf),
            pltpu.VMEM((HF, 3 * PART), bf),
            pltpu.VMEM((2, 4, 4, 4, 16, 2 * HF), jnp.float32),
            pltpu.VMEM((2, 4, 4, 4, 16, HF), bf),
            pltpu.VMEM((3, 4, 4, 4, 16, PART), bf),
            pltpu.VMEM((3, 4, 4, 16, PART), bf),
            pltpu.VMEM((3, 4, 4, 4, 16, PART), bf),
            pltpu.VMEM((3, 2, 2, 4, 16, PART), bf),
            pltpu.VMEM((3, 2, 4, 4, 16, PART), bf),
            pltpu.VMEM((3, 2, 2, 16, PART), bf),
            pltpu.VMEM((3, 2, 4, 16, PART), bf),
            pltpu.VMEM((3, 3, 16, PART), bf),
            pltpu.SemaphoreType.DMA((len(GROUPS),)),
            pltpu.SemaphoreType.DMA((KEYS,)),
            pltpu.SemaphoreType.DMA((7,)),
        ],
        compiler_params=pltpu.CompilerParams(
            collective_id=0, has_side_effects=True, vmem_limit_bytes=67043328
        ),
        name="moe",
    )(x_in, hidden, gate, up, down)


HALF = D // 2


def project_kernel(
    att, resid_hbm, gain_hbm, router_hbm, ids_hbm, w_hbm, hidden_out, x_out,
    resid, gain, router, ids, w, seen, part, pair_out, pair_in, ra1, ra2, rc,
    send_sem, recv_sem, all_send, all_recv, load_sem,
):
    here = Place()
    c = here.c
    other = 1 - c
    rel, device = here.rel, here.device
    ep, dp = lax.axis_index("ep"), lax.axis_index("dp")
    names = Names()
    groups = ("sum", "a1", "a2", "c")
    loads = [
        pltpu.make_async_copy(src, dst, load_sem.at[i])
        for i, (src, dst) in enumerate(
            ((w_hbm, w), (resid_hbm, resid), (gain_hbm, gain), (router_hbm, router), (ids_hbm, ids))
        )
    ]
    for copy in loads:
        copy.start()

    def send(src, dst, key, dev):
        pltpu.make_async_remote_copy(
            src_ref=src, dst_ref=dst, send_sem=send_sem.at[groups.index(key[1])], recv_sem=recv_sem.at[names(*key)],
            device_id=dev, device_id_type=MESH,
        ).start()

    def landed(ref, key):
        pltpu.make_async_remote_copy(
            src_ref=ref, dst_ref=ref, send_sem=send_sem.at[0], recv_sem=recv_sem.at[names(*key)],
            device_id=device(other_core=True), device_id_type=MESH,
        ).wait_recv()

    def sent(ref, group):
        pltpu.make_async_remote_copy(
            src_ref=ref, dst_ref=ref, send_sem=send_sem.at[groups.index(group)], recv_sem=recv_sem.at[0],
            device_id=device(other_core=True), device_id_type=MESH,
        ).wait_send()

    def slot(e):
        return lax.rem(e, 2) * 16 + lax.div(e, 2)

    barrier = pltpu.get_barrier_semaphore()
    for k in range(1, 32):
        pl.semaphore_signal(barrier, inc=1, device_id=(lax.rem(ep + k, 32), dp), device_id_type=MESH)
    seen[slot(ep)] = att[:, pl.ds(pl.multiple_of(ep * 256, 256), 256)]
    pl.semaphore_wait(barrier, 31)

    for k in range(1, 32):
        to = lax.rem(ep + k, 32)
        pltpu.make_async_remote_copy(
            src_ref=att.at[:, pl.ds(pl.multiple_of(to * 256, 256), 256)],
            dst_ref=seen.at[slot(ep)],
            send_sem=all_send.at[0],
            recv_sem=all_recv.at[0],
            device_id=(to, dp),
            device_id_type=MESH,
        ).start()
    everything = pltpu.make_async_remote_copy(
        src_ref=seen.at[pl.ds(0, 31)], dst_ref=seen.at[pl.ds(0, 31)],
        send_sem=all_send.at[0], recv_sem=all_recv.at[0],
        device_id=device(other_core=True), device_id_type=MESH,
    )
    loads[0].wait()
    everything.wait_recv()

    first_dim = ("x", "y")
    second_dim = ("y", "x")

    def spot(q, o1, o2):
        at = {first_dim[q]: rel(first_dim[q], o1), second_dim[q]: rel(second_dim[q], o2)}
        return part.at[q, at["y"], at["x"]]

    def product(q):
        @pl.loop(0, HALF // 256, unroll=4)
        def _(n):
            start = pl.multiple_of(n * 256, 256)
            theirs = seen[pl.ds(other * 16, 16)].reshape(256, 256)
            ours = seen[pl.ds(c * 16, 16)].reshape(256, 256)
            rows = jnp.concatenate([theirs, ours], axis=0)
            cols = pl.ds(pl.multiple_of(q * HALF + start, 256), 256)
            y = jnp.dot(rows, w[:, cols], preferred_element_type=jnp.float32).astype(jnp.bfloat16)
            pair_out[q, :, :, :, pl.ds(start, 256)] = y[:256].reshape(4, 4, 16, 256)
            part[q, :, :, :, pl.ds(start, 256)] = y[256:].reshape(4, 4, 16, 256)

    def add(dst, *srcs):
        total = dst[...].astype(jnp.float32)
        for src in srcs:
            total += src[...].astype(jnp.float32)
        dst[...] = total.astype(jnp.bfloat16)

    UPWARD, DOWNWARD = (2, 1), (3, 0)
    for q in range(2):
        product(q)
    for o1 in (2, 1, 3, 0):
        for q in range(2):
            far = rel(first_dim[q], o1)
            mine = (q, slice(None), far) if q == 0 else (q, far)
            send(pair_out.at[mine], pair_in.at[mine], (q, "sum", o1), device(other_core=True))

    def join(o1):
        for q in range(2):
            landed(pair_in.at[q, 0], (q, "sum", o1))
            for o2 in (2, 3, 1, 0):
                at = {first_dim[q]: rel(first_dim[q], o1), second_dim[q]: rel(second_dim[q], o2)}
                add(spot(q, o1, o2), pair_in.at[q, at["y"], at["x"]])
                if o1 == 2:
                    way = 0 if o2 in UPWARD else 1
                    n = (UPWARD, DOWNWARD)[way].index(o2)
                    send(spot(q, 2, o2), ra1.at[q, way, n], (q, "a1", way, n), device(first_dim[q], 1 + 2 * way))

    join(2)
    join(1)
    join(3)

    def second(direction, j):
        for q in range(2):
            o1, joined = (1, UPWARD) if direction == 0 else (3, DOWNWARD)
            if j in joined:
                k = joined.index(j)
                landed(ra1.at[q, direction, k], (q, "a1", direction, k))
                add(spot(q, o1, j), ra1.at[q, direction, k])
            send(spot(q, o1, j), ra2.at[q, direction, j], (q, "a2", j), device(first_dim[q], o1))

    for up_block, down_block in ((3, 2), (2, 3), (1, 1), (0, 0)):
        second(0, up_block)
        second(1, down_block)
    join(0)

    def finish(q, j):
        landed(ra2.at[q, 0, pl.ds(0, 2)], (q, "a2", j))
        add(spot(q, 0, j), ra2.at[q, 0, j], ra2.at[q, 1, j])

    for o in (2, 3, 1):
        for q in range(2):
            finish(q, o)
            send(spot(q, 0, o), rc.at[q, o - 1], (q, "c"), device(second_dim[q], o))
    for q in range(2):
        finish(q, 0)
    for copy in loads[1:]:
        copy.wait()
    square = jnp.zeros((16, 1), jnp.float32)
    for q in range(2):
        landed(rc.at[q], (q, "c"))
        total = spot(q, 0, 0)[...].astype(jnp.float32)
        for o in (3, 1, 2):
            total += rc[q, o - 1].astype(jnp.float32)
        cols = slice(q * HALF, (q + 1) * HALF)
        hidden = resid[:, cols].astype(jnp.float32) + total
        hidden_out[:, cols] = hidden
        square += jnp.sum(hidden * hidden, axis=1, keepdims=True)
    scale = lax.rsqrt(jnp.maximum(square * (1.0 / D), 0.25))
    logits = jnp.zeros((router.shape[0], 16), jnp.float32)
    for q in range(2):
        cols = slice(q * HALF, (q + 1) * HALF)
        normed = (hidden_out[:, cols] * scale * gain[:, cols]).astype(jnp.bfloat16)
        x_out[:, cols] = normed
        logits += lax.dot_general(
            router[:, cols], normed, (((1,), (1,)), ((), ())), preferred_element_type=jnp.float32
        )
    labels = lax.broadcasted_iota(jnp.int32, logits.shape, 0)
    named = ids[0:1, :] == labels
    for k in range(1, TOP):
        named = named | (ids[k : k + 1, :] == labels)
    peak = jnp.max(jnp.where(named, logits, -jnp.inf), axis=0, keepdims=True)
    grown = jnp.where(named, jnp.exp(jnp.where(named, logits - peak, 0.0)), 0.0)
    probs = (grown / jnp.sum(grown, axis=0, keepdims=True)).astype(jnp.bfloat16)
    experts = router.shape[0]
    spread = (experts, 3 * PART - D)
    ones = lax.broadcasted_iota(jnp.int32, spread, 0) == lax.broadcasted_iota(jnp.int32, spread, 1)
    x_out[:, D:] = lax.dot_general(
        probs, ones.astype(jnp.float32).astype(jnp.bfloat16), (((0,), (0,)), ((), ())),
        preferred_element_type=jnp.float32,
    ).astype(jnp.bfloat16)

    everything.wait_send()
    sent(pair_out, "sum")
    sent(part.at[0, pl.ds(0, 2)], "a1")
    sent(part.at[0], "a2")
    sent(part.at[:, 0, pl.ds(0, 3)], "c")
    assert len(names.table) == 26


def attention_out(attended, resid, norm_gain, router, expert_ids, out_proj):
    bf = jnp.bfloat16
    vmem = pl.BlockSpec(memory_space=pltpu.VMEM)
    return pl.pallas_call(
        project_kernel,
        out_shape=(
            jax.ShapeDtypeStruct((16, D), jnp.float32),
            jax.ShapeDtypeStruct((16, 3 * PART), bf),
        ),
        in_specs=[vmem] + [pl.BlockSpec(memory_space=pl.ANY)] * 5,
        out_specs=(vmem, vmem),
        scratch_shapes=[
            pltpu.VMEM((16, D), bf),
            pltpu.VMEM((1, D), jnp.float32),
            pltpu.VMEM(router.shape[::-1], bf),
            pltpu.VMEM((TOP, 16), jnp.int32),
            pltpu.VMEM((256, D), bf),
            pltpu.VMEM((32, 16, 256), bf),
            pltpu.VMEM((2, 4, 4, 16, HALF), bf),
            pltpu.VMEM((2, 4, 4, 16, HALF), bf),
            pltpu.VMEM((2, 4, 4, 16, HALF), bf),
            pltpu.VMEM((2, 2, 2, 16, HALF), bf),
            pltpu.VMEM((2, 2, 4, 16, HALF), bf),
            pltpu.VMEM((2, 3, 16, HALF), bf),
            pltpu.SemaphoreType.DMA((4,)),
            pltpu.SemaphoreType.DMA((26,)),
            pltpu.SemaphoreType.DMA((1,)),
            pltpu.SemaphoreType.DMA((1,)),
            pltpu.SemaphoreType.DMA((5,)),
        ],
        compiler_params=pltpu.CompilerParams(
            collective_id=1, has_side_effects=True, vmem_limit_bytes=67043328
        ),
        name="attention_out",
    )(attended, resid, norm_gain.reshape(1, D), router.T, expert_ids.T, out_proj)


def local(
    resid,
    queries,
    new_keys,
    new_values,
    cache_keys,
    cache_values,
    cache_len,
    out_proj,
    norm_gain,
    router,
    expert_ids,
    gate_slab,
    up_slab,
    down_slab,
):
    attended = attend(queries, new_keys, new_values, cache_keys, cache_values, cache_len)
    hidden, x_in = attention_out(attended, resid, norm_gain, router, expert_ids, out_proj)
    return moe(x_in, hidden, gate_slab[0], up_slab[0], down_slab[0])


def solution(mesh):
    in_specs = (
        P(("ep", "dp"), None),
        P(("ep", "dp"), None),
        P(("ep", "dp"), None),
        P(("ep", "dp"), None),
        P(("ep", "dp"), None, None),
        P(("ep", "dp"), None, None),
        P(("ep", "dp")),
        P("ep", None),
        P(),
        P(),
        P(("ep", "dp"), None),
        P(("ep", "dp"), None, None),
        P(("ep", "dp"), None, None),
        P(("ep", "dp"), None, None),
    )
    out_specs = P(("ep", "dp"), None)
    return jax.shard_map(local, mesh=mesh, in_specs=in_specs, out_specs=out_specs, check_vma=False)
```

```python
import functools
import math

import jax
import jax.numpy as jnp
from jax import lax
from jax.experimental import pallas as pl
from jax.experimental.pallas import tpu as pltpu
from jax.sharding import PartitionSpec as P

D = 4096
H = 64
KVH = 4
HD = 128
TOP = 8
MESH = pl.DeviceIdType.MESH

PART = 1408
ORDER = (("x", "y", "z"), ("y", "z", "x"), ("z", "x", "y"))
HF = 384


def attend(lengths, keys, values, q32, own_keys, own_values, blended32, arrived):
    group = H // KVH
    scale = 1.0 / math.sqrt(HD)

    def token(t):
        position = lax.broadcasted_iota(jnp.int32, (group, keys.shape[1]), 1)
        kept = position < lengths[t]
        for g in range(KVH):
            cols = slice(g * HD, (g + 1) * HD)
            heads = pl.ds(g * group * 16 + t, group, stride=16)
            q = q32[heads, :]
            scores = lax.dot_general(
                q.astype(jnp.bfloat16), keys[t, :, cols], (((1,), (1,)), ((), ())),
                preferred_element_type=jnp.float32,
            )
            scores = jnp.where(kept, scores * scale, -1e30)
            own = jnp.sum(q * own_keys[pl.ds(t, 1), cols], axis=1, keepdims=True) * scale
            peak = jnp.maximum(jnp.max(scores, axis=1, keepdims=True), own)
            grown, own_grown = jnp.exp(scores - peak), jnp.exp(own - peak)
            total = jnp.sum(grown, axis=1, keepdims=True) + own_grown
            weights = (grown / total).astype(jnp.bfloat16)
            own_weight = (own_grown / total).astype(jnp.bfloat16).astype(jnp.float32)
            mixed = jnp.dot(weights, values[t, :, cols], preferred_element_type=jnp.float32)
            blended32[heads, :] = mixed + own_weight * own_values[pl.ds(t, 1), cols]

    for chunk in range(4):
        arrived(chunk)

        @pl.loop(4 * chunk, 4 * chunk + 4, unroll=4)
        def _(t):
            token(t)


class Place:
    def __init__(self):
        ep = lax.axis_index("ep")
        self.c = lax.rem(ep, 2)
        self.coord = {
            "x": lax.rem(lax.div(ep, 2), 4),
            "y": lax.div(ep, 8),
            "z": lax.axis_index("dp"),
        }

    def rel(self, dim, offset):
        if isinstance(offset, int) and offset == 0:
            return self.coord[dim]
        return lax.rem(self.coord[dim] + offset, 4)

    def device(self, dim=None, offset=0, other_core=False):
        at = dict(self.coord)
        if dim is not None:
            at[dim] = self.rel(dim, offset)
        core = 1 - self.c if other_core else self.c
        return ((at["y"] * 4 + at["x"]) * 2 + core, at["z"])


class Names:
    def __init__(self):
        self.table = {}

    def __call__(self, *key):
        return self.table.setdefault(key, len(self.table))


GROUPS = ("1", "2", "2g", "3", "3g", "pair", "a1", "a2", "b1", "b2", "c", ("sum", 0), ("sum", 1), ("sum", 2))
KEYS = 129


def moe_kernel(
    x_in, hidden, gate, up, down, out,
    residual, rows, gu, dn, acc, act, part, pair_out, pair_in, ra1, ra2, rb1, rb2, rc,
    send_sem, recv_sem, load_sem,
):
    here = Place()
    c = here.c
    other = 1 - c
    rel, device = here.rel, here.device
    names = Names()
    parts = range(3)
    dims = ORDER

    def send(src, dst, key, dev, group):
        copy = pltpu.make_async_remote_copy(
            src_ref=src, dst_ref=dst, send_sem=send_sem.at[GROUPS.index(group)], recv_sem=recv_sem.at[names(*key)],
            device_id=dev, device_id_type=MESH,
        )
        copy.start()
        return copy

    def landed(ref, key):
        pltpu.make_async_remote_copy(
            src_ref=ref, dst_ref=ref, send_sem=send_sem.at[0], recv_sem=recv_sem.at[names(*key)],
            device_id=device(other_core=True), device_id_type=MESH,
        ).wait_recv()

    def sent(ref, group):
        pltpu.make_async_remote_copy(
            src_ref=ref, dst_ref=ref, send_sem=send_sem.at[GROUPS.index(group)], recv_sem=recv_sem.at[0],
            device_id=device(other_core=True), device_id_type=MESH,
        ).wait_send()

    def amount(p, n):
        if n == 1:
            return rows.at[p, 0, 0, 0, 0]
        if n < 4:
            return rows.at[p, 0, 0, 0, pl.ds(0, n)]
        if n < 16:
            return rows.at[p, 0, 0, pl.ds(0, n // 4)]
        return rows.at[p, 0, pl.ds(0, n // 16)]

    def where(p, o1, o2, o3):
        at = {d: (slice(None) if o is None else rel(d, o)) for d, o in zip(ORDER[p], (o1, o2, o3))}
        return at["y"], at["x"], at["z"]

    def block(p, o1, o2, o3, core=None):
        return rows.at[(p, c if core is None else core) + where(p, o1, o2, o3)]

    def send_sub(p, j):
        ref = block(p, j, 0, 0)
        send(ref, ref, (p, "2", j), device(dims[p][1], 1), "2")
        send(ref, ref, (p, "2", j), device(dims[p][1], 3), "2")

    def send_line(p, j):
        ref = block(p, None, j, 0)
        send(ref, ref, (p, "3", j), device(dims[p][2], 1), "3")
        send(ref, ref, (p, "3", j), device(dims[p][2], 3), "3")

    def send_block(p, i, j):
        ref = block(p, i, j, 0)
        send(ref, ref, (p, "3", j), device(dims[p][2], 1), "3")
        send(ref, ref, (p, "3", j), device(dims[p][2], 3), "3")

    def unit(o2, o3):
        if o3 in (1, 3):
            return "near", o2
        if o3 == 0:
            return "own", (0, 1, 2, 1)[o2]
        return "far", o2 in (0, 1)

    def pass_on(p, o2, o3):
        ref = block(p, None, o2, o3)
        send(ref, ref, (p, "pair") + unit(o2, o3), device(other_core=True), "pair")

    def project(*lines):
        for p in parts:
            landed(amount(p, 4 * len(lines)), (p, "pair") + unit(*lines[0]))
            at = [where(p, None, o2, o3) for o2, o3 in lines]

            @pl.loop(0, 3, unroll=3)
            def _(n):
                cols = pl.ds(pl.multiple_of(n * 256, 256), 256)
                x = [rows[(p, slice(None)) + a].reshape(128, PART) for a in at]
                x = jnp.concatenate(x, axis=0)
                w = gu[p * PART : (p + 1) * PART, cols]
                y = jnp.dot(x, w, preferred_element_type=jnp.float32)
                for i, a in enumerate(at):
                    idx = (slice(None),) + a + (slice(None), cols)
                    acc[idx] += y[i * 128 : (i + 1) * 128].reshape(2, 4, 16, 256)

    barrier = pltpu.get_barrier_semaphore()
    for dim in ("x", "y", "z"):
        for o in (1, 2, 3):
            pl.semaphore_signal(barrier, inc=1, device_id=device(dim, o), device_id_type=MESH)
    pl.semaphore_signal(barrier, inc=1, device_id=device(other_core=True), device_id_type=MESH)

    fetch = pltpu.make_async_copy(hidden, residual, load_sem.at[3])
    fetch.start()
    starts = [
        pltpu.make_async_copy(x_in.at[:, pl.ds(p * PART, PART)], rows.at[(p, c) + where(p, 0, 0, 0)], load_sem.at[4 + p])
        for p in range(3)
    ]
    for copy in starts:
        copy.start()
    loads = [
        pltpu.make_async_copy(gate, gu.at[pl.ds(0, D), pl.ds(0, HF)], load_sem.at[0]),
        pltpu.make_async_copy(up, gu.at[pl.ds(0, D), pl.ds(HF, HF)], load_sem.at[1]),
        pltpu.make_async_copy(down, dn.at[:, pl.ds(0, D)], load_sem.at[2]),
    ]
    for copy in loads:
        copy.start()
    pl.semaphore_wait(barrier, 10)

    for copy in starts:
        copy.wait()
    fetch.wait()
    for p in parts:
        own = block(p, 0, 0, 0)
        for o in (1, 3):
            send(own, own, (p, "1n"), device(dims[p][0], o), "1")
        send(own, own, (p, "1f"), device(dims[p][0], 2), "1")
    for p in parts:
        send_sub(p, 0)

    gu[D:, :] = jnp.zeros((3 * PART - D, 2 * HF), jnp.bfloat16)
    dn[:, D:] = jnp.zeros((HF, 3 * PART - D), jnp.bfloat16)

    @pl.loop(0, 32)
    def _(i):
        acc[i // 16, lax.rem(i, 16) // 4, lax.rem(i, 4)] = jnp.zeros((4, 16, 2 * HF), jnp.float32)

    for p in parts:
        send_block(p, 0, 0)
    for p in parts:
        landed(amount(p, 2), (p, "1n"))
        send_sub(p, 1)
        send_sub(p, 3)
    for p in parts:
        landed(amount(p, 1), (p, "1f"))
        send_sub(p, 2)
    for p in parts:
        for i in (1, 3, 2):
            send_block(p, i, 0)
        pass_on(p, 0, 0)
    for copy in loads:
        copy.wait()
    project((0, 0))
    for j in (0, 1, 3, 2):
        for p in parts:
            landed(amount(p, 2), (p, "2", j))
            o = 3 if j in (0, 1) else 1
            ref = block(p, j, o, 0)
            send(ref, ref, (p, "2g"), device(dims[p][1], 4 - o), "2g")
            send_block(p, j, 1)
            send_block(p, j, 3)
    for p in parts:
        pass_on(p, 1, 0)
        pass_on(p, 3, 0)
    project((1, 0), (3, 0))
    for p in parts:
        landed(amount(p, 4), (p, "2g"))
        send_line(p, 2)
        pass_on(p, 2, 0)

    def neighbours(j):
        for p in parts:
            landed(amount(p, 8), (p, "3", j))
            o = 3 if j in (0, 3) else 1
            ref = block(p, None, j, o)
            send(ref, ref, (p, "3g", j in (0, 1)), device(dims[p][2], 4 - o), "3g")
            pass_on(p, j, 3)
            pass_on(p, j, 1)

    def opposite(*lines):
        for p in parts:
            landed(amount(p, 8), (p, "3g", lines[0] in (0, 1)))
            for j in lines:
                pass_on(p, j, 2)

    neighbours(0)
    project((2, 0))
    neighbours(1)
    project((0, 3), (0, 1))
    neighbours(3)
    project((1, 3), (1, 1))
    neighbours(2)
    project((3, 3), (3, 1))
    opposite(0, 1)
    project((2, 3), (2, 1))
    opposite(3, 2)
    project((0, 2), (1, 2))
    project((3, 2), (2, 2))

    expert = lax.div(lax.axis_index("ep") * 4 + lax.axis_index("dp"), 2)

    def activate(at):
        sums = acc[at].reshape(64, 2 * HF)
        tail = rows[(2,) + at + (slice(None), slice(PART - 128, PART))]
        tail = tail.reshape(64, 128).astype(jnp.float32)
        lanes = lax.broadcasted_iota(jnp.int32, (64, 128), 1)
        prob = jnp.sum(jnp.where(lanes == expert, tail, 0.0), axis=1, keepdims=True)
        g, u = sums[:, :HF], sums[:, HF:]
        h = (g * (0.5 + 0.5 * jnp.tanh(0.5 * g)) * u).astype(jnp.bfloat16).astype(jnp.float32) * prob
        act[at] = h.astype(jnp.bfloat16).reshape(4, 16, HF)

    every = slice(None)

    def activate_opposite(p):
        far = rel(dims[p][2], 2)

        @pl.loop(0, 8)
        def _(i):
            core, k = i // 4, lax.rem(i, 4)
            activate(((core, k, every, far), (core, k, far, every), (core, far, k, every))[p])

    def activate_rest():
        @pl.loop(0, 18)
        def _(i):
            k = lax.rem(i, 9)
            oy, ox = k // 3, lax.rem(k, 3)
            oy, ox = oy + oy // 2, ox + ox // 2
            activate((i // 9, rel("y", oy), rel("x", ox), every))

    def spot(p, o2, o3):
        a2 = slice(None) if o2 is None else rel(dims[p][1], o2)
        a3 = slice(None) if o3 is None else rel(dims[p][0], o3)
        return (a3, a2) if p == 1 else (a2, a3)

    def line(p, o1, o2):
        return part.at[(p, o1) + spot(p, o2, None)]

    def sub(p, o3):
        return part.at[(p, 0) + spot(p, 0, o3)]

    def hidden_of(p, o1, core):
        at = {d: (rel(d, o1) if d == dims[p][2] else slice(None)) for d in "xyz"}
        return act[core, at["y"], at["x"], at["z"]].reshape(256, HF)

    def product(p, o1):
        def piece(cols, wcols, width):
            h = jnp.concatenate([hidden_of(p, o1, other), hidden_of(p, o1, c)], axis=0)
            y = jnp.dot(h, dn[:, wcols], preferred_element_type=jnp.float32).astype(jnp.bfloat16)
            pair_out[p, :, :, :, cols] = y[:256].reshape(4, 4, 16, width)
            part[p, o1, :, :, :, cols] = y[256:].reshape(4, 4, 16, width)

        @pl.loop(0, 5, unroll=5)
        def _(n):
            start = pl.multiple_of(n * 256, 256)
            piece(pl.ds(start, 256), pl.ds(pl.multiple_of(p * PART + start, 128), 256), 256)

        if p < 2:
            piece(pl.ds(1280, 128), pl.ds(p * PART + 1280, 128), 128)
        else:
            pair_out[p, :, :, :, 1280:] = jnp.zeros((4, 4, 16, 128), jnp.bfloat16)
            part[p, o1, :, :, :, 1280:] = jnp.zeros((4, 4, 16, 128), jnp.bfloat16)

    def add(dst, *srcs):
        @pl.loop(0, 4)
        def _(i):
            total = dst[i].astype(jnp.float32)
            for s in srcs:
                total += s[i].astype(jnp.float32)
            dst[i] = total.astype(jnp.bfloat16)

    def add_sub(dst, *srcs):
        total = dst[...].astype(jnp.float32)
        for s in srcs:
            total += s[...].astype(jnp.float32)
        dst[...] = total.astype(jnp.bfloat16)

    last = {}

    def sums_for(o1, then, before=None):
        def finish(p):
            landed(pair_in.at[p, o1], (p, "sum", o1))

            @pl.loop(0, 4)
            def _(i):
                add(part.at[p, o1, i], pair_in.at[p, o1, i])

            then(p)

        for p in parts:
            if p in last:
                last[p].wait_send()
            if before is not None:
                before(p)
            product(p, o1)
            last[p] = send(pair_out.at[p], pair_in.at[p, o1], (p, "sum", o1), device(other_core=True), ("sum", p))
            if p:
                finish(p - 1)
        finish(2)

    def up_of(p, level):
        return device(dims[p][level], 1)

    def down_of(p, level):
        return device(dims[p][level], 3)

    UPWARD, DOWNWARD = (2, 1), (3, 0)

    def first(p):
        for k in range(2):
            send(line(p, 2, UPWARD[k]), ra1.at[p, 0, k], (p, "a1", 0, k), up_of(p, 2), "a1")
            send(line(p, 2, DOWNWARD[k]), ra1.at[p, 1, k], (p, "a1", 1, k), down_of(p, 2), "a1")

    def nothing(p):
        pass

    def second(direction, j):
        o1, joined = (1, UPWARD) if direction == 0 else (3, DOWNWARD)
        for p in parts:
            if j in joined:
                k = joined.index(j)
                landed(ra1.at[p, direction, k], (p, "a1", direction, k))
                add(line(p, o1, j), ra1.at[p, direction, k])
            send(line(p, o1, j), ra2.at[p, direction, j], (p, "a2", j), device(dims[p][2], o1), "a2")

    sums_for(2, first, activate_opposite)
    activate_rest()
    sums_for(1, nothing)
    sums_for(3, nothing)
    second(0, 2)
    second(1, 2)
    second(0, 1)
    second(1, 3)
    second(0, 3)
    second(1, 1)
    sums_for(0, nothing)

    def finish_line(p, j):
        landed(ra2.at[p, 0, pl.ds(0, 2)], (p, "a2", j))
        add(line(p, 0, j), ra2.at[p, 0, j], ra2.at[p, 1, j])

    def block_of(p, o2, o3):
        return part.at[(p, 0) + spot(p, o2, o3)]

    for p in parts:
        finish_line(p, 2)
        for k in range(2):
            send(block_of(p, 2, UPWARD[k]), rb1.at[p, 0, k], (p, "b1", 0, k), up_of(p, 1), "b1")
            send(block_of(p, 2, DOWNWARD[k]), rb1.at[p, 1, k], (p, "b1", 1, k), down_of(p, 1), "b1")
    second(0, 0)
    second(1, 0)
    for p in parts:
        finish_line(p, 3)
        for j in UPWARD:
            send(block_of(p, 3, j), rb2.at[p, 1, j], (p, "b2", j), down_of(p, 1), "b2")
    for p in parts:
        finish_line(p, 1)
        for j in DOWNWARD:
            send(block_of(p, 1, j), rb2.at[p, 0, j], (p, "b2", j), up_of(p, 1), "b2")
    for k in range(2):
        for p in parts:
            j = UPWARD[k]
            landed(rb1.at[p, 0, k], (p, "b1", 0, k))
            add_sub(block_of(p, 1, j), rb1.at[p, 0, k])
            send(block_of(p, 1, j), rb2.at[p, 0, j], (p, "b2", j), up_of(p, 1), "b2")
            j = DOWNWARD[k]
            landed(rb1.at[p, 1, k], (p, "b1", 1, k))
            add_sub(block_of(p, 3, j), rb1.at[p, 1, k])
            send(block_of(p, 3, j), rb2.at[p, 1, j], (p, "b2", j), down_of(p, 1), "b2")
    for p in parts:
        finish_line(p, 0)

    def finish_block(p, j):
        landed(rb2.at[p, 0, pl.ds(0, 2)], (p, "b2", j))
        add_sub(sub(p, j), rb2.at[p, 0, j], rb2.at[p, 1, j])

    for o in (2, 3, 1):
        for p in parts:
            finish_block(p, o)
            send(sub(p, o), rc.at[p, o - 1], (p, "c"), device(dims[p][0], o), "c")
    for p in parts:
        finish_block(p, 0)
    for p in parts:
        landed(rc.at[p], (p, "c"))
        total = sub(p, 0)[...].astype(jnp.float32)
        for o in (3, 1, 2):
            total += rc[p, o - 1].astype(jnp.float32)
        width = min(PART, D - p * PART)
        cols = slice(p * PART, p * PART + width)
        out[:, cols] = residual[:, cols] + total[:, :width]
    for group, n in (("1", 3), ("2", 8), ("2g", 4), ("3", 32), ("3g", 16), ("pair", 64)):
        sent(amount(slice(None), n), group)
    for group, n in (("a1", 16), ("a2", 32), ("b1", 4), ("b2", 8), ("c", 3)):
        sent(amount(slice(None), n), group)
    for p in parts:
        last[p].wait_send()
    assert len(names.table) == KEYS, len(names.table)


def moe(x_in, hidden, gate, up, down):
    bf = jnp.bfloat16
    vmem = pl.BlockSpec(memory_space=pltpu.VMEM)
    hbm = pl.BlockSpec(memory_space=pl.ANY)
    return pl.pallas_call(
        moe_kernel,
        out_shape=jax.ShapeDtypeStruct((16, D), jnp.float32),
        in_specs=[hbm] * 5,
        out_specs=vmem,
        scratch_shapes=[
            pltpu.VMEM((16, D), jnp.float32),
            pltpu.VMEM((3, 2, 4, 4, 4, 16, PART), bf),
            pltpu.VMEM((3 * PART, 2 * HF), bf),
            pltpu.VMEM((HF, 3 * PART), bf),
            pltpu.VMEM((2, 4, 4, 4, 16, 2 * HF), jnp.float32),
            pltpu.VMEM((2, 4, 4, 4, 16, HF), bf),
            pltpu.VMEM((3, 4, 4, 4, 16, PART), bf),
            pltpu.VMEM((3, 4, 4, 16, PART), bf),
            pltpu.VMEM((3, 4, 4, 4, 16, PART), bf),
            pltpu.VMEM((3, 2, 2, 4, 16, PART), bf),
            pltpu.VMEM((3, 2, 4, 4, 16, PART), bf),
            pltpu.VMEM((3, 2, 2, 16, PART), bf),
            pltpu.VMEM((3, 2, 4, 16, PART), bf),
            pltpu.VMEM((3, 3, 16, PART), bf),
            pltpu.SemaphoreType.DMA((len(GROUPS),)),
            pltpu.SemaphoreType.DMA((KEYS,)),
            pltpu.SemaphoreType.DMA((7,)),
        ],
        compiler_params=pltpu.CompilerParams(
            collective_id=0, has_side_effects=True, vmem_limit_bytes=67043328
        ),
        name="moe",
    )(x_in, hidden, gate, up, down)


HALF = D // 2


def project_kernel(
    lengths, q_hbm, nk_hbm, nv_hbm, key_hbm, value_hbm, resid_hbm, gain_hbm, router_hbm, ids_hbm, w_hbm, hidden_out, x_out,
    q, nk, nv, keys, values, q32, own_keys, own_values, blended32, att,
    resid, gain, router, ids, w, seen, part, pair_out, pair_in, ra1, ra2, rc,
    send_sem, recv_sem, all_send, all_recv, load_sem,
):
    here = Place()
    c = here.c
    other = 1 - c
    rel, device = here.rel, here.device
    ep, dp = lax.axis_index("ep"), lax.axis_index("dp")
    names = Names()
    groups = ("sum", "a1", "a2", "c")
    loads = [
        pltpu.make_async_copy(src, dst, load_sem.at[i])
        for i, (src, dst) in enumerate(
            ((w_hbm, w), (resid_hbm, resid), (gain_hbm, gain), (router_hbm, router), (ids_hbm, ids))
        )
    ]
    heads = [
        pltpu.make_async_copy(src, dst, load_sem.at[5 + i])
        for i, (src, dst) in enumerate(((q_hbm, q), (nk_hbm, nk), (nv_hbm, nv)))
    ]
    cached = [
        pltpu.make_async_copy(src.at[pl.ds(4 * i, 4)], dst.at[pl.ds(4 * i, 4)], load_sem.at[8 + 2 * i + n])
        for i in range(4)
        for n, (src, dst) in enumerate(((key_hbm, keys), (value_hbm, values)))
    ]
    for copy in heads + cached + loads:
        copy.start()

    def send(src, dst, key, dev):
        pltpu.make_async_remote_copy(
            src_ref=src, dst_ref=dst, send_sem=send_sem.at[groups.index(key[1])], recv_sem=recv_sem.at[names(*key)],
            device_id=dev, device_id_type=MESH,
        ).start()

    def landed(ref, key):
        pltpu.make_async_remote_copy(
            src_ref=ref, dst_ref=ref, send_sem=send_sem.at[0], recv_sem=recv_sem.at[names(*key)],
            device_id=device(other_core=True), device_id_type=MESH,
        ).wait_recv()

    def sent(ref, group):
        pltpu.make_async_remote_copy(
            src_ref=ref, dst_ref=ref, send_sem=send_sem.at[groups.index(group)], recv_sem=recv_sem.at[0],
            device_id=device(other_core=True), device_id_type=MESH,
        ).wait_send()

    def slot(e):
        return lax.rem(e, 2) * 16 + lax.div(e, 2)

    barrier = pltpu.get_barrier_semaphore()
    for k in range(1, 32):
        pl.semaphore_signal(barrier, inc=1, device_id=(lax.rem(ep + k, 32), dp), device_id_type=MESH)
    for copy in heads:
        copy.wait()
    for h in range(H):
        q32[h * 16 : (h + 1) * 16, :] = q[:, h * HD : (h + 1) * HD].astype(jnp.float32)
    own_keys[...] = nk[...].astype(jnp.float32)
    own_values[...] = nv[...].astype(jnp.float32)

    def arrived(chunk):
        cached[2 * chunk].wait()
        cached[2 * chunk + 1].wait()

    attend(lengths, keys, values, q32, own_keys, own_values, blended32, arrived)
    att[...] = blended32[...].astype(jnp.bfloat16).reshape(H, 16, HD)
    seen[slot(ep)] = att[pl.ds(2 * ep, 2)]
    pl.semaphore_wait(barrier, 31)

    for k in range(1, 32):
        to = lax.rem(ep + k, 32)
        pltpu.make_async_remote_copy(
            src_ref=att.at[pl.ds(2 * to, 2)],
            dst_ref=seen.at[slot(ep)],
            send_sem=all_send.at[0],
            recv_sem=all_recv.at[0],
            device_id=(to, dp),
            device_id_type=MESH,
        ).start()
    everything = pltpu.make_async_remote_copy(
        src_ref=seen.at[pl.ds(0, 31)], dst_ref=seen.at[pl.ds(0, 31)],
        send_sem=all_send.at[0], recv_sem=all_recv.at[0],
        device_id=device(other_core=True), device_id_type=MESH,
    )
    loads[0].wait()
    everything.wait_recv()

    first_dim = ("x", "y")
    second_dim = ("y", "x")

    def spot(q, o1, o2):
        at = {first_dim[q]: rel(first_dim[q], o1), second_dim[q]: rel(second_dim[q], o2)}
        return part.at[q, at["y"], at["x"]]

    def product(q):
        @pl.loop(0, HALF // 256, unroll=4)
        def _(n):
            start = pl.multiple_of(n * 256, 256)
            halves = [
                jnp.concatenate([seen[pl.ds(core * 16, 16), i].reshape(256, HD) for core in (other, c)], axis=0)
                for i in range(2)
            ]
            rows = jnp.concatenate(halves, axis=1)
            cols = pl.ds(pl.multiple_of(q * HALF + start, 256), 256)
            y = jnp.dot(rows, w[:, cols], preferred_element_type=jnp.float32).astype(jnp.bfloat16)
            pair_out[q, :, :, :, pl.ds(start, 256)] = y[:256].reshape(4, 4, 16, 256)
            part[q, :, :, :, pl.ds(start, 256)] = y[256:].reshape(4, 4, 16, 256)

    def add(dst, *srcs):
        total = dst[...].astype(jnp.float32)
        for src in srcs:
            total += src[...].astype(jnp.float32)
        dst[...] = total.astype(jnp.bfloat16)

    UPWARD, DOWNWARD = (2, 1), (3, 0)
    for q in range(2):
        product(q)
    for o1 in (2, 1, 3, 0):
        for q in range(2):
            far = rel(first_dim[q], o1)
            mine = (q, slice(None), far) if q == 0 else (q, far)
            send(pair_out.at[mine], pair_in.at[mine], (q, "sum", o1), device(other_core=True))

    def join(o1):
        for q in range(2):
            landed(pair_in.at[q, 0], (q, "sum", o1))
            for o2 in (2, 3, 1, 0):
                at = {first_dim[q]: rel(first_dim[q], o1), second_dim[q]: rel(second_dim[q], o2)}
                add(spot(q, o1, o2), pair_in.at[q, at["y"], at["x"]])
                if o1 == 2:
                    way = 0 if o2 in UPWARD else 1
                    n = (UPWARD, DOWNWARD)[way].index(o2)
                    send(spot(q, 2, o2), ra1.at[q, way, n], (q, "a1", way, n), device(first_dim[q], 1 + 2 * way))

    join(2)
    join(1)
    join(3)

    def second(direction, j):
        for q in range(2):
            o1, joined = (1, UPWARD) if direction == 0 else (3, DOWNWARD)
            if j in joined:
                k = joined.index(j)
                landed(ra1.at[q, direction, k], (q, "a1", direction, k))
                add(spot(q, o1, j), ra1.at[q, direction, k])
            send(spot(q, o1, j), ra2.at[q, direction, j], (q, "a2", j), device(first_dim[q], o1))

    for up_block, down_block in ((3, 2), (2, 3), (1, 1), (0, 0)):
        second(0, up_block)
        second(1, down_block)
    join(0)

    def finish(q, j):
        landed(ra2.at[q, 0, pl.ds(0, 2)], (q, "a2", j))
        add(spot(q, 0, j), ra2.at[q, 0, j], ra2.at[q, 1, j])

    for o in (2, 3, 1):
        for q in range(2):
            finish(q, o)
            send(spot(q, 0, o), rc.at[q, o - 1], (q, "c"), device(second_dim[q], o))
    for q in range(2):
        finish(q, 0)
    for copy in loads[1:]:
        copy.wait()
    square = jnp.zeros((16, 1), jnp.float32)
    for q in range(2):
        landed(rc.at[q], (q, "c"))
        total = spot(q, 0, 0)[...].astype(jnp.float32)
        for o in (3, 1, 2):
            total += rc[q, o - 1].astype(jnp.float32)
        cols = slice(q * HALF, (q + 1) * HALF)
        hidden = resid[:, cols].astype(jnp.float32) + total
        hidden_out[:, cols] = hidden
        square += jnp.sum(hidden * hidden, axis=1, keepdims=True)
    scale = lax.rsqrt(jnp.maximum(square * (1.0 / D), 0.25))
    logits = jnp.zeros((router.shape[0], 16), jnp.float32)
    for q in range(2):
        cols = slice(q * HALF, (q + 1) * HALF)
        normed = (hidden_out[:, cols] * scale * gain[:, cols]).astype(jnp.bfloat16)
        x_out[:, cols] = normed
        logits += lax.dot_general(
            router[:, cols], normed, (((1,), (1,)), ((), ())), preferred_element_type=jnp.float32
        )
    labels = lax.broadcasted_iota(jnp.int32, logits.shape, 0)
    named = ids[0:1, :] == labels
    for k in range(1, TOP):
        named = named | (ids[k : k + 1, :] == labels)
    peak = jnp.max(jnp.where(named, logits, -jnp.inf), axis=0, keepdims=True)
    grown = jnp.where(named, jnp.exp(jnp.where(named, logits - peak, 0.0)), 0.0)
    probs = (grown / jnp.sum(grown, axis=0, keepdims=True)).astype(jnp.bfloat16)
    experts = router.shape[0]
    spread = (experts, 3 * PART - D)
    ones = lax.broadcasted_iota(jnp.int32, spread, 0) == lax.broadcasted_iota(jnp.int32, spread, 1)
    x_out[:, D:] = lax.dot_general(
        probs, ones.astype(jnp.float32).astype(jnp.bfloat16), (((0,), (0,)), ((), ())),
        preferred_element_type=jnp.float32,
    ).astype(jnp.bfloat16)

    everything.wait_send()
    sent(pair_out, "sum")
    sent(part.at[0, pl.ds(0, 2)], "a1")
    sent(part.at[0], "a2")
    sent(part.at[:, 0, pl.ds(0, 3)], "c")
    assert len(names.table) == 26


def attention_out(
    cache_len, queries, new_keys, new_values, cache_keys, cache_values, resid, norm_gain, router, expert_ids, out_proj
):
    bf = jnp.bfloat16
    vmem = pl.BlockSpec(memory_space=pltpu.VMEM)
    return pl.pallas_call(
        project_kernel,
        out_shape=(
            jax.ShapeDtypeStruct((16, D), jnp.float32),
            jax.ShapeDtypeStruct((16, 3 * PART), bf),
        ),
        in_specs=[pl.BlockSpec(memory_space=pltpu.SMEM)] + [pl.BlockSpec(memory_space=pl.ANY)] * 10,
        out_specs=(vmem, vmem),
        scratch_shapes=[
            pltpu.VMEM(queries.shape, bf),
            pltpu.VMEM(new_keys.shape, bf),
            pltpu.VMEM(new_values.shape, bf),
            pltpu.VMEM(cache_keys.shape, bf),
            pltpu.VMEM(cache_values.shape, bf),
            pltpu.VMEM((16 * H, HD), jnp.float32),
            pltpu.VMEM(new_keys.shape, jnp.float32),
            pltpu.VMEM(new_values.shape, jnp.float32),
            pltpu.VMEM((16 * H, HD), jnp.float32),
            pltpu.VMEM((H, 16, HD), bf),
            pltpu.VMEM((16, D), bf),
            pltpu.VMEM((1, D), jnp.float32),
            pltpu.VMEM(router.shape[::-1], bf),
            pltpu.VMEM((TOP, 16), jnp.int32),
            pltpu.VMEM((256, D), bf),
            pltpu.VMEM((32, 2, 16, HD), bf),
            pltpu.VMEM((2, 4, 4, 16, HALF), bf),
            pltpu.VMEM((2, 4, 4, 16, HALF), bf),
            pltpu.VMEM((2, 4, 4, 16, HALF), bf),
            pltpu.VMEM((2, 2, 2, 16, HALF), bf),
            pltpu.VMEM((2, 2, 4, 16, HALF), bf),
            pltpu.VMEM((2, 3, 16, HALF), bf),
            pltpu.SemaphoreType.DMA((4,)),
            pltpu.SemaphoreType.DMA((26,)),
            pltpu.SemaphoreType.DMA((1,)),
            pltpu.SemaphoreType.DMA((1,)),
            pltpu.SemaphoreType.DMA((16,)),
        ],
        compiler_params=pltpu.CompilerParams(
            collective_id=1, has_side_effects=True, vmem_limit_bytes=67043328
        ),
        name="attention_out",
    )(cache_len, queries, new_keys, new_values, cache_keys, cache_values, resid, norm_gain.reshape(1, D), router.T, expert_ids.T, out_proj)


def local(
    resid,
    queries,
    new_keys,
    new_values,
    cache_keys,
    cache_values,
    cache_len,
    out_proj,
    norm_gain,
    router,
    expert_ids,
    gate_slab,
    up_slab,
    down_slab,
):
    hidden, x_in = attention_out(
        cache_len, queries, new_keys, new_values, cache_keys, cache_values, resid, norm_gain, router, expert_ids, out_proj
    )
    return moe(x_in, hidden, gate_slab[0], up_slab[0], down_slab[0])


def solution(mesh):
    in_specs = (
        P(("ep", "dp"), None),
        P(("ep", "dp"), None),
        P(("ep", "dp"), None),
        P(("ep", "dp"), None),
        P(("ep", "dp"), None, None),
        P(("ep", "dp"), None, None),
        P(("ep", "dp")),
        P("ep", None),
        P(),
        P(),
        P(("ep", "dp"), None),
        P(("ep", "dp"), None, None),
        P(("ep", "dp"), None, None),
        P(("ep", "dp"), None, None),
    )
    out_specs = P(("ep", "dp"), None)
    return jax.shard_map(local, mesh=mesh, in_specs=in_specs, out_specs=out_specs, check_vma=False)
```

```python
import functools
import math

import jax
import jax.numpy as jnp
from jax import lax
from jax.experimental import pallas as pl
from jax.experimental.pallas import tpu as pltpu
from jax.sharding import PartitionSpec as P

D = 4096
H = 64
KVH = 4
HD = 128
TOP = 8
MESH = pl.DeviceIdType.MESH

PART = 1408
ORDER = (("x", "y", "z"), ("y", "z", "x"), ("z", "x", "y"))
HF = 384


def attend(lengths, keys, values, q32, own_keys, own_values, blended32, arrived):
    group = H // KVH
    scale = 1.0 / math.sqrt(HD)

    def token(t):
        position = lax.broadcasted_iota(jnp.int32, (group * KVH, keys.shape[1]), 1)
        kept = position < lengths[t]
        slices = [slice(g * HD, (g + 1) * HD) for g in range(KVH)]
        qs = [q32[pl.ds(g * group * 16 + t, group, stride=16), :] for g in range(KVH)]
        scores = jnp.concatenate(
            [
                lax.dot_general(
                    q.astype(jnp.bfloat16), keys[t, :, cols], (((1,), (1,)), ((), ())),
                    preferred_element_type=jnp.float32,
                )
                for q, cols in zip(qs, slices)
            ],
            axis=0,
        )
        scores = jnp.where(kept, scores * scale, -1e30)
        own = jnp.concatenate([q * own_keys[pl.ds(t, 1), cols] for q, cols in zip(qs, slices)], axis=0)
        own = jnp.sum(own, axis=1, keepdims=True) * scale
        peak = jnp.maximum(jnp.max(scores, axis=1, keepdims=True), own)
        grown, own_grown = jnp.exp(scores - peak), jnp.exp(own - peak)
        total = jnp.sum(grown, axis=1, keepdims=True) + own_grown
        weights = (grown / total).astype(jnp.bfloat16)
        own_weight = (own_grown / total).astype(jnp.bfloat16).astype(jnp.float32)
        for g, cols in enumerate(slices):
            here = slice(g * group, (g + 1) * group)
            mixed = jnp.dot(weights[here], values[t, :, cols], preferred_element_type=jnp.float32)
            mixed += own_weight[here] * own_values[pl.ds(t, 1), cols]
            blended32[pl.ds(g * group * 16 + t, group, stride=16), :] = mixed

    for chunk in range(4):
        arrived(chunk)

        @pl.loop(4 * chunk, 4 * chunk + 4, unroll=4)
        def _(t):
            token(t)


class Place:
    def __init__(self):
        ep = lax.axis_index("ep")
        self.c = lax.rem(ep, 2)
        self.coord = {
            "x": lax.rem(lax.div(ep, 2), 4),
            "y": lax.div(ep, 8),
            "z": lax.axis_index("dp"),
        }

    def rel(self, dim, offset):
        if isinstance(offset, int) and offset == 0:
            return self.coord[dim]
        return lax.rem(self.coord[dim] + offset, 4)

    def device(self, dim=None, offset=0, other_core=False):
        at = dict(self.coord)
        if dim is not None:
            at[dim] = self.rel(dim, offset)
        core = 1 - self.c if other_core else self.c
        return ((at["y"] * 4 + at["x"]) * 2 + core, at["z"])


class Names:
    def __init__(self):
        self.table = {}

    def __call__(self, *key):
        return self.table.setdefault(key, len(self.table))


GROUPS = ("1", "2", "2g", "3", "3g", "pair", "a1", "a2", "b1", "b2", "c", ("sum", 0), ("sum", 1), ("sum", 2))
KEYS = 129


def moe_kernel(
    x_in, hidden, gate, up, down, out,
    residual, rows, gu, dn, acc, act, part, pair_out, pair_in, ra1, ra2, rb1, rb2, rc,
    send_sem, recv_sem, load_sem,
):
    here = Place()
    c = here.c
    other = 1 - c
    rel, device = here.rel, here.device
    names = Names()
    parts = range(3)
    dims = ORDER

    def send(src, dst, key, dev, group):
        copy = pltpu.make_async_remote_copy(
            src_ref=src, dst_ref=dst, send_sem=send_sem.at[GROUPS.index(group)], recv_sem=recv_sem.at[names(*key)],
            device_id=dev, device_id_type=MESH,
        )
        copy.start()
        return copy

    def landed(ref, key):
        pltpu.make_async_remote_copy(
            src_ref=ref, dst_ref=ref, send_sem=send_sem.at[0], recv_sem=recv_sem.at[names(*key)],
            device_id=device(other_core=True), device_id_type=MESH,
        ).wait_recv()

    def sent(ref, group):
        pltpu.make_async_remote_copy(
            src_ref=ref, dst_ref=ref, send_sem=send_sem.at[GROUPS.index(group)], recv_sem=recv_sem.at[0],
            device_id=device(other_core=True), device_id_type=MESH,
        ).wait_send()

    def amount(p, n):
        if n == 1:
            return rows.at[p, 0, 0, 0, 0]
        if n < 4:
            return rows.at[p, 0, 0, 0, pl.ds(0, n)]
        if n < 16:
            return rows.at[p, 0, 0, pl.ds(0, n // 4)]
        return rows.at[p, 0, pl.ds(0, n // 16)]

    def where(p, o1, o2, o3):
        at = {d: (slice(None) if o is None else rel(d, o)) for d, o in zip(ORDER[p], (o1, o2, o3))}
        return at["y"], at["x"], at["z"]

    def block(p, o1, o2, o3, core=None):
        return rows.at[(p, c if core is None else core) + where(p, o1, o2, o3)]

    def send_sub(p, j):
        ref = block(p, j, 0, 0)
        send(ref, ref, (p, "2", j), device(dims[p][1], 1), "2")
        send(ref, ref, (p, "2", j), device(dims[p][1], 3), "2")

    def send_line(p, j):
        ref = block(p, None, j, 0)
        send(ref, ref, (p, "3", j), device(dims[p][2], 1), "3")
        send(ref, ref, (p, "3", j), device(dims[p][2], 3), "3")

    def send_block(p, i, j):
        ref = block(p, i, j, 0)
        send(ref, ref, (p, "3", j), device(dims[p][2], 1), "3")
        send(ref, ref, (p, "3", j), device(dims[p][2], 3), "3")

    def unit(o2, o3):
        if o3 in (1, 3):
            return "near", o2
        if o3 == 0:
            return "own", (0, 1, 2, 1)[o2]
        return "far", o2 in (0, 1)

    def pass_on(p, o2, o3):
        ref = block(p, None, o2, o3)
        send(ref, ref, (p, "pair") + unit(o2, o3), device(other_core=True), "pair")

    def project(*lines):
        for p in parts:
            landed(amount(p, 4 * len(lines)), (p, "pair") + unit(*lines[0]))
            at = [where(p, None, o2, o3) for o2, o3 in lines]

            @pl.loop(0, 3, unroll=3)
            def _(n):
                cols = pl.ds(pl.multiple_of(n * 256, 256), 256)
                x = [rows[(p, slice(None)) + a].reshape(128, PART) for a in at]
                x = jnp.concatenate(x, axis=0)
                w = gu[p * PART : (p + 1) * PART, cols]
                y = jnp.dot(x, w, preferred_element_type=jnp.float32)
                for i, a in enumerate(at):
                    idx = (slice(None),) + a + (slice(None), cols)
                    acc[idx] += y[i * 128 : (i + 1) * 128].reshape(2, 4, 16, 256)

    barrier = pltpu.get_barrier_semaphore()
    for dim in ("x", "y", "z"):
        for o in (1, 2, 3):
            pl.semaphore_signal(barrier, inc=1, device_id=device(dim, o), device_id_type=MESH)
    pl.semaphore_signal(barrier, inc=1, device_id=device(other_core=True), device_id_type=MESH)

    fetch = pltpu.make_async_copy(hidden, residual, load_sem.at[3])
    fetch.start()
    starts = [
        pltpu.make_async_copy(x_in.at[:, pl.ds(p * PART, PART)], rows.at[(p, c) + where(p, 0, 0, 0)], load_sem.at[4 + p])
        for p in range(3)
    ]
    for copy in starts:
        copy.start()
    loads = [
        pltpu.make_async_copy(gate, gu.at[pl.ds(0, D), pl.ds(0, HF)], load_sem.at[0]),
        pltpu.make_async_copy(up, gu.at[pl.ds(0, D), pl.ds(HF, HF)], load_sem.at[1]),
        pltpu.make_async_copy(down, dn.at[:, pl.ds(0, D)], load_sem.at[2]),
    ]
    for copy in loads:
        copy.start()
    pl.semaphore_wait(barrier, 10)

    for copy in starts:
        copy.wait()
    fetch.wait()
    for p in parts:
        own = block(p, 0, 0, 0)
        for o in (1, 3):
            send(own, own, (p, "1n"), device(dims[p][0], o), "1")
        send(own, own, (p, "1f"), device(dims[p][0], 2), "1")
    for p in parts:
        send_sub(p, 0)

    gu[D:, :] = jnp.zeros((3 * PART - D, 2 * HF), jnp.bfloat16)
    dn[:, D:] = jnp.zeros((HF, 3 * PART - D), jnp.bfloat16)

    @pl.loop(0, 32)
    def _(i):
        acc[i // 16, lax.rem(i, 16) // 4, lax.rem(i, 4)] = jnp.zeros((4, 16, 2 * HF), jnp.float32)

    for p in parts:
        send_block(p, 0, 0)
    for p in parts:
        landed(amount(p, 2), (p, "1n"))
        send_sub(p, 1)
        send_sub(p, 3)
    for p in parts:
        landed(amount(p, 1), (p, "1f"))
        send_sub(p, 2)
    for p in parts:
        for i in (1, 3, 2):
            send_block(p, i, 0)
        pass_on(p, 0, 0)
    for copy in loads:
        copy.wait()
    project((0, 0))
    for j in (0, 1, 3, 2):
        for p in parts:
            landed(amount(p, 2), (p, "2", j))
            o = 3 if j in (0, 1) else 1
            ref = block(p, j, o, 0)
            send(ref, ref, (p, "2g"), device(dims[p][1], 4 - o), "2g")
            send_block(p, j, 1)
            send_block(p, j, 3)
    for p in parts:
        pass_on(p, 1, 0)
        pass_on(p, 3, 0)
    project((1, 0), (3, 0))
    for p in parts:
        landed(amount(p, 4), (p, "2g"))
        send_line(p, 2)
        pass_on(p, 2, 0)

    def neighbours(j):
        for p in parts:
            landed(amount(p, 8), (p, "3", j))
            o = 3 if j in (0, 3) else 1
            ref = block(p, None, j, o)
            send(ref, ref, (p, "3g", j in (0, 1)), device(dims[p][2], 4 - o), "3g")
            pass_on(p, j, 3)
            pass_on(p, j, 1)

    def opposite(*lines):
        for p in parts:
            landed(amount(p, 8), (p, "3g", lines[0] in (0, 1)))
            for j in lines:
                pass_on(p, j, 2)

    neighbours(0)
    project((2, 0))
    neighbours(1)
    project((0, 3), (0, 1))
    neighbours(3)
    project((1, 3), (1, 1))
    neighbours(2)
    project((3, 3), (3, 1))
    opposite(0, 1)
    project((2, 3), (2, 1))
    opposite(3, 2)
    project((0, 2), (1, 2))
    project((3, 2), (2, 2))

    expert = lax.div(lax.axis_index("ep") * 4 + lax.axis_index("dp"), 2)

    def activate(at):
        sums = acc[at].reshape(64, 2 * HF)
        tail = rows[(2,) + at + (slice(None), slice(PART - 128, PART))]
        tail = tail.reshape(64, 128).astype(jnp.float32)
        lanes = lax.broadcasted_iota(jnp.int32, (64, 128), 1)
        prob = jnp.sum(jnp.where(lanes == expert, tail, 0.0), axis=1, keepdims=True)
        g, u = sums[:, :HF], sums[:, HF:]
        h = (g * (0.5 + 0.5 * jnp.tanh(0.5 * g)) * u).astype(jnp.bfloat16).astype(jnp.float32) * prob
        act[at] = h.astype(jnp.bfloat16).reshape(4, 16, HF)

    every = slice(None)

    def activate_opposite(p):
        far = rel(dims[p][2], 2)

        @pl.loop(0, 8)
        def _(i):
            core, k = i // 4, lax.rem(i, 4)
            activate(((core, k, every, far), (core, k, far, every), (core, far, k, every))[p])

    def activate_rest():
        @pl.loop(0, 18)
        def _(i):
            k = lax.rem(i, 9)
            oy, ox = k // 3, lax.rem(k, 3)
            oy, ox = oy + oy // 2, ox + ox // 2
            activate((i // 9, rel("y", oy), rel("x", ox), every))

    def spot(p, o2, o3):
        a2 = slice(None) if o2 is None else rel(dims[p][1], o2)
        a3 = slice(None) if o3 is None else rel(dims[p][0], o3)
        return (a3, a2) if p == 1 else (a2, a3)

    def line(p, o1, o2):
        return part.at[(p, o1) + spot(p, o2, None)]

    def sub(p, o3):
        return part.at[(p, 0) + spot(p, 0, o3)]

    def hidden_of(p, o1, core):
        at = {d: (rel(d, o1) if d == dims[p][2] else slice(None)) for d in "xyz"}
        return act[core, at["y"], at["x"], at["z"]].reshape(256, HF)

    def product(p, o1):
        def piece(cols, wcols, width):
            h = jnp.concatenate([hidden_of(p, o1, other), hidden_of(p, o1, c)], axis=0)
            y = jnp.dot(h, dn[:, wcols], preferred_element_type=jnp.float32).astype(jnp.bfloat16)
            pair_out[p, :, :, :, cols] = y[:256].reshape(4, 4, 16, width)
            part[p, o1, :, :, :, cols] = y[256:].reshape(4, 4, 16, width)

        @pl.loop(0, 5, unroll=5)
        def _(n):
            start = pl.multiple_of(n * 256, 256)
            piece(pl.ds(start, 256), pl.ds(pl.multiple_of(p * PART + start, 128), 256), 256)

        if p < 2:
            piece(pl.ds(1280, 128), pl.ds(p * PART + 1280, 128), 128)
        else:
            pair_out[p, :, :, :, 1280:] = jnp.zeros((4, 4, 16, 128), jnp.bfloat16)
            part[p, o1, :, :, :, 1280:] = jnp.zeros((4, 4, 16, 128), jnp.bfloat16)

    def add(dst, *srcs):
        @pl.loop(0, 4)
        def _(i):
            total = dst[i].astype(jnp.float32)
            for s in srcs:
                total += s[i].astype(jnp.float32)
            dst[i] = total.astype(jnp.bfloat16)

    def add_sub(dst, *srcs):
        total = dst[...].astype(jnp.float32)
        for s in srcs:
            total += s[...].astype(jnp.float32)
        dst[...] = total.astype(jnp.bfloat16)

    last = {}

    def sums_for(o1, then, before=None):
        def finish(p):
            landed(pair_in.at[p, o1], (p, "sum", o1))

            @pl.loop(0, 4)
            def _(i):
                add(part.at[p, o1, i], pair_in.at[p, o1, i])

            then(p)

        for p in parts:
            if p in last:
                last[p].wait_send()
            if before is not None:
                before(p)
            product(p, o1)
            last[p] = send(pair_out.at[p], pair_in.at[p, o1], (p, "sum", o1), device(other_core=True), ("sum", p))
            if p:
                finish(p - 1)
        finish(2)

    def up_of(p, level):
        return device(dims[p][level], 1)

    def down_of(p, level):
        return device(dims[p][level], 3)

    UPWARD, DOWNWARD = (2, 1), (3, 0)

    def first(p):
        for k in range(2):
            send(line(p, 2, UPWARD[k]), ra1.at[p, 0, k], (p, "a1", 0, k), up_of(p, 2), "a1")
            send(line(p, 2, DOWNWARD[k]), ra1.at[p, 1, k], (p, "a1", 1, k), down_of(p, 2), "a1")

    def nothing(p):
        pass

    def second(direction, j):
        o1, joined = (1, UPWARD) if direction == 0 else (3, DOWNWARD)
        for p in parts:
            if j in joined:
                k = joined.index(j)
                landed(ra1.at[p, direction, k], (p, "a1", direction, k))
                add(line(p, o1, j), ra1.at[p, direction, k])
            send(line(p, o1, j), ra2.at[p, direction, j], (p, "a2", j), device(dims[p][2], o1), "a2")

    sums_for(2, first, activate_opposite)
    activate_rest()
    sums_for(1, nothing)
    sums_for(3, nothing)
    second(0, 2)
    second(1, 2)
    second(0, 1)
    second(1, 3)
    second(0, 3)
    second(1, 1)
    sums_for(0, nothing)

    def finish_line(p, j):
        landed(ra2.at[p, 0, pl.ds(0, 2)], (p, "a2", j))
        add(line(p, 0, j), ra2.at[p, 0, j], ra2.at[p, 1, j])

    def block_of(p, o2, o3):
        return part.at[(p, 0) + spot(p, o2, o3)]

    for p in parts:
        finish_line(p, 2)
        for k in range(2):
            send(block_of(p, 2, UPWARD[k]), rb1.at[p, 0, k], (p, "b1", 0, k), up_of(p, 1), "b1")
            send(block_of(p, 2, DOWNWARD[k]), rb1.at[p, 1, k], (p, "b1", 1, k), down_of(p, 1), "b1")
    second(0, 0)
    second(1, 0)
    for p in parts:
        finish_line(p, 3)
        for j in UPWARD:
            send(block_of(p, 3, j), rb2.at[p, 1, j], (p, "b2", j), down_of(p, 1), "b2")
    for p in parts:
        finish_line(p, 1)
        for j in DOWNWARD:
            send(block_of(p, 1, j), rb2.at[p, 0, j], (p, "b2", j), up_of(p, 1), "b2")
    for k in range(2):
        for p in parts:
            j = UPWARD[k]
            landed(rb1.at[p, 0, k], (p, "b1", 0, k))
            add_sub(block_of(p, 1, j), rb1.at[p, 0, k])
            send(block_of(p, 1, j), rb2.at[p, 0, j], (p, "b2", j), up_of(p, 1), "b2")
            j = DOWNWARD[k]
            landed(rb1.at[p, 1, k], (p, "b1", 1, k))
            add_sub(block_of(p, 3, j), rb1.at[p, 1, k])
            send(block_of(p, 3, j), rb2.at[p, 1, j], (p, "b2", j), down_of(p, 1), "b2")
    for p in parts:
        finish_line(p, 0)

    def finish_block(p, j):
        landed(rb2.at[p, 0, pl.ds(0, 2)], (p, "b2", j))
        add_sub(sub(p, j), rb2.at[p, 0, j], rb2.at[p, 1, j])

    for o in (2, 3, 1):
        for p in parts:
            finish_block(p, o)
            send(sub(p, o), rc.at[p, o - 1], (p, "c"), device(dims[p][0], o), "c")
    for p in parts:
        finish_block(p, 0)
    for p in parts:
        landed(rc.at[p], (p, "c"))
        total = sub(p, 0)[...].astype(jnp.float32)
        for o in (3, 1, 2):
            total += rc[p, o - 1].astype(jnp.float32)
        width = min(PART, D - p * PART)
        cols = slice(p * PART, p * PART + width)
        out[:, cols] = residual[:, cols] + total[:, :width]
    for group, n in (("1", 3), ("2", 8), ("2g", 4), ("3", 32), ("3g", 16), ("pair", 64)):
        sent(amount(slice(None), n), group)
    for group, n in (("a1", 16), ("a2", 32), ("b1", 4), ("b2", 8), ("c", 3)):
        sent(amount(slice(None), n), group)
    for p in parts:
        last[p].wait_send()
    assert len(names.table) == KEYS, len(names.table)


def moe(x_in, hidden, gate, up, down):
    bf = jnp.bfloat16
    vmem = pl.BlockSpec(memory_space=pltpu.VMEM)
    hbm = pl.BlockSpec(memory_space=pl.ANY)
    return pl.pallas_call(
        moe_kernel,
        out_shape=jax.ShapeDtypeStruct((16, D), jnp.float32),
        in_specs=[hbm] * 5,
        out_specs=vmem,
        scratch_shapes=[
            pltpu.VMEM((16, D), jnp.float32),
            pltpu.VMEM((3, 2, 4, 4, 4, 16, PART), bf),
            pltpu.VMEM((3 * PART, 2 * HF), bf),
            pltpu.VMEM((HF, 3 * PART), bf),
            pltpu.VMEM((2, 4, 4, 4, 16, 2 * HF), jnp.float32),
            pltpu.VMEM((2, 4, 4, 4, 16, HF), bf),
            pltpu.VMEM((3, 4, 4, 4, 16, PART), bf),
            pltpu.VMEM((3, 4, 4, 16, PART), bf),
            pltpu.VMEM((3, 4, 4, 4, 16, PART), bf),
            pltpu.VMEM((3, 2, 2, 4, 16, PART), bf),
            pltpu.VMEM((3, 2, 4, 4, 16, PART), bf),
            pltpu.VMEM((3, 2, 2, 16, PART), bf),
            pltpu.VMEM((3, 2, 4, 16, PART), bf),
            pltpu.VMEM((3, 3, 16, PART), bf),
            pltpu.SemaphoreType.DMA((len(GROUPS),)),
            pltpu.SemaphoreType.DMA((KEYS,)),
            pltpu.SemaphoreType.DMA((7,)),
        ],
        compiler_params=pltpu.CompilerParams(
            collective_id=0, has_side_effects=True, vmem_limit_bytes=67043328
        ),
        name="moe",
    )(x_in, hidden, gate, up, down)


HALF = D // 2


def project_kernel(
    lengths, q_hbm, nk_hbm, nv_hbm, key_hbm, value_hbm, resid_hbm, gain_hbm, router_hbm, ids_hbm, w_hbm, hidden_out, x_out,
    q, nk, nv, keys, values, q32, own_keys, own_values, blended32, att,
    resid, gain, router, ids, w, seen, part, pair_out, pair_in, ra1, ra2, rc,
    send_sem, recv_sem, all_send, all_recv, load_sem,
):
    here = Place()
    c = here.c
    other = 1 - c
    rel, device = here.rel, here.device
    ep, dp = lax.axis_index("ep"), lax.axis_index("dp")
    names = Names()
    groups = ("sum", "a1", "a2", "c")
    loads = [
        pltpu.make_async_copy(src, dst, load_sem.at[i])
        for i, (src, dst) in enumerate(
            ((w_hbm, w), (resid_hbm, resid), (gain_hbm, gain), (router_hbm, router), (ids_hbm, ids))
        )
    ]
    heads = [
        pltpu.make_async_copy(src, dst, load_sem.at[5 + i])
        for i, (src, dst) in enumerate(((q_hbm, q), (nk_hbm, nk), (nv_hbm, nv)))
    ]
    cached = [
        pltpu.make_async_copy(src.at[pl.ds(4 * i, 4)], dst.at[pl.ds(4 * i, 4)], load_sem.at[8 + 2 * i + n])
        for i in range(4)
        for n, (src, dst) in enumerate(((key_hbm, keys), (value_hbm, values)))
    ]
    for copy in heads + cached + loads:
        copy.start()

    def send(src, dst, key, dev):
        pltpu.make_async_remote_copy(
            src_ref=src, dst_ref=dst, send_sem=send_sem.at[groups.index(key[1])], recv_sem=recv_sem.at[names(*key)],
            device_id=dev, device_id_type=MESH,
        ).start()

    def landed(ref, key):
        pltpu.make_async_remote_copy(
            src_ref=ref, dst_ref=ref, send_sem=send_sem.at[0], recv_sem=recv_sem.at[names(*key)],
            device_id=device(other_core=True), device_id_type=MESH,
        ).wait_recv()

    def sent(ref, group):
        pltpu.make_async_remote_copy(
            src_ref=ref, dst_ref=ref, send_sem=send_sem.at[groups.index(group)], recv_sem=recv_sem.at[0],
            device_id=device(other_core=True), device_id_type=MESH,
        ).wait_send()

    def slot(e):
        return lax.rem(e, 2) * 16 + lax.div(e, 2)

    barrier = pltpu.get_barrier_semaphore()
    for k in range(1, 32):
        pl.semaphore_signal(barrier, inc=1, device_id=(lax.rem(ep + k, 32), dp), device_id_type=MESH)
    for copy in heads:
        copy.wait()
    for h in range(H):
        q32[h * 16 : (h + 1) * 16, :] = q[:, h * HD : (h + 1) * HD].astype(jnp.float32)
    own_keys[...] = nk[...].astype(jnp.float32)
    own_values[...] = nv[...].astype(jnp.float32)

    def arrived(chunk):
        cached[2 * chunk].wait()
        cached[2 * chunk + 1].wait()

    attend(lengths, keys, values, q32, own_keys, own_values, blended32, arrived)
    att[...] = blended32[...].astype(jnp.bfloat16).reshape(H, 16, HD)
    seen[slot(ep)] = att[pl.ds(2 * ep, 2)]
    pl.semaphore_wait(barrier, 31)

    for k in range(1, 32):
        to = lax.rem(ep + k, 32)
        pltpu.make_async_remote_copy(
            src_ref=att.at[pl.ds(2 * to, 2)],
            dst_ref=seen.at[slot(ep)],
            send_sem=all_send.at[0],
            recv_sem=all_recv.at[0],
            device_id=(to, dp),
            device_id_type=MESH,
        ).start()
    everything = pltpu.make_async_remote_copy(
        src_ref=seen.at[pl.ds(0, 31)], dst_ref=seen.at[pl.ds(0, 31)],
        send_sem=all_send.at[0], recv_sem=all_recv.at[0],
        device_id=device(other_core=True), device_id_type=MESH,
    )
    loads[0].wait()
    everything.wait_recv()

    first_dim = ("x", "y")
    second_dim = ("y", "x")

    def spot(q, o1, o2):
        at = {first_dim[q]: rel(first_dim[q], o1), second_dim[q]: rel(second_dim[q], o2)}
        return part.at[q, at["y"], at["x"]]

    def product(q):
        @pl.loop(0, HALF // 256, unroll=4)
        def _(n):
            start = pl.multiple_of(n * 256, 256)
            halves = [
                jnp.concatenate([seen[pl.ds(core * 16, 16), i].reshape(256, HD) for core in (other, c)], axis=0)
                for i in range(2)
            ]
            rows = jnp.concatenate(halves, axis=1)
            cols = pl.ds(pl.multiple_of(q * HALF + start, 256), 256)
            y = jnp.dot(rows, w[:, cols], preferred_element_type=jnp.float32).astype(jnp.bfloat16)
            pair_out[q, :, :, :, pl.ds(start, 256)] = y[:256].reshape(4, 4, 16, 256)
            part[q, :, :, :, pl.ds(start, 256)] = y[256:].reshape(4, 4, 16, 256)

    def add(dst, *srcs):
        total = dst[...].astype(jnp.float32)
        for src in srcs:
            total += src[...].astype(jnp.float32)
        dst[...] = total.astype(jnp.bfloat16)

    UPWARD, DOWNWARD = (2, 1), (3, 0)
    for q in range(2):
        product(q)
    for o1 in (2, 1, 3, 0):
        for q in range(2):
            far = rel(first_dim[q], o1)
            mine = (q, slice(None), far) if q == 0 else (q, far)
            send(pair_out.at[mine], pair_in.at[mine], (q, "sum", o1), device(other_core=True))

    def join(o1):
        for q in range(2):
            landed(pair_in.at[q, 0], (q, "sum", o1))
            for o2 in (2, 3, 1, 0):
                at = {first_dim[q]: rel(first_dim[q], o1), second_dim[q]: rel(second_dim[q], o2)}
                add(spot(q, o1, o2), pair_in.at[q, at["y"], at["x"]])
                if o1 == 2:
                    way = 0 if o2 in UPWARD else 1
                    n = (UPWARD, DOWNWARD)[way].index(o2)
                    send(spot(q, 2, o2), ra1.at[q, way, n], (q, "a1", way, n), device(first_dim[q], 1 + 2 * way))

    join(2)
    join(1)
    join(3)

    def second(direction, j):
        for q in range(2):
            o1, joined = (1, UPWARD) if direction == 0 else (3, DOWNWARD)
            if j in joined:
                k = joined.index(j)
                landed(ra1.at[q, direction, k], (q, "a1", direction, k))
                add(spot(q, o1, j), ra1.at[q, direction, k])
            send(spot(q, o1, j), ra2.at[q, direction, j], (q, "a2", j), device(first_dim[q], o1))

    for up_block, down_block in ((3, 2), (2, 3), (1, 1), (0, 0)):
        second(0, up_block)
        second(1, down_block)
    join(0)

    def finish(q, j):
        landed(ra2.at[q, 0, pl.ds(0, 2)], (q, "a2", j))
        add(spot(q, 0, j), ra2.at[q, 0, j], ra2.at[q, 1, j])

    for o in (2, 3, 1):
        for q in range(2):
            finish(q, o)
            send(spot(q, 0, o), rc.at[q, o - 1], (q, "c"), device(second_dim[q], o))
    for q in range(2):
        finish(q, 0)
    for copy in loads[1:]:
        copy.wait()
    square = jnp.zeros((16, 1), jnp.float32)
    for q in range(2):
        landed(rc.at[q], (q, "c"))
        total = spot(q, 0, 0)[...].astype(jnp.float32)
        for o in (3, 1, 2):
            total += rc[q, o - 1].astype(jnp.float32)
        cols = slice(q * HALF, (q + 1) * HALF)
        hidden = resid[:, cols].astype(jnp.float32) + total
        hidden_out[:, cols] = hidden
        square += jnp.sum(hidden * hidden, axis=1, keepdims=True)
    scale = lax.rsqrt(jnp.maximum(square * (1.0 / D), 0.25))
    logits = jnp.zeros((router.shape[0], 16), jnp.float32)
    for q in range(2):
        cols = slice(q * HALF, (q + 1) * HALF)
        normed = (hidden_out[:, cols] * scale * gain[:, cols]).astype(jnp.bfloat16)
        x_out[:, cols] = normed
        logits += lax.dot_general(
            router[:, cols], normed, (((1,), (1,)), ((), ())), preferred_element_type=jnp.float32
        )
    labels = lax.broadcasted_iota(jnp.int32, logits.shape, 0)
    named = ids[0:1, :] == labels
    for k in range(1, TOP):
        named = named | (ids[k : k + 1, :] == labels)
    peak = jnp.max(jnp.where(named, logits, -jnp.inf), axis=0, keepdims=True)
    grown = jnp.where(named, jnp.exp(jnp.where(named, logits - peak, 0.0)), 0.0)
    probs = (grown / jnp.sum(grown, axis=0, keepdims=True)).astype(jnp.bfloat16)
    experts = router.shape[0]
    spread = (experts, 3 * PART - D)
    ones = lax.broadcasted_iota(jnp.int32, spread, 0) == lax.broadcasted_iota(jnp.int32, spread, 1)
    x_out[:, D:] = lax.dot_general(
        probs, ones.astype(jnp.float32).astype(jnp.bfloat16), (((0,), (0,)), ((), ())),
        preferred_element_type=jnp.float32,
    ).astype(jnp.bfloat16)

    everything.wait_send()
    sent(pair_out, "sum")
    sent(part.at[0, pl.ds(0, 2)], "a1")
    sent(part.at[0], "a2")
    sent(part.at[:, 0, pl.ds(0, 3)], "c")
    assert len(names.table) == 26


def attention_out(
    cache_len, queries, new_keys, new_values, cache_keys, cache_values, resid, norm_gain, router, expert_ids, out_proj
):
    bf = jnp.bfloat16
    vmem = pl.BlockSpec(memory_space=pltpu.VMEM)
    return pl.pallas_call(
        project_kernel,
        out_shape=(
            jax.ShapeDtypeStruct((16, D), jnp.float32),
            jax.ShapeDtypeStruct((16, 3 * PART), bf),
        ),
        in_specs=[pl.BlockSpec(memory_space=pltpu.SMEM)] + [pl.BlockSpec(memory_space=pl.ANY)] * 10,
        out_specs=(vmem, vmem),
        scratch_shapes=[
            pltpu.VMEM(queries.shape, bf),
            pltpu.VMEM(new_keys.shape, bf),
            pltpu.VMEM(new_values.shape, bf),
            pltpu.VMEM(cache_keys.shape, bf),
            pltpu.VMEM(cache_values.shape, bf),
            pltpu.VMEM((16 * H, HD), jnp.float32),
            pltpu.VMEM(new_keys.shape, jnp.float32),
            pltpu.VMEM(new_values.shape, jnp.float32),
            pltpu.VMEM((16 * H, HD), jnp.float32),
            pltpu.VMEM((H, 16, HD), bf),
            pltpu.VMEM((16, D), bf),
            pltpu.VMEM((1, D), jnp.float32),
            pltpu.VMEM(router.shape[::-1], bf),
            pltpu.VMEM((TOP, 16), jnp.int32),
            pltpu.VMEM((256, D), bf),
            pltpu.VMEM((32, 2, 16, HD), bf),
            pltpu.VMEM((2, 4, 4, 16, HALF), bf),
            pltpu.VMEM((2, 4, 4, 16, HALF), bf),
            pltpu.VMEM((2, 4, 4, 16, HALF), bf),
            pltpu.VMEM((2, 2, 2, 16, HALF), bf),
            pltpu.VMEM((2, 2, 4, 16, HALF), bf),
            pltpu.VMEM((2, 3, 16, HALF), bf),
            pltpu.SemaphoreType.DMA((4,)),
            pltpu.SemaphoreType.DMA((26,)),
            pltpu.SemaphoreType.DMA((1,)),
            pltpu.SemaphoreType.DMA((1,)),
            pltpu.SemaphoreType.DMA((16,)),
        ],
        compiler_params=pltpu.CompilerParams(
            collective_id=1, has_side_effects=True, vmem_limit_bytes=67043328
        ),
        name="attention_out",
    )(cache_len, queries, new_keys, new_values, cache_keys, cache_values, resid, norm_gain.reshape(1, D), router.T, expert_ids.T, out_proj)


def local(
    resid,
    queries,
    new_keys,
    new_values,
    cache_keys,
    cache_values,
    cache_len,
    out_proj,
    norm_gain,
    router,
    expert_ids,
    gate_slab,
    up_slab,
    down_slab,
):
    hidden, x_in = attention_out(
        cache_len, queries, new_keys, new_values, cache_keys, cache_values, resid, norm_gain, router, expert_ids, out_proj
    )
    return moe(x_in, hidden, gate_slab[0], up_slab[0], down_slab[0])


def solution(mesh):
    in_specs = (
        P(("ep", "dp"), None),
        P(("ep", "dp"), None),
        P(("ep", "dp"), None),
        P(("ep", "dp"), None),
        P(("ep", "dp"), None, None),
        P(("ep", "dp"), None, None),
        P(("ep", "dp")),
        P("ep", None),
        P(),
        P(),
        P(("ep", "dp"), None),
        P(("ep", "dp"), None, None),
        P(("ep", "dp"), None, None),
        P(("ep", "dp"), None, None),
    )
    out_specs = P(("ep", "dp"), None)
    return jax.shard_map(local, mesh=mesh, in_specs=in_specs, out_specs=out_specs, check_vma=False)
```

```python
import functools
import math

import jax
import jax.numpy as jnp
from jax import lax
from jax.experimental import pallas as pl
from jax.experimental.pallas import tpu as pltpu
from jax.sharding import PartitionSpec as P

D = 4096
H = 64
KVH = 4
HD = 128
TOP = 8
MESH = pl.DeviceIdType.MESH

PART = 1408
ORDER = (("x", "y", "z"), ("y", "z", "x"), ("z", "x", "y"))
HF = 384


def attend(lengths, keys, values, q32, own_keys, own_values, blended32, arrived):
    group = H // KVH
    scale = 1.0 / math.sqrt(HD)

    def token(t):
        position = lax.broadcasted_iota(jnp.int32, (group * KVH, keys.shape[1]), 1)
        kept = position < lengths[t]
        slices = [slice(g * HD, (g + 1) * HD) for g in range(KVH)]
        qs = [q32[pl.ds(g * group * 16 + t, group, stride=16), :] for g in range(KVH)]
        scores = jnp.concatenate(
            [
                lax.dot_general(
                    q.astype(jnp.bfloat16), keys[t, :, cols], (((1,), (1,)), ((), ())),
                    preferred_element_type=jnp.float32,
                )
                for q, cols in zip(qs, slices)
            ],
            axis=0,
        )
        scores = jnp.where(kept, scores * scale, -1e30)
        own = jnp.concatenate([q * own_keys[pl.ds(t, 1), cols] for q, cols in zip(qs, slices)], axis=0)
        own = jnp.sum(own, axis=1, keepdims=True) * scale
        peak = jnp.maximum(jnp.max(scores, axis=1, keepdims=True), own)
        grown, own_grown = jnp.exp(scores - peak), jnp.exp(own - peak)
        total = jnp.sum(grown, axis=1, keepdims=True) + own_grown
        weights = (grown / total).astype(jnp.bfloat16)
        own_weight = (own_grown / total).astype(jnp.bfloat16).astype(jnp.float32)
        for g, cols in enumerate(slices):
            here = slice(g * group, (g + 1) * group)
            mixed = jnp.dot(weights[here], values[t, :, cols], preferred_element_type=jnp.float32)
            mixed += own_weight[here] * own_values[pl.ds(t, 1), cols]
            blended32[pl.ds(g * group * 16 + t, group, stride=16), :] = mixed

    for chunk in range(4):
        arrived(chunk)

        @pl.loop(4 * chunk, 4 * chunk + 4, unroll=4)
        def _(t):
            token(t)


class Place:
    def __init__(self):
        ep = lax.axis_index("ep")
        self.c = lax.rem(ep, 2)
        self.coord = {
            "x": lax.rem(lax.div(ep, 2), 4),
            "y": lax.div(ep, 8),
            "z": lax.axis_index("dp"),
        }

    def rel(self, dim, offset):
        if isinstance(offset, int) and offset == 0:
            return self.coord[dim]
        return lax.rem(self.coord[dim] + offset, 4)

    def device(self, dim=None, offset=0, other_core=False):
        at = dict(self.coord)
        if dim is not None:
            at[dim] = self.rel(dim, offset)
        core = 1 - self.c if other_core else self.c
        return ((at["y"] * 4 + at["x"]) * 2 + core, at["z"])


class Names:
    def __init__(self):
        self.table = {}

    def __call__(self, *key):
        return self.table.setdefault(key, len(self.table))


GROUPS = ("1", "2", "2g", "3", "3g", "pair", "a1", "a2", "b1", "b2", "c", ("sum", 0), ("sum", 1), ("sum", 2))
KEYS = 129


def moe_kernel(
    x_in, hidden, gate, up, down, out,
    residual, rows, gu, dn, acc, act, part, pair_out, pair_in, ra1, ra2, rb1, rb2, rc,
    send_sem, recv_sem, load_sem,
):
    here = Place()
    c = here.c
    other = 1 - c
    rel, device = here.rel, here.device
    names = Names()
    parts = range(3)
    dims = ORDER

    def send(src, dst, key, dev, group):
        copy = pltpu.make_async_remote_copy(
            src_ref=src, dst_ref=dst, send_sem=send_sem.at[GROUPS.index(group)], recv_sem=recv_sem.at[names(*key)],
            device_id=dev, device_id_type=MESH,
        )
        copy.start()
        return copy

    def landed(ref, key):
        pltpu.make_async_remote_copy(
            src_ref=ref, dst_ref=ref, send_sem=send_sem.at[0], recv_sem=recv_sem.at[names(*key)],
            device_id=device(other_core=True), device_id_type=MESH,
        ).wait_recv()

    def sent(ref, group):
        pltpu.make_async_remote_copy(
            src_ref=ref, dst_ref=ref, send_sem=send_sem.at[GROUPS.index(group)], recv_sem=recv_sem.at[0],
            device_id=device(other_core=True), device_id_type=MESH,
        ).wait_send()

    def amount(p, n):
        if n == 1:
            return rows.at[p, 0, 0, 0, 0]
        if n < 4:
            return rows.at[p, 0, 0, 0, pl.ds(0, n)]
        if n < 16:
            return rows.at[p, 0, 0, pl.ds(0, n // 4)]
        return rows.at[p, 0, pl.ds(0, n // 16)]

    def where(p, o1, o2, o3):
        at = {d: (slice(None) if o is None else rel(d, o)) for d, o in zip(ORDER[p], (o1, o2, o3))}
        return at["y"], at["x"], at["z"]

    def block(p, o1, o2, o3, core=None):
        return rows.at[(p, c if core is None else core) + where(p, o1, o2, o3)]

    def send_sub(p, j):
        ref = block(p, j, 0, 0)
        send(ref, ref, (p, "2", j), device(dims[p][1], 1), "2")
        send(ref, ref, (p, "2", j), device(dims[p][1], 3), "2")

    def send_line(p, j):
        ref = block(p, None, j, 0)
        send(ref, ref, (p, "3", j), device(dims[p][2], 1), "3")
        send(ref, ref, (p, "3", j), device(dims[p][2], 3), "3")

    def send_block(p, i, j):
        ref = block(p, i, j, 0)
        send(ref, ref, (p, "3", j), device(dims[p][2], 1), "3")
        send(ref, ref, (p, "3", j), device(dims[p][2], 3), "3")

    def unit(o2, o3):
        if o3 in (1, 3):
            return "near", o2
        if o3 == 0:
            return "own", (0, 1, 2, 1)[o2]
        return "far", o2 in (0, 1)

    def pass_on(p, o2, o3):
        ref = block(p, None, o2, o3)
        send(ref, ref, (p, "pair") + unit(o2, o3), device(other_core=True), "pair")

    def project(*lines):
        for p in parts:
            landed(amount(p, 4 * len(lines)), (p, "pair") + unit(*lines[0]))
            at = [where(p, None, o2, o3) for o2, o3 in lines]

            @pl.loop(0, 3, unroll=3)
            def _(n):
                cols = pl.ds(pl.multiple_of(n * 256, 256), 256)
                x = [rows[(p, slice(None)) + a].reshape(128, PART) for a in at]
                x = jnp.concatenate(x, axis=0)
                w = gu[p * PART : (p + 1) * PART, cols]
                y = jnp.dot(x, w, preferred_element_type=jnp.float32)
                for i, a in enumerate(at):
                    idx = (slice(None),) + a + (slice(None), cols)
                    acc[idx] += y[i * 128 : (i + 1) * 128].reshape(2, 4, 16, 256)

    barrier = pltpu.get_barrier_semaphore()
    for dim in ("x", "y", "z"):
        for o in (1, 2, 3):
            pl.semaphore_signal(barrier, inc=1, device_id=device(dim, o), device_id_type=MESH)
    pl.semaphore_signal(barrier, inc=1, device_id=device(other_core=True), device_id_type=MESH)

    fetch = pltpu.make_async_copy(hidden, residual, load_sem.at[3])
    fetch.start()
    starts = [
        pltpu.make_async_copy(x_in.at[:, pl.ds(p * PART, PART)], rows.at[(p, c) + where(p, 0, 0, 0)], load_sem.at[4 + p])
        for p in range(3)
    ]
    for copy in starts:
        copy.start()
    loads = [
        pltpu.make_async_copy(gate, gu.at[pl.ds(0, D), pl.ds(0, HF)], load_sem.at[0]),
        pltpu.make_async_copy(up, gu.at[pl.ds(0, D), pl.ds(HF, HF)], load_sem.at[1]),
        pltpu.make_async_copy(down, dn.at[:, pl.ds(0, D)], load_sem.at[2]),
    ]
    for copy in loads:
        copy.start()
    pl.semaphore_wait(barrier, 10)

    for copy in starts:
        copy.wait()
    fetch.wait()
    for p in parts:
        own = block(p, 0, 0, 0)
        for o in (1, 3):
            send(own, own, (p, "1n"), device(dims[p][0], o), "1")
        send(own, own, (p, "1f"), device(dims[p][0], 2), "1")
    for p in parts:
        send_sub(p, 0)

    gu[D:, :] = jnp.zeros((3 * PART - D, 2 * HF), jnp.bfloat16)
    dn[:, D:] = jnp.zeros((HF, 3 * PART - D), jnp.bfloat16)

    @pl.loop(0, 32)
    def _(i):
        acc[i // 16, lax.rem(i, 16) // 4, lax.rem(i, 4)] = jnp.zeros((4, 16, 2 * HF), jnp.float32)

    for p in parts:
        send_block(p, 0, 0)
    for p in parts:
        landed(amount(p, 2), (p, "1n"))
        send_sub(p, 1)
        send_sub(p, 3)
    for p in parts:
        landed(amount(p, 1), (p, "1f"))
        send_sub(p, 2)
    for p in parts:
        for i in (1, 3, 2):
            send_block(p, i, 0)
        pass_on(p, 0, 0)
    for copy in loads:
        copy.wait()
    project((0, 0))
    for j in (0, 1, 3, 2):
        for p in parts:
            landed(amount(p, 2), (p, "2", j))
            o = 3 if j in (0, 1) else 1
            ref = block(p, j, o, 0)
            send(ref, ref, (p, "2g"), device(dims[p][1], 4 - o), "2g")
            send_block(p, j, 1)
            send_block(p, j, 3)
    for p in parts:
        pass_on(p, 1, 0)
        pass_on(p, 3, 0)
    project((1, 0), (3, 0))
    for p in parts:
        landed(amount(p, 4), (p, "2g"))
        send_line(p, 2)
        pass_on(p, 2, 0)

    def neighbours(j):
        for p in parts:
            landed(amount(p, 8), (p, "3", j))
            o = 3 if j in (0, 3) else 1
            ref = block(p, None, j, o)
            send(ref, ref, (p, "3g", j in (0, 1)), device(dims[p][2], 4 - o), "3g")
            pass_on(p, j, 3)
            pass_on(p, j, 1)

    def opposite(*lines):
        for p in parts:
            landed(amount(p, 8), (p, "3g", lines[0] in (0, 1)))
            for j in lines:
                pass_on(p, j, 2)

    neighbours(0)
    project((2, 0))
    neighbours(1)
    project((0, 3), (0, 1))
    neighbours(3)
    project((1, 3), (1, 1))
    neighbours(2)
    project((3, 3), (3, 1))
    opposite(0, 1)
    project((2, 3), (2, 1))
    opposite(3, 2)
    project((0, 2), (1, 2))
    project((3, 2), (2, 2))

    expert = lax.div(lax.axis_index("ep") * 4 + lax.axis_index("dp"), 2)

    def activate(at):
        sums = acc[at].reshape(64, 2 * HF)
        tail = rows[(2,) + at + (slice(None), slice(PART - 128, PART))]
        tail = tail.reshape(64, 128).astype(jnp.float32)
        lanes = lax.broadcasted_iota(jnp.int32, (64, 128), 1)
        prob = jnp.sum(jnp.where(lanes == expert, tail, 0.0), axis=1, keepdims=True)
        g, u = sums[:, :HF], sums[:, HF:]
        h = (g * (0.5 + 0.5 * jnp.tanh(0.5 * g)) * u).astype(jnp.bfloat16).astype(jnp.float32) * prob
        act[at] = h.astype(jnp.bfloat16).reshape(4, 16, HF)

    every = slice(None)

    def activate_opposite(p):
        far = rel(dims[p][2], 2)

        @pl.loop(0, 8, unroll=2)
        def _(i):
            core, k = i // 4, lax.rem(i, 4)
            activate(((core, k, every, far), (core, k, far, every), (core, far, k, every))[p])

    def activate_rest():
        @pl.loop(0, 18)
        def _(i):
            k = lax.rem(i, 9)
            oy, ox = k // 3, lax.rem(k, 3)
            oy, ox = oy + oy // 2, ox + ox // 2
            activate((i // 9, rel("y", oy), rel("x", ox), every))

    def spot(p, o2, o3):
        a2 = slice(None) if o2 is None else rel(dims[p][1], o2)
        a3 = slice(None) if o3 is None else rel(dims[p][0], o3)
        return (a3, a2) if p == 1 else (a2, a3)

    def line(p, o1, o2):
        return part.at[(p, o1) + spot(p, o2, None)]

    def sub(p, o3):
        return part.at[(p, 0) + spot(p, 0, o3)]

    def hidden_of(p, o1, core):
        at = {d: (rel(d, o1) if d == dims[p][2] else slice(None)) for d in "xyz"}
        return act[core, at["y"], at["x"], at["z"]].reshape(256, HF)

    def product(p, o1):
        def piece(cols, wcols, width):
            h = jnp.concatenate([hidden_of(p, o1, other), hidden_of(p, o1, c)], axis=0)
            y = jnp.dot(h, dn[:, wcols], preferred_element_type=jnp.float32).astype(jnp.bfloat16)
            pair_out[p, :, :, :, cols] = y[:256].reshape(4, 4, 16, width)
            part[p, o1, :, :, :, cols] = y[256:].reshape(4, 4, 16, width)

        @pl.loop(0, 5, unroll=5)
        def _(n):
            start = pl.multiple_of(n * 256, 256)
            piece(pl.ds(start, 256), pl.ds(pl.multiple_of(p * PART + start, 128), 256), 256)

        if p < 2:
            piece(pl.ds(1280, 128), pl.ds(p * PART + 1280, 128), 128)
        else:
            pair_out[p, :, :, :, 1280:] = jnp.zeros((4, 4, 16, 128), jnp.bfloat16)
            part[p, o1, :, :, :, 1280:] = jnp.zeros((4, 4, 16, 128), jnp.bfloat16)

    def add(dst, *srcs):
        total = dst[...].astype(jnp.float32)
        for s in srcs:
            total += s[...].astype(jnp.float32)
        dst[...] = total.astype(jnp.bfloat16)

    def add_sub(dst, *srcs):
        total = dst[...].astype(jnp.float32)
        for s in srcs:
            total += s[...].astype(jnp.float32)
        dst[...] = total.astype(jnp.bfloat16)

    last = {}

    def sums_for(o1, then, before=None):
        def finish(p):
            landed(pair_in.at[p, o1], (p, "sum", o1))

            @pl.loop(0, 4)
            def _(i):
                total = part[p, o1, i].astype(jnp.float32) + pair_in[p, o1, i].astype(jnp.float32)
                part[p, o1, i] = total.astype(jnp.bfloat16)

            then(p)

        for p in parts:
            if p in last:
                last[p].wait_send()
            if before is not None:
                before(p)
            product(p, o1)
            last[p] = send(pair_out.at[p], pair_in.at[p, o1], (p, "sum", o1), device(other_core=True), ("sum", p))
            if p:
                finish(p - 1)
        finish(2)

    def up_of(p, level):
        return device(dims[p][level], 1)

    def down_of(p, level):
        return device(dims[p][level], 3)

    UPWARD, DOWNWARD = (2, 1), (3, 0)

    def first(p):
        for k in range(2):
            send(line(p, 2, UPWARD[k]), ra1.at[p, 0, k], (p, "a1", 0, k), up_of(p, 2), "a1")
            send(line(p, 2, DOWNWARD[k]), ra1.at[p, 1, k], (p, "a1", 1, k), down_of(p, 2), "a1")

    def nothing(p):
        pass

    def second(direction, j):
        o1, joined = (1, UPWARD) if direction == 0 else (3, DOWNWARD)
        for p in parts:
            if j in joined:
                k = joined.index(j)
                landed(ra1.at[p, direction, k], (p, "a1", direction, k))
                add(line(p, o1, j), ra1.at[p, direction, k])
            send(line(p, o1, j), ra2.at[p, direction, j], (p, "a2", j), device(dims[p][2], o1), "a2")

    sums_for(2, first, activate_opposite)
    activate_rest()
    sums_for(1, nothing)
    sums_for(3, nothing)
    second(0, 2)
    second(1, 2)
    second(0, 1)
    second(1, 3)
    second(0, 3)
    second(1, 1)
    sums_for(0, nothing)

    def finish_line(p, j):
        landed(ra2.at[p, 0, pl.ds(0, 2)], (p, "a2", j))
        add(line(p, 0, j), ra2.at[p, 0, j], ra2.at[p, 1, j])

    def block_of(p, o2, o3):
        return part.at[(p, 0) + spot(p, o2, o3)]

    for p in parts:
        finish_line(p, 2)
        for k in range(2):
            send(block_of(p, 2, UPWARD[k]), rb1.at[p, 0, k], (p, "b1", 0, k), up_of(p, 1), "b1")
            send(block_of(p, 2, DOWNWARD[k]), rb1.at[p, 1, k], (p, "b1", 1, k), down_of(p, 1), "b1")
    second(0, 0)
    second(1, 0)
    for p in parts:
        finish_line(p, 3)
        for j in UPWARD:
            send(block_of(p, 3, j), rb2.at[p, 1, j], (p, "b2", j), down_of(p, 1), "b2")
    for p in parts:
        finish_line(p, 1)
        for j in DOWNWARD:
            send(block_of(p, 1, j), rb2.at[p, 0, j], (p, "b2", j), up_of(p, 1), "b2")
    for k in range(2):
        for p in parts:
            j = UPWARD[k]
            landed(rb1.at[p, 0, k], (p, "b1", 0, k))
            add_sub(block_of(p, 1, j), rb1.at[p, 0, k])
            send(block_of(p, 1, j), rb2.at[p, 0, j], (p, "b2", j), up_of(p, 1), "b2")
            j = DOWNWARD[k]
            landed(rb1.at[p, 1, k], (p, "b1", 1, k))
            add_sub(block_of(p, 3, j), rb1.at[p, 1, k])
            send(block_of(p, 3, j), rb2.at[p, 1, j], (p, "b2", j), down_of(p, 1), "b2")
    for p in parts:
        finish_line(p, 0)

    def finish_block(p, j):
        landed(rb2.at[p, 0, pl.ds(0, 2)], (p, "b2", j))
        add_sub(sub(p, j), rb2.at[p, 0, j], rb2.at[p, 1, j])

    for o in (2, 3, 1):
        for p in parts:
            finish_block(p, o)
            send(sub(p, o), rc.at[p, o - 1], (p, "c"), device(dims[p][0], o), "c")
    for p in parts:
        finish_block(p, 0)
    for p in parts:
        landed(rc.at[p], (p, "c"))
        total = sub(p, 0)[...].astype(jnp.float32)
        for o in (3, 1, 2):
            total += rc[p, o - 1].astype(jnp.float32)
        width = min(PART, D - p * PART)
        cols = slice(p * PART, p * PART + width)
        out[:, cols] = residual[:, cols] + total[:, :width]
    for group, n in (("1", 3), ("2", 8), ("2g", 4), ("3", 32), ("3g", 16), ("pair", 64)):
        sent(amount(slice(None), n), group)
    for group, n in (("a1", 16), ("a2", 32), ("b1", 4), ("b2", 8), ("c", 3)):
        sent(amount(slice(None), n), group)
    for p in parts:
        last[p].wait_send()
    assert len(names.table) == KEYS, len(names.table)


def moe(x_in, hidden, gate, up, down):
    bf = jnp.bfloat16
    vmem = pl.BlockSpec(memory_space=pltpu.VMEM)
    hbm = pl.BlockSpec(memory_space=pl.ANY)
    return pl.pallas_call(
        moe_kernel,
        out_shape=jax.ShapeDtypeStruct((16, D), jnp.float32),
        in_specs=[hbm] * 5,
        out_specs=vmem,
        scratch_shapes=[
            pltpu.VMEM((16, D), jnp.float32),
            pltpu.VMEM((3, 2, 4, 4, 4, 16, PART), bf),
            pltpu.VMEM((3 * PART, 2 * HF), bf),
            pltpu.VMEM((HF, 3 * PART), bf),
            pltpu.VMEM((2, 4, 4, 4, 16, 2 * HF), jnp.float32),
            pltpu.VMEM((2, 4, 4, 4, 16, HF), bf),
            pltpu.VMEM((3, 4, 4, 4, 16, PART), bf),
            pltpu.VMEM((3, 4, 4, 16, PART), bf),
            pltpu.VMEM((3, 4, 4, 4, 16, PART), bf),
            pltpu.VMEM((3, 2, 2, 4, 16, PART), bf),
            pltpu.VMEM((3, 2, 4, 4, 16, PART), bf),
            pltpu.VMEM((3, 2, 2, 16, PART), bf),
            pltpu.VMEM((3, 2, 4, 16, PART), bf),
            pltpu.VMEM((3, 3, 16, PART), bf),
            pltpu.SemaphoreType.DMA((len(GROUPS),)),
            pltpu.SemaphoreType.DMA((KEYS,)),
            pltpu.SemaphoreType.DMA((7,)),
        ],
        compiler_params=pltpu.CompilerParams(
            collective_id=0, has_side_effects=True, vmem_limit_bytes=67043328
        ),
        name="moe",
    )(x_in, hidden, gate, up, down)


HALF = D // 2


def project_kernel(
    lengths, q_hbm, nk_hbm, nv_hbm, key_hbm, value_hbm, resid_hbm, gain_hbm, router_hbm, ids_hbm, w_hbm, hidden_out, x_out,
    q, nk, nv, keys, values, q32, own_keys, own_values, blended32, att,
    resid, gain, router, ids, w, seen, part, pair_out, pair_in, ra1, ra2, rc,
    send_sem, recv_sem, all_send, all_recv, load_sem,
):
    here = Place()
    c = here.c
    other = 1 - c
    rel, device = here.rel, here.device
    ep, dp = lax.axis_index("ep"), lax.axis_index("dp")
    names = Names()
    groups = ("sum", "a1", "a2", "c")
    loads = [
        pltpu.make_async_copy(src, dst, load_sem.at[i])
        for i, (src, dst) in enumerate(
            ((w_hbm, w), (resid_hbm, resid), (gain_hbm, gain), (router_hbm, router), (ids_hbm, ids))
        )
    ]
    heads = [
        pltpu.make_async_copy(src, dst, load_sem.at[5 + i])
        for i, (src, dst) in enumerate(((q_hbm, q), (nk_hbm, nk), (nv_hbm, nv)))
    ]
    cached = [
        pltpu.make_async_copy(src.at[pl.ds(4 * i, 4)], dst.at[pl.ds(4 * i, 4)], load_sem.at[8 + 2 * i + n])
        for i in range(4)
        for n, (src, dst) in enumerate(((key_hbm, keys), (value_hbm, values)))
    ]
    for copy in heads + cached + loads:
        copy.start()

    def send(src, dst, key, dev):
        pltpu.make_async_remote_copy(
            src_ref=src, dst_ref=dst, send_sem=send_sem.at[groups.index(key[1])], recv_sem=recv_sem.at[names(*key)],
            device_id=dev, device_id_type=MESH,
        ).start()

    def landed(ref, key):
        pltpu.make_async_remote_copy(
            src_ref=ref, dst_ref=ref, send_sem=send_sem.at[0], recv_sem=recv_sem.at[names(*key)],
            device_id=device(other_core=True), device_id_type=MESH,
        ).wait_recv()

    def sent(ref, group):
        pltpu.make_async_remote_copy(
            src_ref=ref, dst_ref=ref, send_sem=send_sem.at[groups.index(group)], recv_sem=recv_sem.at[0],
            device_id=device(other_core=True), device_id_type=MESH,
        ).wait_send()

    def slot(e):
        return lax.rem(e, 2) * 16 + lax.div(e, 2)

    barrier = pltpu.get_barrier_semaphore()
    for k in range(1, 32):
        pl.semaphore_signal(barrier, inc=1, device_id=(lax.rem(ep + k, 32), dp), device_id_type=MESH)
    for copy in heads:
        copy.wait()
    for h in range(H):
        q32[h * 16 : (h + 1) * 16, :] = q[:, h * HD : (h + 1) * HD].astype(jnp.float32)
    own_keys[...] = nk[...].astype(jnp.float32)
    own_values[...] = nv[...].astype(jnp.float32)

    def arrived(chunk):
        cached[2 * chunk].wait()
        cached[2 * chunk + 1].wait()

    attend(lengths, keys, values, q32, own_keys, own_values, blended32, arrived)
    att[...] = blended32[...].astype(jnp.bfloat16).reshape(H, 16, HD)
    seen[slot(ep)] = att[pl.ds(2 * ep, 2)]
    pl.semaphore_wait(barrier, 31)

    for k in range(1, 32):
        to = lax.rem(ep + k, 32)
        pltpu.make_async_remote_copy(
            src_ref=att.at[pl.ds(2 * to, 2)],
            dst_ref=seen.at[slot(ep)],
            send_sem=all_send.at[0],
            recv_sem=all_recv.at[0],
            device_id=(to, dp),
            device_id_type=MESH,
        ).start()
    everything = pltpu.make_async_remote_copy(
        src_ref=seen.at[pl.ds(0, 31)], dst_ref=seen.at[pl.ds(0, 31)],
        send_sem=all_send.at[0], recv_sem=all_recv.at[0],
        device_id=device(other_core=True), device_id_type=MESH,
    )
    loads[0].wait()
    everything.wait_recv()

    first_dim = ("x", "y")
    second_dim = ("y", "x")

    def spot(q, o1, o2):
        at = {first_dim[q]: rel(first_dim[q], o1), second_dim[q]: rel(second_dim[q], o2)}
        return part.at[q, at["y"], at["x"]]

    def product(q):
        @pl.loop(0, HALF // 256, unroll=4)
        def _(n):
            start = pl.multiple_of(n * 256, 256)
            halves = [
                jnp.concatenate([seen[pl.ds(core * 16, 16), i].reshape(256, HD) for core in (other, c)], axis=0)
                for i in range(2)
            ]
            rows = jnp.concatenate(halves, axis=1)
            cols = pl.ds(pl.multiple_of(q * HALF + start, 256), 256)
            y = jnp.dot(rows, w[:, cols], preferred_element_type=jnp.float32).astype(jnp.bfloat16)
            pair_out[q, :, :, :, pl.ds(start, 256)] = y[:256].reshape(4, 4, 16, 256)
            part[q, :, :, :, pl.ds(start, 256)] = y[256:].reshape(4, 4, 16, 256)

    def add(dst, *srcs):
        total = dst[...].astype(jnp.float32)
        for src in srcs:
            total += src[...].astype(jnp.float32)
        dst[...] = total.astype(jnp.bfloat16)

    UPWARD, DOWNWARD = (2, 1), (3, 0)
    for q in range(2):
        product(q)
    for o1 in (2, 1, 3, 0):
        for q in range(2):
            far = rel(first_dim[q], o1)
            mine = (q, slice(None), far) if q == 0 else (q, far)
            send(pair_out.at[mine], pair_in.at[mine], (q, "sum", o1), device(other_core=True))

    def join(o1):
        for q in range(2):
            landed(pair_in.at[q, 0], (q, "sum", o1))
            for o2 in (2, 3, 1, 0):
                at = {first_dim[q]: rel(first_dim[q], o1), second_dim[q]: rel(second_dim[q], o2)}
                add(spot(q, o1, o2), pair_in.at[q, at["y"], at["x"]])
                if o1 == 2:
                    way = 0 if o2 in UPWARD else 1
                    n = (UPWARD, DOWNWARD)[way].index(o2)
                    send(spot(q, 2, o2), ra1.at[q, way, n], (q, "a1", way, n), device(first_dim[q], 1 + 2 * way))

    join(2)
    join(1)
    join(3)

    def second(direction, j):
        for q in range(2):
            o1, joined = (1, UPWARD) if direction == 0 else (3, DOWNWARD)
            if j in joined:
                k = joined.index(j)
                landed(ra1.at[q, direction, k], (q, "a1", direction, k))
                add(spot(q, o1, j), ra1.at[q, direction, k])
            send(spot(q, o1, j), ra2.at[q, direction, j], (q, "a2", j), device(first_dim[q], o1))

    for up_block, down_block in ((3, 2), (2, 3), (1, 1), (0, 0)):
        second(0, up_block)
        second(1, down_block)
    join(0)

    def finish(q, j):
        landed(ra2.at[q, 0, pl.ds(0, 2)], (q, "a2", j))
        add(spot(q, 0, j), ra2.at[q, 0, j], ra2.at[q, 1, j])

    for o in (2, 3, 1):
        for q in range(2):
            finish(q, o)
            send(spot(q, 0, o), rc.at[q, o - 1], (q, "c"), device(second_dim[q], o))
    for q in range(2):
        finish(q, 0)
    for copy in loads[1:]:
        copy.wait()
    square = jnp.zeros((16, 1), jnp.float32)
    for q in range(2):
        landed(rc.at[q], (q, "c"))
        total = spot(q, 0, 0)[...].astype(jnp.float32)
        for o in (3, 1, 2):
            total += rc[q, o - 1].astype(jnp.float32)
        cols = slice(q * HALF, (q + 1) * HALF)
        hidden = resid[:, cols].astype(jnp.float32) + total
        hidden_out[:, cols] = hidden
        square += jnp.sum(hidden * hidden, axis=1, keepdims=True)
    scale = lax.rsqrt(jnp.maximum(square * (1.0 / D), 0.25))
    logits = jnp.zeros((router.shape[0], 16), jnp.float32)
    for q in range(2):
        cols = slice(q * HALF, (q + 1) * HALF)
        normed = (hidden_out[:, cols] * scale * gain[:, cols]).astype(jnp.bfloat16)
        x_out[:, cols] = normed
        logits += lax.dot_general(
            router[:, cols], normed, (((1,), (1,)), ((), ())), preferred_element_type=jnp.float32
        )
    labels = lax.broadcasted_iota(jnp.int32, logits.shape, 0)
    named = ids[0:1, :] == labels
    for k in range(1, TOP):
        named = named | (ids[k : k + 1, :] == labels)
    peak = jnp.max(jnp.where(named, logits, -jnp.inf), axis=0, keepdims=True)
    grown = jnp.where(named, jnp.exp(jnp.where(named, logits - peak, 0.0)), 0.0)
    probs = (grown / jnp.sum(grown, axis=0, keepdims=True)).astype(jnp.bfloat16)
    experts = router.shape[0]
    spread = (experts, 3 * PART - D)
    ones = lax.broadcasted_iota(jnp.int32, spread, 0) == lax.broadcasted_iota(jnp.int32, spread, 1)
    x_out[:, D:] = lax.dot_general(
        probs, ones.astype(jnp.float32).astype(jnp.bfloat16), (((0,), (0,)), ((), ())),
        preferred_element_type=jnp.float32,
    ).astype(jnp.bfloat16)

    everything.wait_send()
    sent(pair_out, "sum")
    sent(part.at[0, pl.ds(0, 2)], "a1")
    sent(part.at[0], "a2")
    sent(part.at[:, 0, pl.ds(0, 3)], "c")
    assert len(names.table) == 26


def attention_out(
    cache_len, queries, new_keys, new_values, cache_keys, cache_values, resid, norm_gain, router, expert_ids, out_proj
):
    bf = jnp.bfloat16
    vmem = pl.BlockSpec(memory_space=pltpu.VMEM)
    return pl.pallas_call(
        project_kernel,
        out_shape=(
            jax.ShapeDtypeStruct((16, D), jnp.float32),
            jax.ShapeDtypeStruct((16, 3 * PART), bf),
        ),
        in_specs=[pl.BlockSpec(memory_space=pltpu.SMEM)] + [pl.BlockSpec(memory_space=pl.ANY)] * 10,
        out_specs=(vmem, vmem),
        scratch_shapes=[
            pltpu.VMEM(queries.shape, bf),
            pltpu.VMEM(new_keys.shape, bf),
            pltpu.VMEM(new_values.shape, bf),
            pltpu.VMEM(cache_keys.shape, bf),
            pltpu.VMEM(cache_values.shape, bf),
            pltpu.VMEM((16 * H, HD), jnp.float32),
            pltpu.VMEM(new_keys.shape, jnp.float32),
            pltpu.VMEM(new_values.shape, jnp.float32),
            pltpu.VMEM((16 * H, HD), jnp.float32),
            pltpu.VMEM((H, 16, HD), bf),
            pltpu.VMEM((16, D), bf),
            pltpu.VMEM((1, D), jnp.float32),
            pltpu.VMEM(router.shape[::-1], bf),
            pltpu.VMEM((TOP, 16), jnp.int32),
            pltpu.VMEM((256, D), bf),
            pltpu.VMEM((32, 2, 16, HD), bf),
            pltpu.VMEM((2, 4, 4, 16, HALF), bf),
            pltpu.VMEM((2, 4, 4, 16, HALF), bf),
            pltpu.VMEM((2, 4, 4, 16, HALF), bf),
            pltpu.VMEM((2, 2, 2, 16, HALF), bf),
            pltpu.VMEM((2, 2, 4, 16, HALF), bf),
            pltpu.VMEM((2, 3, 16, HALF), bf),
            pltpu.SemaphoreType.DMA((4,)),
            pltpu.SemaphoreType.DMA((26,)),
            pltpu.SemaphoreType.DMA((1,)),
            pltpu.SemaphoreType.DMA((1,)),
            pltpu.SemaphoreType.DMA((16,)),
        ],
        compiler_params=pltpu.CompilerParams(
            collective_id=1, has_side_effects=True, vmem_limit_bytes=67043328
        ),
        name="attention_out",
    )(cache_len, queries, new_keys, new_values, cache_keys, cache_values, resid, norm_gain.reshape(1, D), router.T, expert_ids.T, out_proj)


def local(
    resid,
    queries,
    new_keys,
    new_values,
    cache_keys,
    cache_values,
    cache_len,
    out_proj,
    norm_gain,
    router,
    expert_ids,
    gate_slab,
    up_slab,
    down_slab,
):
    hidden, x_in = attention_out(
        cache_len, queries, new_keys, new_values, cache_keys, cache_values, resid, norm_gain, router, expert_ids, out_proj
    )
    return moe(x_in, hidden, gate_slab[0], up_slab[0], down_slab[0])


def solution(mesh):
    in_specs = (
        P(("ep", "dp"), None),
        P(("ep", "dp"), None),
        P(("ep", "dp"), None),
        P(("ep", "dp"), None),
        P(("ep", "dp"), None, None),
        P(("ep", "dp"), None, None),
        P(("ep", "dp")),
        P("ep", None),
        P(),
        P(),
        P(("ep", "dp"), None),
        P(("ep", "dp"), None, None),
        P(("ep", "dp"), None, None),
        P(("ep", "dp"), None, None),
    )
    out_specs = P(("ep", "dp"), None)
    return jax.shard_map(local, mesh=mesh, in_specs=in_specs, out_specs=out_specs, check_vma=False)
```
